256 devices in a mesh: seq: 64 (over y, z, core), frame: 4 (over x).
Axes of the slice: x: 4, y: 4, z: 8, core: 2. Of those that a mesh axis runs over, the one named last changes fastest.
Arguments:
- tokens: bfloat16 [4, 128, 128, 512], P('frame', 'seq'), may hold values from -6 to 6
- row_select: bfloat16 [4, 128, 128, 64], P('frame', 'seq'), may hold values from -2 to 2
- row_decay: float32 [4, 8, 128, 128], P('frame', None, 'seq'), may hold values from -1.5 to 0, as said below
- row_gain: float32 [512], replicated, may hold values from 0.25 to 1.75
- row_skip: float32 [8], replicated, may hold values from 0.5 to 1.5
- row_in: bfloat16 [512, 512], replicated, may hold values from -0.25 to 0.25
- row_out: bfloat16 [512, 512], replicated, may hold values from -0.25 to 0.25
- col_select: bfloat16 [4, 128, 128, 64], P('frame', 'seq'), may hold values from -2 to 2
- col_decay: float32 [4, 8, 128, 128], P('frame', None, 'seq'), may hold values from -1.5 to 0, as said below
- col_gain: float32 [512], replicated, may hold values from 0.25 to 1.75
- col_skip: float32 [8], replicated, may hold values from 0.5 to 1.5
- col_in: bfloat16 [512, 512], replicated, may hold values from -0.25 to 0.25
- col_out: bfloat16 [512, 512], replicated, may hold values from -0.25 to 0.25
- cotangent: bfloat16 [4, 128, 128, 512], P('frame', 'seq'), may hold values from -6 to 6
Outputs:
- mixed: bfloat16 [4, 128, 128, 512], P('frame', 'seq')
- grad_tokens: bfloat16 [4, 128, 128, 512], P('frame', 'seq')
The draws below stay inside these ranges and needn't reach their ends.
Inputs may be any that keep to these rules, and one draw needn't show every extreme that they name: `row_decay`: every entry is below zero. `col_decay`: every entry is below zero.
All inputs are finite; a program needn't handle non-finite values.
Results may differ from the reference program's by a relative error of at most 0.013.
Values may be sent and summed in bfloat16 or wider, within the bound.
No kernel may reach another device: no remote copies, remote signals or barrier semaphores. Data moves between devices by JAX's collectives and lax.ppermute only.
A program may use at most 128 MiB of HBM per device.

```python
import jax
import jax.numpy as jnp
from jax import lax

D = 512
SCANNER_GROUPS = 8
STATE = 32
TOK_DEV = 256
ROWS = 128
COLS = 128
N_FRAME = 4


def decay_chain(key, first_count, second_count, fast_share):
    series_extent = N_FRAME * first_count * second_count
    current_paths = jax.random.split(key, 7)
    fast_heads = jax.random.uniform(current_paths[0], (SCANNER_GROUPS, 1)) < fast_share
    slow_rate = jnp.exp(jax.random.uniform(current_paths[1], (SCANNER_GROUPS, 1), minval=jnp.log(0.05), maxval=jnp.log(0.5))) / series_extent
    fast_rate = jnp.exp(jax.random.uniform(current_paths[2], (SCANNER_GROUPS, 1), minval=jnp.log(0.03), maxval=jnp.log(0.1)))
    attention_fading_speed = jnp.where(fast_heads, fast_rate, slow_rate)
    boundary_perturbation = jax.random.uniform(current_paths[3], (SCANNER_GROUPS, series_extent), minval=0.5, maxval=1.5)
    segments = series_extent // TOK_DEV
    segment_scale = jnp.exp(jax.random.uniform(current_paths[4], (SCANNER_GROUPS, segments, 1), minval=jnp.log(0.6), maxval=jnp.log(1.6)))
    dispersion_multiplier = jnp.broadcast_to(segment_scale, (SCANNER_GROUPS, segments, TOK_DEV)).reshape(SCANNER_GROUPS, series_extent)
    sudden_placements = jax.random.randint(current_paths[5], (2,), 0, series_extent)
    sudden_penalty_amounts = jnp.log(jax.random.uniform(current_paths[6], (SCANNER_GROUPS, 2), minval=0.55, maxval=0.8))
    indicator_switches = (jnp.arange(series_extent)[None, :] == sudden_placements[:, None]).astype(jnp.float32)
    sudden_occurrences = jnp.dot(sudden_penalty_amounts, indicator_switches)
    connected_series = sudden_occurrences - attention_fading_speed * boundary_perturbation * dispersion_multiplier
    return connected_series.reshape(SCANNER_GROUPS, N_FRAME, first_count, second_count).transpose(1, 0, 2, 3).astype(jnp.float32)


def draw_row_decay(key, part):
    fast_share = 0.5
    return decay_chain(jax.random.fold_in(key, 11), ROWS, COLS, fast_share)


def draw_col_decay(key, part):
    fast_share = 0.5
    return decay_chain(jax.random.fold_in(key, 23), COLS, ROWS, fast_share)


def block_levels(own_key, shape, cuts, least, largest):
    factor_of = 1.0
    for axis_at, blocks in cuts:
        steps = jax.random.uniform(jax.random.fold_in(jax.random.fold_in(own_key, 6), axis_at), (blocks,), jnp.float32, least / len(cuts), largest / len(cuts))
        factor_of = factor_of * jnp.repeat(jnp.exp(steps), shape[axis_at] // blocks).reshape((-1,) + (1,) * (len(shape) - 1 - axis_at))
    return factor_of


def gaussian(rng, shape, spread, limit, cuts=(), held_as=jnp.bfloat16):
    level = block_levels(rng, shape, cuts, -0.22, 0.18) if cuts else 1.0
    values = jax.random.normal(rng, shape, jnp.float32) * spread * level
    return jnp.minimum(jnp.maximum(values, -limit), limit).astype(held_as)


def setup_inputs(seed: int = 0) -> dict:
    keys = jax.random.split(jax.random.key(seed), 15)
    tokens = gaussian(keys[0], (N_FRAME, ROWS, COLS, D), 1.0, 6.0, ((0, 4), (1, 64)))
    row_select = gaussian(keys[1], (N_FRAME, ROWS, COLS, 2 * STATE), 0.35, 2.0, ((0, 4), (1, 64)))
    row_decay = draw_row_decay(jax.random.fold_in(keys[14], 71), 0)
    row_gain = jnp.clip(1.0 + 0.15 * jax.random.normal(keys[3], (D,), jnp.float32), 0.25, 1.75)
    row_skip = jnp.clip(jax.random.uniform(keys[4], (SCANNER_GROUPS,), jnp.float32, 0.5, 1.5), 0.5, 1.5)
    row_in = gaussian(keys[5], (D, D), D ** -0.5, 0.25)
    row_out = gaussian(keys[6], (D, D), D ** -0.5, 0.25)
    col_select = gaussian(keys[7], (N_FRAME, COLS, ROWS, 2 * STATE), 0.35, 2.0, ((0, 4), (1, 64)))
    col_decay = draw_col_decay(jax.random.fold_in(keys[14], 71), 0)
    col_gain = jnp.clip(1.0 + 0.15 * jax.random.normal(keys[9], (D,), jnp.float32), 0.25, 1.75)
    col_skip = jnp.clip(jax.random.uniform(keys[10], (SCANNER_GROUPS,), jnp.float32, 0.5, 1.5), 0.5, 1.5)
    col_in = gaussian(keys[11], (D, D), D ** -0.5, 0.25)
    col_out = gaussian(keys[12], (D, D), D ** -0.5, 0.25)
    cotangent = gaussian(keys[13], (N_FRAME, COLS, ROWS, D), 1.0, 6.0, ((0, 4), (1, 64)))
    return dict(tokens=tokens, row_select=row_select, row_decay=row_decay, row_gain=row_gain, row_skip=row_skip, row_in=row_in, row_out=row_out, col_select=col_select, col_decay=col_decay, col_gain=col_gain, col_skip=col_skip, col_in=col_in, col_out=col_out, cotangent=cotangent)


EPSILON = 1e-05
PRECISE = lax.Precision.HIGHEST

def rounded(values):
    return lax.optimization_barrier(values.astype(jnp.bfloat16)).astype(jnp.float32)

def norm_rows(values, norm_gain):
    floats = values.astype(jnp.float32)
    factor = lax.rsqrt(lax.optimization_barrier(jnp.mean(floats * floats, axis=-1, keepdims=True)) + EPSILON)
    return (floats * factor * norm_gain).astype(jnp.bfloat16)

def block_terms(select_block, decay_block):
    extent = decay_block.shape[1]
    half_width = select_block.shape[1] // 2
    summed = jnp.cumsum(decay_block, axis=1)
    inward = jnp.sqrt(-jnp.expm1(2.0 * decay_block))
    target = lax.broadcasted_iota(jnp.int32, (extent, extent), 0)
    source = lax.broadcasted_iota(jnp.int32, (extent, extent), 1)
    causal = (target >= source).astype(jnp.float32)
    gap_sums = jnp.minimum(summed[:, :, None] - summed[:, None, :], 0.0)
    affinity = jnp.dot(select_block[:, half_width:], select_block[:, :half_width].T, preferred_element_type=jnp.float32)
    mixing = rounded(jnp.exp(gap_sums) * causal * affinity[None] * inward[:, None, :])
    opening = jnp.exp(summed)
    ending = jnp.exp(summed[:, -1:] - summed) * inward
    return (mixing, opening, ending, jnp.exp(summed[:, -1]))

def forward_block(memory, block_piece, skip_gain):
    values, select_block, decay_block = block_piece
    half_width = select_block.shape[1] // 2
    mixing, opening, ending, through = block_terms(select_block, decay_block)
    floats = values.astype(jnp.float32)
    readout = select_block[:, half_width:].astype(jnp.float32)
    writein = select_block[:, :half_width].astype(jnp.float32)
    within = jnp.einsum('hts,shp->thp', mixing, floats, precision=PRECISE)
    carried = jnp.einsum('tn,hpn->thp', readout, memory, precision=PRECISE) * opening.T[:, :, None]
    output = within + carried + skip_gain[None, :, None] * floats
    weighted = rounded(floats * ending.T[:, :, None])
    memory = through[:, None, None] * memory + jnp.einsum('shp,sn->hpn', weighted, writein, precision=PRECISE)
    return (memory, output)

def backward_block(memory, block_piece, skip_gain):
    values, select_block, decay_block = block_piece
    half_width = select_block.shape[1] // 2
    mixing, opening, ending, through = block_terms(select_block, decay_block)
    floats = values.astype(jnp.float32)
    readout = select_block[:, half_width:].astype(jnp.float32)
    writein = select_block[:, :half_width].astype(jnp.float32)
    within = jnp.einsum('hts,thp->shp', mixing, floats, precision=PRECISE)
    carried = jnp.einsum('sn,hpn->shp', writein, memory, precision=PRECISE) * ending.T[:, :, None]
    output = within + carried + skip_gain[None, :, None] * floats
    weighted = rounded(floats * opening.T[:, :, None])
    memory = through[:, None, None] * memory + jnp.einsum('thp,tn->hpn', weighted, readout, precision=PRECISE)
    return (memory, output)

def run_chain(values, select, decay, skip_gain, backward):
    series_extent, model_width = values.shape
    head_count = decay.shape[0]
    half_width = select.shape[1] // 2
    block_size = min(512, TOK_DEV)
    block_count = series_extent // block_size
    pieces = (values.reshape(block_count, block_size, head_count, model_width // head_count), select.reshape(block_count, block_size, select.shape[1]), decay.reshape(head_count, block_count, block_size).transpose(1, 0, 2))
    zero_state = jnp.zeros((head_count, model_width // head_count, half_width), jnp.float32)

    def advance(memory, block_piece):
        if backward:
            return backward_block(memory, block_piece, skip_gain)
        return forward_block(memory, block_piece, skip_gain)
    last_state, results = lax.scan(advance, zero_state, pieces, reverse=backward)
    return results.reshape(series_extent, model_width).astype(jnp.bfloat16)

def mixer_forward(inputs, select, decay, norm_gain, skip_gain, weight_in, weight_out):
    normed = norm_rows(inputs, norm_gain)
    projected = jnp.dot(normed, weight_in, preferred_element_type=jnp.float32).astype(jnp.bfloat16)
    scanned = run_chain(projected, select, decay, skip_gain, False)
    total = inputs.astype(jnp.float32) + jnp.dot(scanned, weight_out, preferred_element_type=jnp.float32)
    return total.astype(jnp.bfloat16)

def mixer_backward(inputs, incoming, select, decay, norm_gain, skip_gain, weight_in, weight_out):
    pulled = jnp.dot(incoming, weight_out.T, preferred_element_type=jnp.float32).astype(jnp.bfloat16)
    scanned = run_chain(pulled, select, decay, skip_gain, True)
    returned = jnp.dot(scanned, weight_in.T, preferred_element_type=jnp.float32)
    floats = inputs.astype(jnp.float32)
    factor = lax.rsqrt(lax.optimization_barrier(jnp.mean(floats * floats, axis=-1, keepdims=True)) + EPSILON)
    scaled = norm_gain * returned
    result = incoming.astype(jnp.float32) + factor * scaled - floats * factor ** 3 * lax.optimization_barrier(jnp.mean(scaled * floats, axis=-1, keepdims=True))
    return result.astype(jnp.bfloat16)

def reference(tokens, row_select, row_decay, row_gain, row_skip, row_in, row_out, col_select, col_decay, col_gain, col_skip, col_in, col_out, cotangent):
    frame_count, row_count, col_count, model_width = tokens.shape
    head_count = row_skip.shape[0]
    doubled = row_select.shape[-1]
    row_inputs = tokens.reshape(-1, model_width)
    row_lam = row_decay.transpose(1, 0, 2, 3).reshape(head_count, -1)
    col_lam = col_decay.transpose(1, 0, 2, 3).reshape(head_count, -1)
    row_mixed = mixer_forward(row_inputs, row_select.reshape(-1, doubled), row_lam, row_gain, row_skip, row_in, row_out)
    col_tokens = row_mixed.reshape(frame_count, row_count, col_count, model_width).transpose(0, 2, 1, 3).reshape(-1, model_width)
    mixed = mixer_forward(col_tokens, col_select.reshape(-1, doubled), col_lam, col_gain, col_skip, col_in, col_out)
    col_grad = mixer_backward(col_tokens, cotangent.reshape(-1, model_width), col_select.reshape(-1, doubled), col_lam, col_gain, col_skip, col_in, col_out)
    row_grad = col_grad.reshape(frame_count, col_count, row_count, model_width).transpose(0, 2, 1, 3).reshape(-1, model_width)
    grad_tokens = mixer_backward(row_inputs, row_grad, row_select.reshape(-1, doubled), row_lam, row_gain, row_skip, row_in, row_out)
    return (mixed.reshape(frame_count, col_count, row_count, model_width), grad_tokens.reshape(frame_count, row_count, col_count, model_width))
```

```python
from functools import partial

import jax
import jax.numpy as jnp
from jax import lax
from jax.experimental import pallas as pl
from jax.experimental.pallas import tpu as pltpu
from jax.sharding import Mesh
from jax.sharding import PartitionSpec as P

SEQ = ("seq_0", "seq_1", "seq_2")
INNER = ("seq_1", "seq_2")
OUTER = ("frame", "seq_0")

EPSILON = 1e-05
LOG2E = 1.4426950408889634

TOK = 256
WIDTH = 512
HEADS = 8
PART = 64
STATE = 32
GROUP = 16
ROWS8 = 8
HALF = 256

F32 = jnp.float32
BF16 = jnp.bfloat16


def iota(shape, axis):
    return lax.broadcasted_iota(jnp.int32, shape, axis)


def nn(left, right):
    return lax.dot_general(left, right, (((1,), (0,)), ((), ())), preferred_element_type=F32)


def nt(left, right):
    return lax.dot_general(left, right, (((1,), (1,)), ((), ())), preferred_element_type=F32)


def pieces(values, count):
    out = []
    rest = values
    for _ in range(count):
        piece = rest.astype(BF16)
        out.append(piece)
        rest = rest - piece.astype(F32)
    return out


def one_minus_exp(v):
    series = 1.0 - v * (1.0 / 9.0)
    for k in range(8, 1, -1):
        series = 1.0 - v * (1.0 / k) * series
    return jnp.where(v < 0.5, v * series, 1.0 - jnp.exp(-v))


def decay_terms(lam_ref):
    lam = jnp.concatenate([lam_ref[:, 0, :], lam_ref[:, 1, :]], axis=1)
    parts = pieces(lam, 3)
    first = iota((TOK, TOK), 0)
    second = iota((TOK, TOK), 1)
    upto = (second <= first).astype(F32).astype(BF16)
    same = (second == first).astype(F32).astype(BF16)
    cum_col = sum(nt(upto, p) for p in reversed(parts))
    cum_row = sum(nt(p, upto) for p in reversed(parts))
    lam_col = sum(nt(same, p) for p in reversed(parts))
    square_col = one_minus_exp(-2.0 * lam_col)
    square_row = one_minus_exp(-2.0 * lam)
    return cum_col, cum_row, square_col, square_row


def cum_of(lam_ref):
    lam = jnp.concatenate([lam_ref[:, 0, :], lam_ref[:, 1, :]], axis=1)
    parts = pieces(lam, 3)
    first = iota((TOK, TOK), 0)
    second = iota((TOK, TOK), 1)
    upto = (second <= first).astype(F32).astype(BF16)
    same = (second == first).astype(F32).astype(BF16)
    cum_col = sum(nt(upto, p) for p in reversed(parts))
    lam_col = sum(nt(same, p) for p in reversed(parts))
    return cum_col, lam_col


def spread_heads(values, count):
    spread = (iota((HEADS, WIDTH), 1) // PART == iota((HEADS, WIDTH), 0)).astype(F32).astype(BF16)
    return sum(nn(p, spread) for p in reversed(pieces(values, count)))


def opening_of(cum_col):
    return spread_heads(jnp.exp(cum_col), 2)


def ending_of(cum_col, lam_col):
    last = cum_col[TOK - 1 : TOK, :]
    return spread_heads(jnp.exp(last - cum_col) * jnp.sqrt(one_minus_exp(-2.0 * lam_col)), 2)


def placed(select, offset, slot, copies):
    at = iota((2 * STATE, GROUP * ROWS8), 0)
    col = iota((2 * STATE, GROUP * ROWS8), 1)
    k = col % ROWS8 - slot
    hit = (at == offset + 2 * (col // ROWS8) + k % 2) & (k >= 0) & (k < copies)
    return nn(select, hit.astype(F32).astype(BF16)).astype(BF16)


def placed_rows(select, offset, slot):
    at = iota((GROUP * ROWS8, 2 * STATE), 1)
    row = iota((GROUP * ROWS8, 2 * STATE), 0)
    k = row % ROWS8 - slot
    hit = (at == offset + 2 * (row // ROWS8) + k) & (k >= 0) & (k < 2)
    return nt(hit.astype(F32).astype(BF16), select).astype(BF16)


def spent_rows(cum_col):
    tail = spread_heads(cum_col[TOK - 8 :, :], 3)[7:8, :]
    high = tail.astype(BF16).astype(F32)
    return high, tail - high


def message_part(weighted, select, offset, slot, cum_col):
    state = nn(placed_rows(select, offset, slot), weighted)
    high, low = spent_rows(cum_col)
    row = iota((GROUP * ROWS8, WIDTH), 0) % ROWS8
    return jnp.where(row == slot + 2, high, jnp.where(row == slot + 3, low, state))


def normalized(x, gain):
    factor = lax.rsqrt(jnp.mean(x * x, axis=-1, keepdims=True) + EPSILON)
    return (x * factor * gain).astype(BF16)


def local_scan(values, select, lam_ref, skip_ref, out_ref, backward):
    cum_col, cum_row, square_col, square_row = decay_terms(lam_ref)
    source = select[:, :STATE]
    target = select[:, STATE:]
    if backward:
        affinity = nt(source, target)
        left = (0.5 * jnp.log2(square_col)) - cum_col * LOG2E
        right = cum_row * LOG2E
    else:
        affinity = nt(target, source)
        left = cum_col * LOG2E
        right = (0.5 * jnp.log2(square_row)) - cum_row * LOG2E
    first = iota((128, 128), 0)
    second = iota((128, 128), 1)
    keep = second >= first if backward else second <= first
    for h in range(HEADS):
        span = slice(h * PART, (h + 1) * PART)
        v = values[:, span]
        lo, hi = slice(0, 128), slice(128, 256)
        lc = left[:, h : h + 1]
        rr = right[h : h + 1, :]

        def tile(a, b, masked):
            m = jnp.exp2(lc[a] + rr[:, b]) * affinity[a, b]
            return (jnp.where(keep, m, 0.0) if masked else m).astype(BF16)

        skip = skip_ref[h]
        if backward:
            top = nn(tile(lo, lo, True), v[lo]) + nn(tile(lo, hi, False), v[hi])
            low = nn(tile(hi, hi, True), v[hi])
        else:
            top = nn(tile(lo, lo, True), v[lo])
            low = nn(tile(hi, lo, False), v[lo]) + nn(tile(hi, hi, True), v[hi])
        out_ref[lo, span] = top + skip * v[lo].astype(F32)
        out_ref[hi, span] = low + skip * v[hi].astype(F32)


def start_kernel(
    x_ref, rsel_ref, rlam_ref, gain_ref, win_ref, y_ref, csel_ref, clam_ref, wout_ref,
    value_ref, pulled_ref, message_ref,
):
    value = nn(normalized(x_ref[...].astype(F32), gain_ref[...]), win_ref[...]).astype(BF16)
    value_ref[...] = value
    rcum, rlam = cum_of(rlam_ref)
    weighted = (value.astype(F32) * ending_of(rcum, rlam)).astype(BF16)
    first = message_part(weighted, rsel_ref[...], 0, 0, rcum)
    pulled = nt(y_ref[...], wout_ref[...]).astype(BF16)
    pulled_ref[...] = pulled
    ccum, _ = cum_of(clam_ref)
    weighted = (pulled.astype(F32) * opening_of(ccum)).astype(BF16)
    second = message_part(weighted, csel_ref[...], STATE, 4, ccum)
    row = iota((GROUP * ROWS8, WIDTH), 0) % ROWS8
    message_ref[...] = jnp.where(row < 4, first, second).astype(BF16)


def scan_kernel(value_ref, select_ref, lam_ref, skip_ref, out_ref, *, backward):
    local_scan(value_ref[...], select_ref[...], lam_ref, skip_ref, out_ref, backward)


def inner_kernel(got_ref, before_ref, total_ref):
    row = iota((ROWS8, WIDTH), 0)

    def tile(j):
        return got_ref[j * ROWS8 : (j + 1) * ROWS8, :].astype(F32)

    def spent(t, slot):
        return t[slot + 2 : slot + 3, :] + t[slot + 3 : slot + 4, :]

    gone = jnp.zeros((1, WIDTH), F32)
    state = jnp.zeros((ROWS8, WIDTH), F32)
    for j in range(GROUP):
        t = tile(j)
        before_ref[j * ROWS8 : (j + 1) * ROWS8, :] = jnp.where(row < 2, state, jnp.exp(gone))
        step = spent(t, 0)
        state = jnp.exp(step) * state + t
        gone = gone + step
    forward_state, forward_gone = state, gone
    gone = jnp.zeros((1, WIDTH), F32)
    state = jnp.zeros((ROWS8, WIDTH), F32)
    for j in reversed(range(GROUP)):
        t = tile(j)
        at = slice(j * ROWS8, (j + 1) * ROWS8)
        before_ref[at, :] = jnp.where(
            row < 4, before_ref[at, :], jnp.where(row < 6, state, jnp.exp(gone))
        )
        step = spent(t, 4)
        state = jnp.exp(step) * state + t
        gone = gone + step
    total = jnp.where(row < 2, forward_state, state)
    spent_both = jnp.where(row < 4, forward_gone, gone)
    high = spent_both.astype(BF16).astype(F32)
    total = jnp.where(row % 4 < 2, total, jnp.where(row % 4 == 2, high, spent_both - high))
    total = total.astype(BF16)
    for j in range(GROUP):
        total_ref[j * ROWS8 : (j + 1) * ROWS8, :] = total


def outer_kernel(mine_ref, got_ref, before_ref, out_ref):
    mine = mine_ref[0]
    row = iota((ROWS8, WIDTH), 0)

    def tile(j):
        return got_ref[j * ROWS8 : (j + 1) * ROWS8, :].astype(F32)

    def entering(slot, order, passed):
        state = jnp.zeros((ROWS8, WIDTH), F32)
        for j in order:
            t = tile(j)
            step = t[slot + 2 : slot + 3, :] + t[slot + 3 : slot + 4, :]
            state = jnp.where(passed(j), jnp.exp(step) * state + t, state)
        return state

    first = entering(0, range(GROUP), lambda j: j < mine)
    second = entering(4, reversed(range(GROUP)), lambda j: j > mine)
    both = jnp.where(row < 4, first, second)
    for j in range(GROUP):
        at = slice(j * ROWS8, (j + 1) * ROWS8)
        t = before_ref[at, :]
        through = jnp.where(row < 4, t[2:3, :], t[6:7, :])
        full = through * both + t
        high = full.astype(BF16).astype(F32)
        low = pltpu.roll(full - high, 2, 0)
        out_ref[at, :] = jnp.where(row % 4 < 2, high, low).astype(BF16)


def row_target(token, half):
    column = token % 128
    return (column // 2) * 8 + half * 4 + (column % 2) * 2 + token // 128


def column_target(token, half):
    row = token % 128
    return (row // 2) * 8 + half * 4 + (token // 128) * 2 + row % 2


def to_message(tokens, target):
    at = iota((2 * TOK, TOK), 0)
    token = iota((1, TOK), 1)
    out = None
    for half in (0, 1):
        hot = (at == target(token, half)).astype(F32).astype(BF16)
        part = nn(hot, tokens[:, half * HALF : (half + 1) * HALF])
        out = part if out is None else out + part
    return out.astype(BF16)


def from_message(message, target):
    at = iota((2 * TOK, TOK), 0)
    token = iota((1, TOK), 1)
    out = []
    for half in (0, 1):
        hot = (at == target(token, half)).astype(F32).astype(BF16)
        out.append(
            lax.dot_general(hot, message, (((0,), (0,)), ((), ())), preferred_element_type=F32)
        )
    return jnp.concatenate(out, axis=1)


def row_finish_kernel(x_ref, sel_ref, lam_ref, local_ref, got_ref, wout_ref, message_ref):
    cum, _ = cum_of(lam_ref)
    carried = nn(placed(sel_ref[...], STATE, 0, 4), got_ref[...]) * opening_of(cum)
    scanned = (local_ref[...] + carried).astype(BF16)
    mixed = (x_ref[...].astype(F32) + nn(scanned, wout_ref[...])).astype(BF16)
    message_ref[...] = to_message(mixed, row_target)


def col_returned_kernel(sel_ref, lam_ref, local_ref, got_ref, win_ref, gain_ref, out_ref):
    cum, lam = cum_of(lam_ref)
    carried = nn(placed(sel_ref[...], 0, 4, 4), got_ref[...]) * ending_of(cum, lam)
    scanned = (local_ref[...] + carried).astype(BF16)
    out_ref[...] = gain_ref[...] * nt(scanned, win_ref[...])


def input_gradient(x, y, scaled):
    factor = lax.rsqrt(jnp.mean(x * x, axis=-1, keepdims=True) + EPSILON)
    inner = jnp.mean(scaled * x, axis=-1, keepdims=True)
    return (y + factor * scaled - x * (factor * factor * factor) * inner).astype(BF16)


def col_grad_kernel(got_ref, y_ref, scaled_ref, x_ref, message_ref):
    x = from_message(got_ref[...], column_target)
    x_ref[...] = x.astype(BF16)
    grad = input_gradient(x, y_ref[...].astype(F32), scaled_ref[...])
    message_ref[...] = to_message(grad, column_target)


def col_value_kernel(x_ref, sel_ref, lam_ref, gain_ref, win_ref, value_ref, part_ref):
    value = nn(normalized(x_ref[...].astype(F32), gain_ref[...]), win_ref[...]).astype(BF16)
    value_ref[...] = value
    cum, lam = cum_of(lam_ref)
    weighted = (value.astype(F32) * ending_of(cum, lam)).astype(BF16)
    part_ref[...] = message_part(weighted, sel_ref[...], 0, 0, cum).astype(BF16)


def row_pull_kernel(
    got_ref, sel_ref, lam_ref, wout_ref, part_ref, y_ref, pulled_ref, message_ref
):
    y = from_message(got_ref[...], row_target).astype(BF16)
    y_ref[...] = y
    pulled = nt(y, wout_ref[...]).astype(BF16)
    pulled_ref[...] = pulled
    cum, _ = cum_of(lam_ref)
    weighted = (pulled.astype(F32) * opening_of(cum)).astype(BF16)
    second = message_part(weighted, sel_ref[...], STATE, 4, cum)
    row = iota((GROUP * ROWS8, WIDTH), 0) % ROWS8
    message_ref[...] = jnp.where(row < 4, part_ref[...].astype(F32), second).astype(BF16)


def end_kernel(
    got_ref, cx_ref, csel_ref, clam_ref, clocal_ref, cwout_ref,
    x_ref, y_ref, rsel_ref, rlam_ref, rlocal_ref, rwin_ref, gain_ref,
    mixed_ref, grad_ref,
):
    got = got_ref[...]
    cum, _ = cum_of(clam_ref)
    carried = nn(placed(csel_ref[...], STATE, 0, 4), got) * opening_of(cum)
    scanned = (clocal_ref[...] + carried).astype(BF16)
    mixed_ref[...] = (cx_ref[...].astype(F32) + nn(scanned, cwout_ref[...])).astype(BF16)
    cum, lam = cum_of(rlam_ref)
    carried = nn(placed(rsel_ref[...], 0, 4, 4), got) * ending_of(cum, lam)
    scanned = (rlocal_ref[...] + carried).astype(BF16)
    scaled = gain_ref[...] * nt(scanned, rwin_ref[...])
    grad_ref[...] = input_gradient(x_ref[...].astype(F32), y_ref[...].astype(F32), scaled)


VM = pl.BlockSpec(memory_space=pltpu.VMEM)
SM = pl.BlockSpec(memory_space=pltpu.SMEM)


def call(kernel, name, outs, args, scalars=(), flops=4e8):
    return pl.pallas_call(
        kernel,
        name=name,
        out_shape=[jax.ShapeDtypeStruct(s, d) for s, d in outs],
        in_specs=[SM if i in scalars else VM for i in range(len(args))],
        out_specs=[VM] * len(outs),
        cost_estimate=pl.CostEstimate(flops=int(flops), bytes_accessed=1 << 20, transcendentals=0),
    )(*args)


TOKS = (TOK, WIDTH)
MSG = (GROUP * ROWS8, WIDTH)
BIG = (2 * TOK, HALF)


def swapped(array, axes):
    count = 1
    for axis in axes:
        count *= lax.axis_size(axis)
    split = array.reshape(count, array.shape[0] // count, array.shape[1])
    return lax.all_to_all(split, axes, split_axis=0, concat_axis=0, tiled=True).reshape(array.shape)


def carry(message, mine):
    got = swapped(message, INNER)
    before, total = call(inner_kernel, "inner", [(MSG, F32), (MSG, BF16)], [got], flops=1e6)
    groups = swapped(total, OUTER)
    (down,) = call(outer_kernel, "outer", [(MSG, BF16)], [mine, groups, before], (0,), flops=1e6)
    return swapped(down, INNER)


def local(value, select, lam, skip, backward, name):
    (out,) = call(
        partial(scan_kernel, backward=backward), name, [(TOKS, F32)],
        [value, select, lam, skip], (3,), flops=2e9,
    )
    return out


def body(
    tokens, row_select, row_decay, row_gain, row_skip, row_in, row_out,
    col_select, col_decay, col_gain, col_skip, col_in, col_out, cotangent,
):
    mine = (lax.axis_index("frame") * lax.axis_size("seq_0") + lax.axis_index("seq_0")).reshape(1)
    x = tokens.reshape(TOKS)
    y = cotangent.reshape(TOKS)
    rsel = row_select.reshape(TOK, 2 * STATE)
    csel = col_select.reshape(TOK, 2 * STATE)
    rlam = row_decay.reshape(HEADS, 2, 128)
    clam = col_decay.reshape(HEADS, 2, 128)
    rgain = row_gain.reshape(1, WIDTH)
    cgain = col_gain.reshape(1, WIDTH)

    rvalue, cpulled, message = call(
        start_kernel, "start", [(TOKS, BF16), (TOKS, BF16), (MSG, BF16)],
        [x, rsel, rlam, rgain, row_in, y, csel, clam, col_out],
    )
    rlocal = local(rvalue, rsel, rlam, row_skip, False, "row_scan")
    clocal = local(cpulled, csel, clam, col_skip, True, "col_scan_back")
    got = carry(message, mine)
    (sending,) = call(
        row_finish_kernel, "row_finish", [(BIG, BF16)], [x, rsel, rlam, rlocal, got, row_out]
    )
    (scaled,) = call(
        col_returned_kernel, "col_returned", [(TOKS, F32)],
        [csel, clam, clocal, got, col_in, cgain],
    )
    arrived = swapped(sending, SEQ)
    cx, returning = call(
        col_grad_kernel, "col_grad", [(TOKS, BF16), (BIG, BF16)], [arrived, y, scaled]
    )
    landed = swapped(returning, SEQ)
    cvalue, part = call(
        col_value_kernel, "col_value", [(TOKS, BF16), (MSG, BF16)], [cx, csel, clam, cgain, col_in]
    )
    clocal2 = local(cvalue, csel, clam, col_skip, False, "col_scan")
    ry, rpulled, message = call(
        row_pull_kernel, "row_pull", [(TOKS, BF16), (TOKS, BF16), (MSG, BF16)],
        [landed, rsel, rlam, row_out, part],
    )
    rlocal2 = local(rpulled, rsel, rlam, row_skip, True, "row_scan_back")
    got = carry(message, mine)
    mixed, grad = call(
        end_kernel, "end", [(TOKS, BF16), (TOKS, BF16)],
        [got, cx, csel, clam, clocal2, col_out, x, ry, rsel, rlam, rlocal2, row_in, rgain],
    )
    return mixed.reshape(cotangent.shape), grad.reshape(tokens.shape)


def solution(mesh):
    torus = Mesh(
        mesh.devices.reshape(4, 8, 2, mesh.shape["frame"]), ("seq_0", "seq_1", "seq_2", "frame")
    )
    tall = P("frame", SEQ, None, None)
    flat = P("frame", None, SEQ, None)
    in_specs = (tall, tall, flat, P(), P(), P(), P(), tall, flat, P(), P(), P(), P(), tall)
    return jax.shard_map(
        body, mesh=torus, in_specs=in_specs, out_specs=(tall, tall), check_vma=False
    )
```

```python
from functools import partial

import jax
import jax.numpy as jnp
from jax import lax
from jax.experimental import pallas as pl
from jax.experimental.pallas import tpu as pltpu
from jax.sharding import Mesh
from jax.sharding import PartitionSpec as P

SEQ = ("seq_0", "seq_1", "seq_2")
INNER = ("seq_2", "seq_1")
OUTER = ("seq_0", "frame")

EPSILON = 1e-05
LOG2E = 1.4426950408889634

TOK = 256
WIDTH = 512
HEADS = 8
PART = 64
STATE = 32
GROUP = 16
HALF = 256
LINES = GROUP * 8
LOGS = 128

F32 = jnp.float32
BF16 = jnp.bfloat16


def iota(shape, axis):
    return lax.broadcasted_iota(jnp.int32, shape, axis)


def onehot(mask):
    return mask.astype(F32).astype(BF16)


def dot(left, right, left_axis, right_axis):
    return lax.dot_general(
        left, right, (((left_axis,), (right_axis,)), ((), ())), preferred_element_type=F32
    )


def nn(left, right):
    return dot(left, right, 1, 0)


def nt(left, right):
    return dot(left, right, 1, 1)


def tn(left, right):
    return dot(left, right, 0, 0)


def parts_of(values, count):
    out = []
    rest = values
    for _ in range(count):
        piece = rest.astype(BF16)
        out.append(piece)
        rest = rest - piece.astype(F32)
    return out


def one_minus_exp(v):
    series = 1.0 - v * (1.0 / 9.0)
    for k in range(8, 1, -1):
        series = 1.0 - v * (1.0 / k) * series
    return jnp.where(v < 0.5, v * series, 1.0 - jnp.exp(-v))


def lam_of(lam_ref):
    return jnp.concatenate([lam_ref[:, 0, :], lam_ref[:, 1, :]], axis=1)


def turned_select(select_ref):
    return jnp.concatenate([select_ref[0], select_ref[1]], axis=1)


def triangle():
    return onehot(iota((TOK, TOK), 1) <= iota((TOK, TOK), 0))


def cum_columns(lam):
    upto = triangle()
    return sum(nt(upto, p) for p in reversed(parts_of(lam, 3)))


def cum_rows(lam):
    upto = triangle()
    return sum(nt(p, upto) for p in reversed(parts_of(lam, 3)))


def columns(lam):
    same = onehot(iota((TOK, TOK), 1) == iota((TOK, TOK), 0))
    return sum(nt(same, p) for p in reversed(parts_of(lam, 3)))


def spread_heads(values):
    spread = onehot(iota((HEADS, WIDTH), 1) // PART == iota((HEADS, WIDTH), 0))
    return sum(nn(p, spread) for p in reversed(parts_of(values, 2)))


def opening_of(cum_col):
    return jnp.exp(cum_col)


def ending_of(cum_col, lam_col):
    last = cum_col[TOK - 1 : TOK, :]
    return jnp.exp(last - cum_col) * jnp.sqrt(one_minus_exp(-2.0 * lam_col))


def placed(select, offset, stream):
    at = iota((2 * STATE, 2 * LINES), 0)
    col = iota((2 * STATE, 2 * LINES), 1)
    row = col % LINES
    hit = (at == offset + 2 * (row // 8) + row % 2) & (row % 8 // 2 == col // LINES * 2 + stream)
    return tn(select, onehot(hit)).astype(BF16)


def carried_of(placed_pair, got):
    return jnp.concatenate(
        [nn(placed_pair[:, half * LINES : (half + 1) * LINES], got) for half in (0, 1)], axis=1
    )


def state_rows(weighted, select, offset, stream):
    at = iota((LINES, 2 * STATE), 1)
    row = iota((LINES, 2 * STATE), 0)
    out = None
    for half in (0, 1):
        hit = (at == offset + 2 * (row // 8) + row % 2) & (row % 8 // 2 == half * 2 + stream)
        rows = nn(onehot(hit), select).astype(BF16)
        part = nn(rows, weighted[:, half * HALF : (half + 1) * HALF])
        out = part if out is None else out + part
    return out


def normalized(x, gain):
    factor = lax.rsqrt(jnp.mean(x * x, axis=-1, keepdims=True) + EPSILON)
    return (x * factor * gain).astype(BF16)


def input_gradient(x, y, scaled):
    factor = lax.rsqrt(jnp.mean(x * x, axis=-1, keepdims=True) + EPSILON)
    inner = jnp.mean(scaled * x, axis=-1, keepdims=True)
    return (y + factor * scaled - x * (factor * factor * factor) * inner).astype(BF16)


def local_scan(values_ref, select, lam, cum_col, lam_col, skip_ref, out_ref, backward):
    cum_row = cum_rows(lam)
    source = select[:STATE]
    target = select[STATE:]
    if backward:
        affinity = tn(source, target)
        left = 0.5 * jnp.log2(one_minus_exp(-2.0 * lam_col)) - cum_col * LOG2E
        right = cum_row * LOG2E
    else:
        affinity = tn(target, source)
        left = cum_col * LOG2E
        right = 0.5 * jnp.log2(one_minus_exp(-2.0 * lam)) - cum_row * LOG2E
    first = iota((128, 128), 0)
    second = iota((128, 128), 1)
    keep = second >= first if backward else second <= first
    lo, hi = slice(0, 128), slice(128, 256)
    for h in range(HEADS):
        span = slice(h * PART, (h + 1) * PART)
        lc = left[:, h : h + 1]
        rr = right[h : h + 1, :]

        def tile(a, b, masked):
            m = jnp.exp2(lc[a] + rr[:, b]) * affinity[a, b]
            return (jnp.where(keep, m, 0.0) if masked else m).astype(BF16)

        v_lo = values_ref[lo, span]
        v_hi = values_ref[hi, span]
        skip = skip_ref[0:1, h : h + 1]
        if backward:
            top = nn(tile(lo, lo, True), v_lo) + nn(tile(lo, hi, False), v_hi)
            low = nn(tile(hi, hi, True), v_hi)
        else:
            top = nn(tile(lo, lo, True), v_lo)
            low = nn(tile(hi, lo, False), v_lo) + nn(tile(hi, hi, True), v_hi)
        out_ref[lo, span] = top + skip * v_lo.astype(F32)
        out_ref[hi, span] = low + skip * v_hi.astype(F32)


def row_target(token):
    column = token % 128
    return column // 2 * 8 + column % 2 * 2 + token // 128


def column_target(token):
    row = token % 128
    return row // 2 * 8 + token // 128 * 2 + row % 2


def to_message(tokens, target):
    off = iota((2 * TOK, TOK), 0) - target(iota((1, TOK), 1))
    left = nn(onehot(off == 0), tokens[:, :HALF])
    return (left + nn(onehot(off == 4), tokens[:, HALF:])).astype(BF16)


def from_message(message, target):
    off = iota((TOK, 2 * TOK), 1) - target(iota((TOK, 1), 0))
    return jnp.concatenate([nn(onehot(off == 0), message), nn(onehot(off == 4), message)], axis=1)


def start_kernel(
    x_hbm, rsel_hbm, rlam_hbm, gain_hbm, win_hbm, y_hbm, csel_hbm, clam_hbm, wout_hbm,
    value_hbm, pulled_hbm, message_ref,
    x_ref, rsel_ref, rlam_ref, gain_ref, win_ref, y_ref, csel_ref, clam_ref, wout_ref,
    value_ref, pulled_ref, sem,
):
    def copy(a, b, i):
        return pltpu.make_async_copy(a, b, sem.at[i])

    rlam_in, clam_in = copy(rlam_hbm, rlam_ref, 0), copy(clam_hbm, clam_ref, 1)
    gain_in, x_in = copy(gain_hbm, gain_ref, 2), copy(x_hbm, x_ref, 3)
    win_in, rsel_in = copy(win_hbm, win_ref, 4), copy(rsel_hbm, rsel_ref, 5)
    y_in, wout_in = copy(y_hbm, y_ref, 6), copy(wout_hbm, wout_ref, 7)
    csel_in = copy(csel_hbm, csel_ref, 8)
    for one in (rlam_in, clam_in, gain_in, x_in, win_in, rsel_in, y_in, wout_in, csel_in):
        one.start()
    rlam_in.wait()
    rlam = lam_of(rlam_ref)
    rcum = cum_columns(rlam)
    ending = spread_heads(ending_of(rcum, columns(rlam)))
    clam_in.wait()
    clam = lam_of(clam_ref)
    ccum = cum_columns(clam)
    opening = spread_heads(opening_of(ccum))
    row = iota((8, HEADS), 0)
    head = iota((8, HEADS), 1)
    logs = jnp.where(row % 4 < 2, rcum[TOK - 1 : TOK, :], ccum[TOK - 1 : TOK, :])
    logs = jnp.where(head // 4 == row // 4, logs, 0.0)
    tile = None
    for k, piece in enumerate(parts_of(logs, 3)):
        place = onehot(iota((HEADS, LOGS), 1) == 4 * k + iota((HEADS, LOGS), 0) % 4)
        part = nn(piece, place)
        tile = part if tile is None else tile + part
    tile = tile.astype(BF16)
    for j in range(GROUP):
        message_ref[j * 8 : (j + 1) * 8, HALF:] = tile
    gain_in.wait()
    x_in.wait()
    normed = normalized(x_ref[...].astype(F32), gain_ref[...])
    win_in.wait()
    value = nn(normed, win_ref[...]).astype(BF16)
    value_ref[...] = value
    value_out = copy(value_ref, value_hbm, 9)
    value_out.start()
    rsel_in.wait()
    weighted = (value.astype(F32) * ending).astype(BF16)
    first = state_rows(weighted, turned_select(rsel_ref), 0, 0)
    y_in.wait()
    wout_in.wait()
    pulled = nt(y_ref[...], wout_ref[...]).astype(BF16)
    pulled_ref[...] = pulled
    pulled_out = copy(pulled_ref, pulled_hbm, 10)
    pulled_out.start()
    csel_in.wait()
    weighted = (pulled.astype(F32) * opening).astype(BF16)
    second = state_rows(weighted, turned_select(csel_ref), STATE, 1)
    message_ref[:, :HALF] = (first + second).astype(BF16)
    value_out.wait()
    pulled_out.wait()


def logs_spread(tiles):
    spread = onehot(
        (iota((LOGS, HALF), 0) % 4 == iota((LOGS, HALF), 1) // PART) & (iota((LOGS, HALF), 0) < 12)
    )
    return nn(tiles, spread)


def inner_order(j):
    return j % 2 * 8 + j // 2


def outer_order(j):
    return j % 4 * 4 + j // 4


def tile_at(j):
    return slice(j * 8, (j + 1) * 8)


def stream_mask():
    return iota((8, HALF), 0) % 4 < 2


def pick(a_forward, forward, backward):
    first = stream_mask()
    return jnp.where(first, forward, backward) if a_forward else jnp.where(first, backward, forward)


def inner_scan(tile, decay, a_forward, before_ref):
    spots = [inner_order(j) for j in range(GROUP)]
    state = jnp.zeros((8, HALF), F32)
    forward = {}
    for j in spots:
        forward[j] = state
        state = decay(j) * state + tile(j)
    ahead = state
    state = jnp.zeros((8, HALF), F32)
    for j in reversed(spots):
        before_ref[tile_at(j), :] = pick(a_forward, forward[j], state)
        state = decay(j) * state + tile(j)
    return pick(a_forward, ahead, state).astype(BF16)


def inner_first_kernel(got_ref, before_ref, decay_ref, through_ref, later_ref, total_ref):
    logs = logs_spread(got_ref[:, HALF:])
    decay_ref[...] = jnp.exp(logs)
    total = inner_scan(
        lambda j: got_ref[tile_at(j), :HALF].astype(F32),
        lambda j: decay_ref[tile_at(j), :], True, before_ref,
    )
    compact = jnp.zeros((8, LOGS), F32)
    for j in range(GROUP):
        compact = compact + got_ref[tile_at(j), HALF:].astype(F32)
    compact = compact + pltpu.roll(compact, LOGS - 4, 1) + pltpu.roll(compact, LOGS - 8, 1)
    compact = jnp.where(iota((8, LOGS), 1) < 4, compact, 0.0)
    high = compact.astype(BF16).astype(F32)
    middle = (compact - high).astype(BF16).astype(F32)
    low = compact - high - middle
    compact = (high + pltpu.roll(middle, 4, 1) + pltpu.roll(low, 8, 1)).astype(BF16)
    for j in range(GROUP):
        total_ref[tile_at(j), :HALF] = total
        total_ref[tile_at(j), HALF:] = compact
    spots = [inner_order(j) for j in range(GROUP)]
    gone = jnp.zeros((8, HALF), F32)
    earlier = {}
    for j in spots:
        earlier[j] = gone
        gone = gone + logs[tile_at(j), :]
    gone = jnp.zeros((8, HALF), F32)
    for j in reversed(spots):
        ahead, behind = jnp.exp(earlier[j]), jnp.exp(gone)
        through_ref[tile_at(j), :] = pick(True, ahead, behind)
        later_ref[tile_at(j), :] = pick(False, ahead, behind)
        gone = gone + logs[tile_at(j), :]


def inner_second_kernel(got_ref, decay_ref, before_ref, total_ref):
    total = inner_scan(
        lambda j: got_ref[tile_at(j), :].astype(F32),
        lambda j: decay_ref[tile_at(j), :], False, before_ref,
    )
    for j in range(GROUP):
        total_ref[tile_at(j), :] = total


def outer_scan(mine, tile, decay, a_forward, before_ref, through_ref, out_ref):
    state = jnp.zeros((8, HALF), F32)
    for j in range(GROUP):
        at = outer_order(j)
        state = jnp.where(j < mine, decay(at) * state + tile(at), state)
    ahead = state
    state = jnp.zeros((8, HALF), F32)
    for j in reversed(range(GROUP)):
        at = outer_order(j)
        state = jnp.where(j > mine, decay(at) * state + tile(at), state)
    both = pick(a_forward, ahead, state)
    for j in range(GROUP):
        at = tile_at(j)
        out_ref[at, :] = (through_ref[at, :] * both + before_ref[at, :]).astype(BF16)


def outer_first_kernel(mine_ref, got_ref, before_ref, through_ref, decay_ref, out_ref):
    decay_ref[...] = jnp.exp(logs_spread(got_ref[:, HALF:]))
    outer_scan(
        mine_ref[0], lambda j: got_ref[tile_at(j), :HALF].astype(F32),
        lambda j: decay_ref[tile_at(j), :], True, before_ref, through_ref, out_ref,
    )


def outer_second_kernel(mine_ref, got_ref, before_ref, through_ref, decay_ref, out_ref):
    outer_scan(
        mine_ref[0], lambda j: got_ref[tile_at(j), :].astype(F32),
        lambda j: decay_ref[tile_at(j), :], False, before_ref, through_ref, out_ref,
    )


def row_scan_kernel(value_ref, sel_ref, lam_ref, skip_ref, local_ref, opening_ref, placed_ref):
    lam = lam_of(lam_ref)
    cum_col = cum_columns(lam)
    select = turned_select(sel_ref)
    opening_ref[...] = opening_of(cum_col)
    placed_ref[...] = placed(select, STATE, 0)
    local_scan(value_ref, select, lam, cum_col, None, skip_ref, local_ref, False)


def row_finish_kernel(x_ref, local_ref, opening_ref, placed_ref, got_ref, wout_ref, message_ref):
    carried = carried_of(placed_ref[...], got_ref[...]) * spread_heads(opening_ref[...])
    scanned = (local_ref[...] + carried).astype(BF16)
    mixed = (x_ref[...].astype(F32) + nn(scanned, wout_ref[...])).astype(BF16)
    message_ref[...] = to_message(mixed, row_target)


def col_back_kernel(
    value_ref, sel_ref, lam_ref, skip_ref, got_ref, win_ref, gain_ref, out_ref, local_ref
):
    lam = lam_of(lam_ref)
    cum_col = cum_columns(lam)
    lam_col = columns(lam)
    select = turned_select(sel_ref)
    local_scan(value_ref, select, lam, cum_col, lam_col, skip_ref, local_ref, True)
    carried = carried_of(placed(select, 0, 1), got_ref[...])
    carried = carried * spread_heads(ending_of(cum_col, lam_col))
    scanned = (local_ref[...] + carried).astype(BF16)
    out_ref[...] = gain_ref[...] * nt(scanned, win_ref[...])


def col_grad_kernel(got_ref, y_ref, scaled_ref, x_ref, message_ref):
    x = from_message(got_ref[...], column_target)
    x_ref[...] = x.astype(BF16)
    grad = input_gradient(x, y_ref[...].astype(F32), scaled_ref[...])
    message_ref[...] = to_message(grad, column_target)


def col_value_kernel(
    x_ref, sel_ref, lam_ref, gain_ref, win_ref, rlam_ref, value_ref, part_ref, ropening_ref
):
    value = nn(normalized(x_ref[...].astype(F32), gain_ref[...]), win_ref[...]).astype(BF16)
    value_ref[...] = value
    lam = lam_of(lam_ref)
    ending = spread_heads(ending_of(cum_columns(lam), columns(lam)))
    weighted = (value.astype(F32) * ending).astype(BF16)
    part_ref[...] = state_rows(weighted, turned_select(sel_ref), 0, 1)
    ropening_ref[...] = opening_of(cum_columns(lam_of(rlam_ref)))


def row_pull_kernel(
    got_ref, sel_ref, opening_ref, wout_ref, part_ref, y_ref, pulled_ref, message_ref
):
    y = from_message(got_ref[...], row_target).astype(BF16)
    y_ref[...] = y
    pulled = nt(y, wout_ref[...]).astype(BF16)
    pulled_ref[...] = pulled
    weighted = (pulled.astype(F32) * spread_heads(opening_ref[...])).astype(BF16)
    second = state_rows(weighted, turned_select(sel_ref), STATE, 0)
    message_ref[...] = (part_ref[...] + second).astype(BF16)


def last_scan_kernel(
    value_ref, sel_ref, lam_ref, skip_ref, gain_ref, local_ref, placed_ref, factor_ref, kept_ref,
    *, backward, offset, stream,
):
    kept_ref[...] = gain_ref[...]
    lam = lam_of(lam_ref)
    select = turned_select(sel_ref)
    placed_ref[...] = placed(select, offset, stream)
    cum_col = cum_columns(lam)
    lam_col = columns(lam) if backward else None
    factor_ref[...] = ending_of(cum_col, lam_col) if backward else opening_of(cum_col)
    local_scan(value_ref, select, lam, cum_col, lam_col, skip_ref, local_ref, backward)


def end_kernel(
    got_ref, cplaced_ref, cfactor_ref, clocal_ref, cwout_ref,
    rplaced_ref, rfactor_ref, rlocal_ref, rwin_ref, gain_ref,
    cx_hbm, x_hbm, y_hbm,
    mixed_hbm, grad_hbm, cx_ref, x_ref, y_ref, mixed_ref, grad_ref, sem,
):
    def copy(a, b, i):
        return pltpu.make_async_copy(a, b, sem.at[i])

    x_in, y_in, cx_in = copy(x_hbm, x_ref, 0), copy(y_hbm, y_ref, 1), copy(cx_hbm, cx_ref, 2)
    for one in (x_in, y_in, cx_in):
        one.start()
    got = got_ref[...]
    carried = carried_of(rplaced_ref[...], got) * spread_heads(rfactor_ref[...])
    scanned = (rlocal_ref[...] + carried).astype(BF16)
    scaled = gain_ref[...] * nt(scanned, rwin_ref[...])
    x_in.wait()
    y_in.wait()
    grad_ref[...] = input_gradient(x_ref[...].astype(F32), y_ref[...].astype(F32), scaled)
    grad_out = copy(grad_ref, grad_hbm, 3)
    grad_out.start()
    carried = carried_of(cplaced_ref[...], got) * spread_heads(cfactor_ref[...])
    scanned = (clocal_ref[...] + carried).astype(BF16)
    cx_in.wait()
    mixed_ref[...] = (cx_ref[...].astype(F32) + nn(scanned, cwout_ref[...])).astype(BF16)
    mixed_out = copy(mixed_ref, mixed_hbm, 4)
    mixed_out.start()
    grad_out.wait()
    mixed_out.wait()


VM = pl.BlockSpec(memory_space=pltpu.VMEM)
SM = pl.BlockSpec(memory_space=pltpu.SMEM)
ANY = pl.BlockSpec(memory_space=pl.ANY)


class Near(tuple):
    pass


class Far(tuple):
    pass


def shaped(out):
    if isinstance(out, Near):
        return pltpu.VMEM(*out)
    if isinstance(out, Far):
        return pltpu.HBM(*out)
    return jax.ShapeDtypeStruct(*out)


def near(array):
    return pltpu.with_memory_space_constraint(array, pltpu.VMEM)


def far(array):
    return pltpu.with_memory_space_constraint(array, pltpu.HBM)


def call(kernel, name, outs, args, scalars=(), left=(), kept=(), scratch=(), flops=1e9):
    return pl.pallas_call(
        kernel,
        name=name,
        out_shape=[shaped(out) for out in outs],
        in_specs=[SM if i in scalars else ANY if i in left else VM for i in range(len(args))],
        out_specs=[ANY if i in kept else VM for i in range(len(outs))],
        scratch_shapes=list(scratch),
        compiler_params=pltpu.CompilerParams(vmem_limit_bytes=16 << 20),
        cost_estimate=pl.CostEstimate(flops=int(flops), bytes_accessed=1 << 20, transcendentals=0),
    )(*args)


TOKS = (TOK, WIDTH)
MSG = (LINES, HALF)
LOGGED = (LINES, HALF + LOGS)
PAIR = (TOK, 2 * LINES)
BIG = (2 * TOK, HALF)
FACTOR = (TOK, HEADS)
SEL = (2, 2 * STATE, 128)
LAM = (HEADS, 2, 128)


def swapped(array, axes):
    count = 1
    for axis in axes:
        count *= lax.axis_size(axis)
    split = array.reshape(count, array.shape[0] // count, array.shape[1])
    return lax.all_to_all(split, axes, split_axis=0, concat_axis=0, tiled=True).reshape(array.shape)


def body(
    tokens, row_select, row_decay, row_gain, row_skip, row_in, row_out,
    col_select, col_decay, col_gain, col_skip, col_in, col_out, cotangent,
):
    mine = (lax.axis_index("frame") * lax.axis_size("seq_0") + lax.axis_index("seq_0")).reshape(1)
    x = tokens.reshape(TOKS)
    y = cotangent.reshape(TOKS)
    rsel = row_select.reshape(2, 128, 2 * STATE).swapaxes(1, 2)
    csel = col_select.reshape(2, 128, 2 * STATE).swapaxes(1, 2)
    rlam = row_decay.reshape(HEADS, 2, 128)
    clam = col_decay.reshape(HEADS, 2, 128)
    rgain = row_gain.reshape(1, WIDTH)
    cgain = col_gain.reshape(1, WIDTH)
    rskip = row_skip.reshape(1, HEADS)
    cskip = col_skip.reshape(1, HEADS)

    rvalue, cpulled, message = call(
        start_kernel, "start", [Far((TOKS, BF16)), Far((TOKS, BF16)), Near((LOGGED, BF16))],
        [far(a) for a in (x, rsel, rlam, rgain, row_in, y, csel, clam, col_out)],
        left=range(9), kept=(0, 1),
        scratch=[
            pltpu.VMEM(TOKS, BF16), pltpu.VMEM(SEL, BF16), pltpu.VMEM(LAM, F32),
            pltpu.VMEM((1, WIDTH), F32), pltpu.VMEM((WIDTH, WIDTH), BF16),
            pltpu.VMEM(TOKS, BF16), pltpu.VMEM(SEL, BF16), pltpu.VMEM(LAM, F32),
            pltpu.VMEM((WIDTH, WIDTH), BF16), pltpu.VMEM(TOKS, BF16), pltpu.VMEM(TOKS, BF16),
            pltpu.SemaphoreType.DMA((11,)),
        ],
    )
    message, mine = lax.optimization_barrier((message, mine))
    got = swapped(message, INNER)
    before, decay, through, later, total = call(
        inner_first_kernel, "inner_first",
        [Near((MSG, F32)), Far((MSG, F32)), Near((MSG, F32)), Far((MSG, F32)), Near((LOGGED, BF16))],
        [near(got)], flops=1e7,
    )
    groups = swapped(total, OUTER)
    outer_decay, down = call(
        outer_first_kernel, "outer_first", [Far((MSG, F32)), Near((MSG, BF16))],
        [mine, near(groups), before, through], (0,), flops=1e7,
    )
    got = near(swapped(down, INNER))
    rlocal, ropening, rplaced = call(
        row_scan_kernel, "row_scan", [Near((TOKS, F32)), Near((FACTOR, F32)), Near((PAIR, BF16))],
        [far(rvalue), far(rsel), far(rlam), far(rskip)],
    )
    (sending,) = call(
        row_finish_kernel, "row_finish", [Near((BIG, BF16))],
        [near(x), rlocal, ropening, rplaced, got, near(row_out)],
    )
    arrived = swapped(sending, SEQ)
    (scaled,) = call(
        col_back_kernel, "col_back", [Near((TOKS, F32))],
        [far(cpulled), far(csel), far(clam), far(cskip), got, far(col_in), far(cgain)],
        scratch=[pltpu.VMEM(TOKS, F32)],
    )
    cx, returning = call(
        col_grad_kernel, "col_grad", [Far((TOKS, BF16)), Near((BIG, BF16))],
        [near(arrived), near(y), scaled],
    )
    landed = swapped(returning, SEQ)
    cvalue, part, ropening = call(
        col_value_kernel, "col_value",
        [Far((TOKS, BF16)), Near((MSG, F32)), Near((FACTOR, F32))],
        [far(cx), far(csel), far(clam), far(cgain), far(col_in), far(rlam)],
    )
    ry, rpulled, message = call(
        row_pull_kernel, "row_pull", [Far((TOKS, BF16)), Far((TOKS, BF16)), Near((MSG, BF16))],
        [near(landed), near(rsel), ropening, near(row_out), part],
    )
    got = swapped(message, INNER)
    before, total = call(
        inner_second_kernel, "inner_second", [Near((MSG, F32)), Near((MSG, BF16))],
        [near(got), near(decay)], flops=1e7,
    )
    groups = swapped(total, OUTER)
    (down,) = call(
        outer_second_kernel, "outer_second", [Near((MSG, BF16))],
        [mine, near(groups), before, near(later), near(outer_decay)], (0,), flops=1e7,
    )
    got = swapped(down, INNER)
    clocal, cplaced, cfactor, _ = call(
        partial(last_scan_kernel, backward=False, offset=STATE, stream=1), "col_scan",
        [Near((TOKS, F32)), Near((PAIR, BF16)), Near((FACTOR, F32)), Near(((1, WIDTH), F32))],
        [far(cvalue), far(csel), far(clam), far(cskip), far(cgain)],
    )
    rlocal, rplaced, rfactor, gain = call(
        partial(last_scan_kernel, backward=True, offset=0, stream=0), "row_scan_back",
        [Near((TOKS, F32)), Near((PAIR, BF16)), Near((FACTOR, F32)), Near(((1, WIDTH), F32))],
        [far(rpulled), far(rsel), far(rlam), far(rskip), far(rgain)],
    )
    mixed, grad = call(
        end_kernel, "end", [Far((TOKS, BF16)), Far((TOKS, BF16))],
        [near(got), cplaced, cfactor, clocal, near(col_out), rplaced, rfactor, rlocal,
         near(row_in), gain, far(cx), far(x), far(ry)],
        left=(10, 11, 12), kept=(0, 1),
        scratch=[pltpu.VMEM(TOKS, BF16)] * 5 + [pltpu.SemaphoreType.DMA((5,))],
    )
    return mixed.reshape(cotangent.shape), grad.reshape(tokens.shape)


def solution(mesh):
    torus = Mesh(
        mesh.devices.reshape(4, 8, 2, mesh.shape["frame"]), ("seq_0", "seq_1", "seq_2", "frame")
    )
    tall = P("frame", SEQ, None, None)
    flat = P("frame", None, SEQ, None)
    in_specs = (tall, tall, flat, P(), P(), P(), P(), tall, flat, P(), P(), P(), P(), tall)
    return jax.shard_map(
        body, mesh=torus, in_specs=in_specs, out_specs=(tall, tall), check_vma=False
    )
```

```python
from functools import partial

import jax
import jax.numpy as jnp
from jax import lax
from jax.experimental import pallas as pl
from jax.experimental.pallas import tpu as pltpu
from jax.sharding import Mesh
from jax.sharding import PartitionSpec as P

SEQ = ("seq_0", "seq_1", "seq_2")
INNER = ("seq_2", "seq_1")
OUTER = ("seq_0", "frame")

EPSILON = 1e-05
LOG2E = 1.4426950408889634

TOK = 256
WIDTH = 512
HEADS = 8
PART = 64
STATE = 32
GROUP = 16
HALF = 256
LINES = GROUP * 8
LOGS = 128

F32 = jnp.float32
BF16 = jnp.bfloat16


def iota(shape, axis):
    return lax.broadcasted_iota(jnp.int32, shape, axis)


def onehot(mask):
    return mask.astype(F32).astype(BF16)


def dot(left, right, left_axis, right_axis):
    return lax.dot_general(
        left, right, (((left_axis,), (right_axis,)), ((), ())), preferred_element_type=F32
    )


def nn(left, right):
    return dot(left, right, 1, 0)


def nt(left, right):
    return dot(left, right, 1, 1)


def tn(left, right):
    return dot(left, right, 0, 0)


def parts_of(values, count):
    out = []
    rest = values
    for _ in range(count):
        piece = rest.astype(BF16)
        out.append(piece)
        rest = rest - piece.astype(F32)
    return out


def one_minus_exp(v):
    series = 1.0 - v * (1.0 / 9.0)
    for k in range(8, 1, -1):
        series = 1.0 - v * (1.0 / k) * series
    return jnp.where(v < 0.5, v * series, 1.0 - jnp.exp(-v))


def lam_of(lam_ref):
    return jnp.concatenate([lam_ref[:, 0, :], lam_ref[:, 1, :]], axis=1)


def turned_select(select_ref):
    return jnp.concatenate([select_ref[0], select_ref[1]], axis=1)


def triangle():
    return onehot(iota((TOK, TOK), 1) <= iota((TOK, TOK), 0))


def cum_columns(lam):
    upto = triangle()
    return sum(nt(upto, p) for p in reversed(parts_of(lam, 3)))


def cum_rows(lam):
    upto = triangle()
    return sum(nt(p, upto) for p in reversed(parts_of(lam, 3)))


def columns(lam):
    same = onehot(iota((TOK, TOK), 1) == iota((TOK, TOK), 0))
    return sum(nt(same, p) for p in reversed(parts_of(lam, 3)))


def spread_heads(values):
    spread = onehot(iota((HEADS, WIDTH), 1) // PART == iota((HEADS, WIDTH), 0))
    return sum(nn(p, spread) for p in reversed(parts_of(values, 2)))


def opening_of(cum_col):
    return jnp.exp(cum_col)


def ending_of(cum_col, lam_col):
    last = cum_col[TOK - 1 : TOK, :]
    return jnp.exp(last - cum_col) * jnp.sqrt(one_minus_exp(-2.0 * lam_col))


def placed(select, offset, stream):
    at = iota((2 * STATE, 2 * LINES), 0)
    col = iota((2 * STATE, 2 * LINES), 1)
    row = col % LINES
    hit = (at == offset + 2 * (row // 8) + row % 2) & (row % 8 // 2 == col // LINES * 2 + stream)
    return tn(select, onehot(hit)).astype(BF16)


def carried_of(placed_pair, got):
    return jnp.concatenate(
        [nn(placed_pair[:, half * LINES : (half + 1) * LINES], got) for half in (0, 1)], axis=1
    )


def state_rows(weighted, select, offset, stream):
    at = iota((LINES, 2 * STATE), 1)
    row = iota((LINES, 2 * STATE), 0)
    out = None
    for half in (0, 1):
        hit = (at == offset + 2 * (row // 8) + row % 2) & (row % 8 // 2 == half * 2 + stream)
        rows = nn(onehot(hit), select).astype(BF16)
        part = nn(rows, weighted[:, half * HALF : (half + 1) * HALF])
        out = part if out is None else out + part
    return out


def normalized(x, gain):
    factor = lax.rsqrt(jnp.mean(x * x, axis=-1, keepdims=True) + EPSILON)
    return (x * factor * gain).astype(BF16)


def input_gradient(x, y, scaled):
    factor = lax.rsqrt(jnp.mean(x * x, axis=-1, keepdims=True) + EPSILON)
    inner = jnp.mean(scaled * x, axis=-1, keepdims=True)
    return (y + factor * scaled - x * (factor * factor * factor) * inner).astype(BF16)


def local_scan(values_ref, select, lam, cum_col, lam_col, skip_ref, out_ref, backward):
    cum_row = cum_rows(lam)
    source = select[:STATE]
    target = select[STATE:]
    if backward:
        affinity = tn(source, target)
        left = 0.5 * jnp.log2(one_minus_exp(-2.0 * lam_col)) - cum_col * LOG2E
        right = cum_row * LOG2E
    else:
        affinity = tn(target, source)
        left = cum_col * LOG2E
        right = 0.5 * jnp.log2(one_minus_exp(-2.0 * lam)) - cum_row * LOG2E
    first = iota((128, 128), 0)
    second = iota((128, 128), 1)
    keep = second >= first if backward else second <= first
    lo, hi = slice(0, 128), slice(128, 256)
    for h in range(HEADS):
        span = slice(h * PART, (h + 1) * PART)
        lc = left[:, h : h + 1]
        rr = right[h : h + 1, :]

        def tile(a, b, masked):
            m = jnp.exp2(lc[a] + rr[:, b]) * affinity[a, b]
            return (jnp.where(keep, m, 0.0) if masked else m).astype(BF16)

        v_lo = values_ref[lo, span]
        v_hi = values_ref[hi, span]
        skip = skip_ref[0:1, h : h + 1]
        if backward:
            top = nn(tile(lo, lo, True), v_lo) + nn(tile(lo, hi, False), v_hi)
            low = nn(tile(hi, hi, True), v_hi)
        else:
            top = nn(tile(lo, lo, True), v_lo)
            low = nn(tile(hi, lo, False), v_lo) + nn(tile(hi, hi, True), v_hi)
        out_ref[lo, span] = top + skip * v_lo.astype(F32)
        out_ref[hi, span] = low + skip * v_hi.astype(F32)


def row_target(token):
    column = token % 128
    return column // 2 * 8 + column % 2 * 2 + token // 128


def column_target(token):
    row = token % 128
    return row // 2 * 8 + token // 128 * 2 + row % 2


def to_message(tokens, target):
    off = iota((2 * TOK, TOK), 0) - target(iota((1, TOK), 1))
    left = nn(onehot(off == 0), tokens[:, :HALF])
    return (left + nn(onehot(off == 4), tokens[:, HALF:])).astype(BF16)


def from_message(message, target):
    off = iota((TOK, 2 * TOK), 1) - target(iota((TOK, 1), 0))
    return jnp.concatenate([nn(onehot(off == 0), message), nn(onehot(off == 4), message)], axis=1)


def start_kernel(
    x_hbm, rsel_hbm, rlam_hbm, rskip_hbm, gain_hbm, win_hbm,
    y_hbm, csel_hbm, clam_hbm, cskip_hbm, wout_hbm,
    rlocal_ref, rfactor_ref, rplaced_ref, clocal_ref, cfactor_ref, cplaced_ref, sent_hbm,
    message_ref,
    x_ref, rsel_ref, rlam_ref, rskip_ref, gain_ref, win_ref,
    y_ref, csel_ref, clam_ref, cskip_ref, wout_ref, value_ref, pulled_ref, sent_ref, sem,
):
    pairs = (
        (rlam_hbm, rlam_ref), (clam_hbm, clam_ref), (rsel_hbm, rsel_ref), (csel_hbm, csel_ref),
        (rskip_hbm, rskip_ref), (cskip_hbm, cskip_ref), (gain_hbm, gain_ref), (x_hbm, x_ref),
        (win_hbm, win_ref), (y_hbm, y_ref), (wout_hbm, wout_ref), (sent_ref, sent_hbm),
    )
    copies = [pltpu.make_async_copy(a, b, sem.at[i]) for i, (a, b) in enumerate(pairs)]
    for copy in copies[:11]:
        copy.start()
    for copy in copies[:7]:
        copy.wait()
    rlam = lam_of(rlam_ref)
    rcum = cum_columns(rlam)
    rsel = turned_select(rsel_ref)
    ending = spread_heads(ending_of(rcum, columns(rlam)))
    clam = lam_of(clam_ref)
    ccum = cum_columns(clam)
    clam_col = columns(clam)
    csel = turned_select(csel_ref)
    row = iota((8, HEADS), 0)
    head = iota((8, HEADS), 1)
    logs = jnp.where(row % 4 < 2, rcum[TOK - 1 : TOK, :], ccum[TOK - 1 : TOK, :])
    logs = jnp.where(head // 4 == row // 4, logs, 0.0)
    tile = None
    for k, piece in enumerate(parts_of(logs, 3)):
        place = onehot(iota((HEADS, LOGS), 1) == 4 * k + iota((HEADS, LOGS), 0) % 4)
        part = nn(piece, place)
        tile = part if tile is None else tile + part
    tile = tile.astype(BF16)
    for j in range(GROUP):
        message_ref[j * 8 : (j + 1) * 8, HALF:] = tile
    rfactor_ref[...] = opening_of(rcum)
    cfactor_ref[...] = ending_of(ccum, clam_col)
    rplaced_ref[...] = placed(rsel, STATE, 0)
    cplaced_ref[...] = placed(csel, 0, 1)
    copies[7].wait()
    normed = normalized(x_ref[...].astype(F32), gain_ref[...])
    copies[8].wait()
    value = nn(normed, win_ref[...]).astype(BF16)
    value_ref[...] = value
    weighted = (value.astype(F32) * ending).astype(BF16)
    first = state_rows(weighted, rsel, 0, 0)
    copies[9].wait()
    sent_ref[...] = to_message(y_ref[...], column_target)
    copies[11].start()
    local_scan(value_ref, rsel, rlam, rcum, None, rskip_ref, rlocal_ref, False)
    copies[10].wait()
    pulled = nt(y_ref[...], wout_ref[...]).astype(BF16)
    pulled_ref[...] = pulled
    weighted = (pulled.astype(F32) * spread_heads(opening_of(ccum))).astype(BF16)
    second = state_rows(weighted, csel, STATE, 1)
    message_ref[:, :HALF] = (first + second).astype(BF16)
    local_scan(pulled_ref, csel, clam, ccum, clam_col, cskip_ref, clocal_ref, True)
    copies[11].wait()


def logs_spread(tiles):
    spread = onehot(
        (iota((LOGS, HALF), 0) % 4 == iota((LOGS, HALF), 1) // PART) & (iota((LOGS, HALF), 0) < 12)
    )
    return nn(tiles, spread)


def inner_order(j):
    return j % 2 * 8 + j // 2


def outer_order(j):
    return j % 4 * 4 + j // 4


def tile_at(j):
    return slice(j * 8, (j + 1) * 8)


def stream_mask():
    return iota((8, HALF), 0) % 4 < 2


def pick(a_forward, forward, backward):
    first = stream_mask()
    return jnp.where(first, forward, backward) if a_forward else jnp.where(first, backward, forward)


def inner_scan(tile, decay, a_forward, before_ref):
    spots = [inner_order(j) for j in range(GROUP)]
    state = jnp.zeros((8, HALF), F32)
    forward = {}
    for j in spots:
        forward[j] = state
        state = decay(j) * state + tile(j)
    ahead = state
    state = jnp.zeros((8, HALF), F32)
    for j in reversed(spots):
        before_ref[tile_at(j), :] = pick(a_forward, forward[j], state)
        state = decay(j) * state + tile(j)
    return pick(a_forward, ahead, state).astype(BF16)


def inner_first_kernel(got_ref, before_ref, decay_ref, through_ref, later_ref, total_ref):
    logs = logs_spread(got_ref[:, HALF:])
    decay_ref[...] = jnp.exp(logs)
    total = inner_scan(
        lambda j: got_ref[tile_at(j), :HALF].astype(F32),
        lambda j: decay_ref[tile_at(j), :], True, before_ref,
    )
    compact = jnp.zeros((8, LOGS), F32)
    for j in range(GROUP):
        compact = compact + got_ref[tile_at(j), HALF:].astype(F32)
    compact = compact + pltpu.roll(compact, LOGS - 4, 1) + pltpu.roll(compact, LOGS - 8, 1)
    compact = jnp.where(iota((8, LOGS), 1) < 4, compact, 0.0)
    high = compact.astype(BF16).astype(F32)
    middle = (compact - high).astype(BF16).astype(F32)
    low = compact - high - middle
    compact = (high + pltpu.roll(middle, 4, 1) + pltpu.roll(low, 8, 1)).astype(BF16)
    for j in range(GROUP):
        total_ref[tile_at(j), :HALF] = total
        total_ref[tile_at(j), HALF:] = compact
    spots = [inner_order(j) for j in range(GROUP)]
    gone = jnp.zeros((8, HALF), F32)
    earlier = {}
    for j in spots:
        earlier[j] = gone
        gone = gone + logs[tile_at(j), :]
    gone = jnp.zeros((8, HALF), F32)
    for j in reversed(spots):
        ahead, behind = jnp.exp(earlier[j]), jnp.exp(gone)
        through_ref[tile_at(j), :] = pick(True, ahead, behind)
        later_ref[tile_at(j), :] = pick(False, ahead, behind)
        gone = gone + logs[tile_at(j), :]


def inner_second_kernel(got_ref, decay_ref, before_ref, total_ref):
    total = inner_scan(
        lambda j: got_ref[tile_at(j), :].astype(F32),
        lambda j: decay_ref[tile_at(j), :], False, before_ref,
    )
    for j in range(GROUP):
        total_ref[tile_at(j), :] = total


def outer_scan(mine, tile, decay, a_forward, before_ref, through_ref, out_ref):
    state = jnp.zeros((8, HALF), F32)
    for j in range(GROUP):
        at = outer_order(j)
        state = jnp.where(j < mine, decay(at) * state + tile(at), state)
    ahead = state
    state = jnp.zeros((8, HALF), F32)
    for j in reversed(range(GROUP)):
        at = outer_order(j)
        state = jnp.where(j > mine, decay(at) * state + tile(at), state)
    both = pick(a_forward, ahead, state)
    for j in range(GROUP):
        at = tile_at(j)
        out_ref[at, :] = (through_ref[at, :] * both + before_ref[at, :]).astype(BF16)


def outer_first_kernel(mine_ref, got_ref, before_ref, through_ref, decay_ref, out_ref):
    decay_ref[...] = jnp.exp(logs_spread(got_ref[:, HALF:]))
    outer_scan(
        mine_ref[0], lambda j: got_ref[tile_at(j), :HALF].astype(F32),
        lambda j: decay_ref[tile_at(j), :], True, before_ref, through_ref, out_ref,
    )


def outer_second_kernel(mine_ref, got_ref, before_ref, through_ref, decay_ref, out_ref):
    outer_scan(
        mine_ref[0], lambda j: got_ref[tile_at(j), :].astype(F32),
        lambda j: decay_ref[tile_at(j), :], False, before_ref, through_ref, out_ref,
    )


def finish_kernel(
    rlocal_ref, rfactor_ref, rplaced_ref, got_ref, wout_ref,
    clocal_ref, cfactor_ref, cplaced_ref, win_ref, gain_hbm, x_hbm, sent_hbm,
    mixed_ref, message_ref, gain_ref, x_ref, sem,
):
    copies = [
        pltpu.make_async_copy(x_hbm, x_ref, sem.at[0]),
        pltpu.make_async_copy(gain_hbm, gain_ref, sem.at[1]),
        pltpu.make_async_copy(sent_hbm, message_ref.at[:, HALF : 2 * HALF], sem.at[2]),
    ]
    for copy in copies:
        copy.start()
    got = got_ref[...]
    carried = carried_of(rplaced_ref[...], got) * spread_heads(rfactor_ref[...])
    scanned = (rlocal_ref[...] + carried).astype(BF16)
    total = nn(scanned, wout_ref[...])
    carried = carried_of(cplaced_ref[...], got) * spread_heads(cfactor_ref[...])
    scanned = (clocal_ref[...] + carried).astype(BF16)
    returned = nt(scanned, win_ref[...])
    copies[0].wait()
    mixed = (x_ref[...].astype(F32) + total).astype(BF16)
    mixed_ref[...] = mixed
    message_ref[:, :HALF] = to_message(mixed, row_target)
    copies[1].wait()
    scaled = (gain_ref[...] * returned).astype(BF16)
    message_ref[:, 2 * HALF :] = to_message(scaled, column_target)
    copies[2].wait()


def cross_kernel(
    got_ref, mixed_ref, rsel_ref, rfactor_ref, wout_ref, csel_ref, cfactor_ref, gain_ref, win_ref,
    cx_ref, cvalue_ref, y_ref, pulled_ref, message_ref,
):
    y = from_message(got_ref[:, HALF : 2 * HALF], row_target)
    scaled = from_message(got_ref[:, 2 * HALF :], row_target)
    y = input_gradient(mixed_ref[...].astype(F32), y, scaled)
    y_ref[...] = y
    pulled = nt(y, wout_ref[...]).astype(BF16)
    pulled_ref[...] = pulled
    weighted = (pulled.astype(F32) * spread_heads(rfactor_ref[...])).astype(BF16)
    first = state_rows(weighted, turned_select(rsel_ref), STATE, 0)
    x = from_message(got_ref[:, :HALF], column_target)
    cx_ref[...] = x.astype(BF16)
    value = nn(normalized(x, gain_ref[...]), win_ref[...]).astype(BF16)
    cvalue_ref[...] = value
    weighted = (value.astype(F32) * spread_heads(cfactor_ref[...])).astype(BF16)
    second = state_rows(weighted, turned_select(csel_ref), 0, 1)
    message_ref[...] = (first + second).astype(BF16)


def col_scan_kernel(
    value_ref, sel_ref, lam_ref, skip_ref, x_ref, local_ref, placed_ref, factor_ref, kept_ref
):
    kept_ref[...] = x_ref[...]
    lam = lam_of(lam_ref)
    select = turned_select(sel_ref)
    placed_ref[...] = placed(select, STATE, 1)
    cum_col = cum_columns(lam)
    factor_ref[...] = opening_of(cum_col)
    local_scan(value_ref, select, lam, cum_col, None, skip_ref, local_ref, False)


def row_scan_back_kernel(
    value_ref, sel_ref, lam_ref, skip_ref, gain_ref, local_ref, placed_ref, factor_ref, kept_ref
):
    kept_ref[...] = gain_ref[...]
    lam = lam_of(lam_ref)
    select = turned_select(sel_ref)
    placed_ref[...] = placed(select, 0, 0)
    cum_col = cum_columns(lam)
    lam_col = columns(lam)
    factor_ref[...] = ending_of(cum_col, lam_col)
    local_scan(value_ref, select, lam, cum_col, lam_col, skip_ref, local_ref, True)


def end_kernel(
    got_ref, cplaced_ref, cfactor_ref, clocal_ref, rplaced_ref, rfactor_ref, rlocal_ref, rwin_ref,
    gain_ref, x_ref, y_ref, cx_hbm, cwout_hbm,
    mixed_hbm, grad_hbm, cx_ref, cwout_ref, mixed_ref, grad_ref, sem,
):
    def copy(a, b, i):
        return pltpu.make_async_copy(a, b, sem.at[i])

    cwout_in, cx_in = copy(cwout_hbm, cwout_ref, 0), copy(cx_hbm, cx_ref, 1)
    cwout_in.start()
    cx_in.start()
    got = got_ref[...]
    carried = carried_of(rplaced_ref[...], got) * spread_heads(rfactor_ref[...])
    scanned = (rlocal_ref[...] + carried).astype(BF16)
    scaled = gain_ref[...] * nt(scanned, rwin_ref[...])
    grad_ref[...] = input_gradient(x_ref[...].astype(F32), y_ref[...].astype(F32), scaled)
    grad_out = copy(grad_ref, grad_hbm, 2)
    grad_out.start()
    carried = carried_of(cplaced_ref[...], got) * spread_heads(cfactor_ref[...])
    scanned = (clocal_ref[...] + carried).astype(BF16)
    cwout_in.wait()
    cx_in.wait()
    outs = [copy(mixed_ref.at[rows], mixed_hbm.at[rows], 3 + k) for k, rows in enumerate(QUARTERS)]
    for rows, out in zip(QUARTERS, outs):
        mixed = cx_ref[rows, :].astype(F32) + nn(scanned[rows, :], cwout_ref[...])
        mixed_ref[rows, :] = mixed.astype(BF16)
        out.start()
    grad_out.wait()
    for out in outs:
        out.wait()


QUARTERS = [slice(k * 64, (k + 1) * 64) for k in range(4)]

VM = pl.BlockSpec(memory_space=pltpu.VMEM)
SM = pl.BlockSpec(memory_space=pltpu.SMEM)
ANY = pl.BlockSpec(memory_space=pl.ANY)


class Near(tuple):
    pass


class Far(tuple):
    pass


def shaped(out):
    if isinstance(out, Near):
        return pltpu.VMEM(*out)
    if isinstance(out, Far):
        return pltpu.HBM(*out)
    return jax.ShapeDtypeStruct(*out)


def near(array):
    return pltpu.with_memory_space_constraint(array, pltpu.VMEM)


def far(array):
    return pltpu.with_memory_space_constraint(array, pltpu.HBM)


def call(kernel, name, outs, args, scalars=(), left=(), kept=(), scratch=(), flops=1e9):
    return pl.pallas_call(
        kernel,
        name=name,
        out_shape=[shaped(out) for out in outs],
        in_specs=[SM if i in scalars else ANY if i in left else VM for i in range(len(args))],
        out_specs=[ANY if i in kept else VM for i in range(len(outs))],
        scratch_shapes=list(scratch),
        compiler_params=pltpu.CompilerParams(vmem_limit_bytes=16 << 20),
        cost_estimate=pl.CostEstimate(flops=int(flops), bytes_accessed=1 << 20, transcendentals=0),
    )(*args)


TOKS = (TOK, WIDTH)
MSG = (LINES, HALF)
LOGGED = (LINES, HALF + LOGS)
PAIR = (TOK, 2 * LINES)
BIG = (2 * TOK, HALF)
WIDE = (2 * TOK, 3 * HALF)
FACTOR = (TOK, HEADS)
SEL = (2, 2 * STATE, 128)
LAM = (HEADS, 2, 128)


def swapped(array, axes):
    count = 1
    for axis in axes:
        count *= lax.axis_size(axis)
    split = array.reshape(count, array.shape[0] // count, array.shape[1])
    return lax.all_to_all(split, axes, split_axis=0, concat_axis=0, tiled=True).reshape(array.shape)


def body(
    tokens, row_select, row_decay, row_gain, row_skip, row_in, row_out,
    col_select, col_decay, col_gain, col_skip, col_in, col_out, cotangent,
):
    mine = (lax.axis_index("frame") * lax.axis_size("seq_0") + lax.axis_index("seq_0")).reshape(1)
    x = tokens.reshape(TOKS)
    y = cotangent.reshape(TOKS)
    rsel = row_select.reshape(2, 128, 2 * STATE).swapaxes(1, 2)
    csel = col_select.reshape(2, 128, 2 * STATE).swapaxes(1, 2)
    rlam = row_decay.reshape(HEADS, 2, 128)
    clam = col_decay.reshape(HEADS, 2, 128)
    rgain = row_gain.reshape(1, WIDTH)
    cgain = col_gain.reshape(1, WIDTH)
    rskip = row_skip.reshape(1, HEADS)
    cskip = col_skip.reshape(1, HEADS)

    rlocal, rfactor, rplaced, clocal, cfactor, cplaced, sent, message = call(
        start_kernel, "start",
        [Near((TOKS, F32)), Near((FACTOR, F32)), Near((PAIR, BF16)),
         Near((TOKS, F32)), Near((FACTOR, F32)), Near((PAIR, BF16)), Far((BIG, BF16)),
         Near((LOGGED, BF16))],
        [far(a) for a in
         (x, rsel, rlam, rskip, rgain, row_in, y, csel, clam, cskip, col_out)],
        left=range(11), kept=(6,),
        scratch=[
            pltpu.VMEM(TOKS, BF16), pltpu.VMEM(SEL, BF16), pltpu.VMEM(LAM, F32),
            pltpu.VMEM((1, HEADS), F32), pltpu.VMEM((1, WIDTH), F32),
            pltpu.VMEM((WIDTH, WIDTH), BF16), pltpu.VMEM(TOKS, BF16), pltpu.VMEM(SEL, BF16),
            pltpu.VMEM(LAM, F32), pltpu.VMEM((1, HEADS), F32), pltpu.VMEM((WIDTH, WIDTH), BF16),
            pltpu.VMEM(TOKS, BF16), pltpu.VMEM(TOKS, BF16), pltpu.VMEM(BIG, BF16),
            pltpu.SemaphoreType.DMA((12,)),
        ],
    )
    message, mine = lax.optimization_barrier((message, mine))
    got = swapped(message, INNER)
    before, decay, through, later, total = call(
        inner_first_kernel, "inner_first",
        [Near((MSG, F32)), Far((MSG, F32)), Near((MSG, F32)), Far((MSG, F32)), Near((LOGGED, BF16))],
        [near(got)], flops=1e7,
    )
    groups = swapped(total, OUTER)
    outer_decay, down = call(
        outer_first_kernel, "outer_first", [Far((MSG, F32)), Near((MSG, BF16))],
        [mine, near(groups), before, through], (0,), flops=1e7,
    )
    got = near(swapped(down, INNER))
    rmixed, sending = call(
        finish_kernel, "finish", [Near((TOKS, BF16)), Near((WIDE, BF16))],
        [rlocal, rfactor, rplaced, got, near(row_out), clocal, cfactor, cplaced, near(col_in),
         far(cgain), far(x), far(sent)],
        left=(9, 10, 11),
        scratch=[
            pltpu.VMEM((1, WIDTH), F32), pltpu.VMEM(TOKS, BF16), pltpu.SemaphoreType.DMA((3,)),
        ],
    )
    arrived = swapped(sending, SEQ)
    cx, cvalue, ry, rpulled, message = call(
        cross_kernel, "cross",
        [Near((TOKS, BF16)), Near((TOKS, BF16)), Near((TOKS, BF16)), Near((TOKS, BF16)),
         Near((MSG, BF16))],
        [near(arrived), rmixed, near(rsel), rfactor, near(row_out), near(csel), cfactor,
         near(cgain), near(col_in)],
    )
    got = swapped(message, INNER)
    before, total = call(
        inner_second_kernel, "inner_second", [Near((MSG, F32)), Near((MSG, BF16))],
        [near(got), near(decay)], flops=1e7,
    )
    groups = swapped(total, OUTER)
    (down,) = call(
        outer_second_kernel, "outer_second", [Near((MSG, BF16))],
        [mine, near(groups), before, near(later), near(outer_decay)], (0,), flops=1e7,
    )
    got = swapped(down, INNER)
    clocal, cplaced, cfactor, cx = call(
        col_scan_kernel, "col_scan",
        [Near((TOKS, F32)), Near((PAIR, BF16)), Near((FACTOR, F32)), Far((TOKS, BF16))],
        [cvalue, far(csel), far(clam), far(cskip), cx],
    )
    rlocal, rplaced, rfactor, gain = call(
        row_scan_back_kernel, "row_scan_back",
        [Near((TOKS, F32)), Near((PAIR, BF16)), Near((FACTOR, F32)), Near(((1, WIDTH), F32))],
        [rpulled, far(rsel), far(rlam), far(rskip), far(rgain)],
    )
    mixed, grad = call(
        end_kernel, "end", [Far((TOKS, BF16)), Far((TOKS, BF16))],
        [near(got), cplaced, cfactor, clocal, rplaced, rfactor, rlocal, near(row_in),
         gain, near(x), ry, far(cx), far(col_out)],
        left=(11, 12), kept=(0, 1),
        scratch=[
            pltpu.VMEM(TOKS, BF16), pltpu.VMEM((WIDTH, WIDTH), BF16), pltpu.VMEM(TOKS, BF16),
            pltpu.VMEM(TOKS, BF16), pltpu.SemaphoreType.DMA((7,)),
        ],
    )
    return mixed.reshape(cotangent.shape), grad.reshape(tokens.shape)


def solution(mesh):
    torus = Mesh(
        mesh.devices.reshape(4, 8, 2, mesh.shape["frame"]), ("seq_0", "seq_1", "seq_2", "frame")
    )
    tall = P("frame", SEQ, None, None)
    flat = P("frame", None, SEQ, None)
    in_specs = (tall, tall, flat, P(), P(), P(), P(), tall, flat, P(), P(), P(), P(), tall)
    return jax.shard_map(
        body, mesh=torus, in_specs=in_specs, out_specs=(tall, tall), check_vma=False
    )
```

```python
from functools import partial

import jax
import jax.numpy as jnp
from jax import lax
from jax.experimental import pallas as pl
from jax.experimental.pallas import tpu as pltpu
from jax.sharding import Mesh
from jax.sharding import PartitionSpec as P

SEQ = ("seq_0", "seq_1", "seq_2")
INNER = ("seq_2", "seq_1")
OUTER = ("seq_0", "frame")

EPSILON = 1e-05
LOG2E = 1.4426950408889634

TOK = 256
WIDTH = 512
HEADS = 8
PART = 64
STATE = 32
GROUP = 16
HALF = 256
LINES = GROUP * 8
LOGS = 128

F32 = jnp.float32
BF16 = jnp.bfloat16


def iota(shape, axis):
    return lax.broadcasted_iota(jnp.int32, shape, axis)


def onehot(mask):
    return mask.astype(F32).astype(BF16)


def dot(left, right, left_axis, right_axis):
    return lax.dot_general(
        left, right, (((left_axis,), (right_axis,)), ((), ())), preferred_element_type=F32
    )


def nn(left, right):
    return dot(left, right, 1, 0)


def nt(left, right):
    return dot(left, right, 1, 1)


def tn(left, right):
    return dot(left, right, 0, 0)


def parts_of(values, count):
    out = []
    rest = values
    for _ in range(count):
        piece = rest.astype(BF16)
        out.append(piece)
        rest = rest - piece.astype(F32)
    return out


def one_minus_exp(v):
    series = 1.0 - v * (1.0 / 9.0)
    for k in range(8, 1, -1):
        series = 1.0 - v * (1.0 / k) * series
    return jnp.where(v < 0.5, v * series, 1.0 - jnp.exp(-v))


def lam_of(lam_ref):
    return jnp.concatenate([lam_ref[:, 0, :], lam_ref[:, 1, :]], axis=1)


def turned_select(select_ref):
    return jnp.concatenate([select_ref[0], select_ref[1]], axis=1)


def block_terms(lam):
    upto = onehot(iota((TOK, TOK), 1) <= iota((TOK, TOK), 0))
    stacked = nt(jnp.concatenate(parts_of(lam, 3), axis=0), upto)
    cum = stacked[:8] + stacked[8:16] + stacked[16:]
    square = one_minus_exp(-2.0 * lam)
    ending = jnp.exp(cum[:, TOK - 1 :] - cum) * jnp.sqrt(square)
    log_inward = jnp.maximum(0.5 * jnp.log2(square), -500.0)
    rows = jnp.concatenate([cum * LOG2E, log_inward - cum * LOG2E], axis=0)
    cols = jnp.concatenate([rows, jnp.exp(cum), ending], axis=0).T
    return cum, rows, cols


OPENING = 16
ENDING = 24


def spread_heads(cols, offset):
    spread = onehot(
        iota((4 * HEADS, WIDTH), 1) // PART + offset == iota((4 * HEADS, WIDTH), 0)
    )
    return sum(nn(p, spread) for p in reversed(parts_of(cols, 2)))


def placed(select, offset, stream):
    at = iota((2 * STATE, 2 * LINES), 0)
    col = iota((2 * STATE, 2 * LINES), 1)
    row = col % LINES
    hit = (at == offset + 2 * (row // 8) + row % 2) & (row % 8 // 2 == col // LINES * 2 + stream)
    return tn(select, onehot(hit)).astype(BF16)


def carried_of(placed_pair, got):
    return jnp.concatenate(
        [nn(placed_pair[:, half * LINES : (half + 1) * LINES], got) for half in (0, 1)], axis=1
    )


def state_rows(weighted, select, offset, stream):
    at = iota((LINES, 2 * STATE), 1)
    row = iota((LINES, 2 * STATE), 0)
    out = None
    for half in (0, 1):
        hit = (at == offset + 2 * (row // 8) + row % 2) & (row % 8 // 2 == half * 2 + stream)
        rows = nn(onehot(hit), select).astype(BF16)
        part = nn(rows, weighted[:, half * HALF : (half + 1) * HALF])
        out = part if out is None else out + part
    return out


def normalized(x, gain):
    factor = lax.rsqrt(jnp.mean(x * x, axis=-1, keepdims=True) + EPSILON)
    return (x * factor * gain).astype(BF16)


def input_gradient(x, y, scaled):
    factor = lax.rsqrt(jnp.mean(x * x, axis=-1, keepdims=True) + EPSILON)
    inner = jnp.mean(scaled * x, axis=-1, keepdims=True)
    return (y + factor * scaled - x * (factor * factor * factor) * inner).astype(BF16)


def local_scan(values_ref, select, rows, cols, skip_ref, out_ref, backward):
    source = select[:STATE]
    target = select[STATE:]
    if backward:
        affinity = tn(source, target)
        left, right = cols[:, HEADS : 2 * HEADS], rows[:HEADS]
    else:
        affinity = tn(target, source)
        left, right = cols[:, :HEADS], rows[HEADS : 2 * HEADS]
    first = iota((128, 128), 0)
    second = iota((128, 128), 1)
    keep = second >= first if backward else second <= first
    lower = iota((1, 2 * PART), 1) < PART
    lo, hi = slice(0, 128), slice(128, 256)

    def tile(h, a, b):
        m = jnp.exp2(left[a, h : h + 1] + right[h : h + 1, b]) * affinity[a, b]
        return (jnp.where(keep, m, 0.0) if a == b else m).astype(BF16)

    def mixed(pair, rows, sources, parts):
        tiles = [tile(h, rows, b) for h in pair for b in sources]
        values = [part[b] for part in parts for b in sources]
        return nn(jnp.concatenate(tiles, axis=1), jnp.concatenate(values, axis=0))

    for h in range(0, HEADS, 2):
        span = slice(h * PART, (h + 2) * PART)
        v = values_ref[:, span].astype(F32)
        parts = [jnp.where(lower, v, 0.0).astype(BF16), jnp.where(lower, 0.0, v).astype(BF16)]
        skip = jnp.where(lower, skip_ref[0:1, h : h + 1], skip_ref[0:1, h + 1 : h + 2])
        top = mixed((h, h + 1), lo, (lo, hi) if backward else (lo,), parts)
        low = mixed((h, h + 1), hi, (hi,) if backward else (lo, hi), parts)
        out_ref[lo, span] = top + skip * v[lo]
        out_ref[hi, span] = low + skip * v[hi]


def row_target(token):
    column = token % 128
    return column // 2 * 8 + column % 2 * 2 + token // 128


def column_target(token):
    row = token % 128
    return row // 2 * 8 + token // 128 * 2 + row % 2


def to_message(tokens, target):
    off = iota((2 * TOK, TOK), 0) - target(iota((1, TOK), 1))
    left = nn(onehot(off == 0), tokens[:, :HALF])
    return (left + nn(onehot(off == 4), tokens[:, HALF:])).astype(BF16)


def from_message(message, target):
    off = iota((TOK, 2 * TOK), 1) - target(iota((TOK, 1), 0))
    return jnp.concatenate([nn(onehot(off == 0), message), nn(onehot(off == 4), message)], axis=1)


def start_kernel(
    x_hbm, rsel_hbm, rlam_hbm, rskip_hbm, gain_hbm, win_hbm,
    y_hbm, csel_hbm, clam_hbm, cskip_hbm, wout_hbm,
    rlocal_ref, rcols_ref, rrows_ref, rplaced_ref, clocal_ref, ccols_ref, crows_ref, cplaced_ref,
    sent_hbm, message_ref,
    x_ref, rsel_ref, rlam_ref, rskip_ref, gain_ref, win_ref,
    y_ref, csel_ref, clam_ref, cskip_ref, wout_ref, value_ref, pulled_ref, sent_ref, sem,
):
    pairs = (
        (rlam_hbm, rlam_ref), (clam_hbm, clam_ref), (rsel_hbm, rsel_ref), (csel_hbm, csel_ref),
        (rskip_hbm, rskip_ref), (cskip_hbm, cskip_ref), (gain_hbm, gain_ref), (x_hbm, x_ref),
        (win_hbm, win_ref), (y_hbm, y_ref), (wout_hbm, wout_ref), (sent_ref, sent_hbm),
    )
    copies = [pltpu.make_async_copy(a, b, sem.at[i]) for i, (a, b) in enumerate(pairs)]
    for copy in copies[:11]:
        copy.start()
    for copy in copies[:7]:
        copy.wait()
    rcum, rrows, rcols = block_terms(lam_of(rlam_ref))
    ccum, crows, ccols = block_terms(lam_of(clam_ref))
    rrows_ref[...] = rrows
    rcols_ref[...] = rcols
    crows_ref[...] = crows
    ccols_ref[...] = ccols
    rsel = turned_select(rsel_ref)
    csel = turned_select(csel_ref)
    row = iota((8, HEADS), 0)
    head = iota((8, HEADS), 1)
    rlast = jnp.broadcast_to(rcum[:, TOK - 1 :], (HEADS, HEADS)).T
    clast = jnp.broadcast_to(ccum[:, TOK - 1 :], (HEADS, HEADS)).T
    logs = jnp.where(row % 4 < 2, rlast, clast)
    logs = jnp.where(head // 4 == row // 4, logs, 0.0)
    tile = None
    for k, piece in enumerate(parts_of(logs, 3)):
        place = onehot(iota((HEADS, LOGS), 1) == 4 * k + iota((HEADS, LOGS), 0) % 4)
        part = nn(piece, place)
        tile = part if tile is None else tile + part
    tile = tile.astype(BF16)
    for j in range(GROUP):
        message_ref[j * 8 : (j + 1) * 8, HALF:] = tile
    rplaced_ref[...] = placed(rsel, STATE, 0)
    cplaced_ref[...] = placed(csel, 0, 1)
    copies[7].wait()
    normed = normalized(x_ref[...].astype(F32), gain_ref[...])
    copies[8].wait()
    value = nn(normed, win_ref[...]).astype(BF16)
    value_ref[...] = value
    weighted = (value.astype(F32) * spread_heads(rcols, ENDING)).astype(BF16)
    first = state_rows(weighted, rsel, 0, 0)
    copies[9].wait()
    sent_ref[...] = to_message(y_ref[...], column_target)
    copies[11].start()
    local_scan(value_ref, rsel, rrows, rcols, rskip_ref, rlocal_ref, False)
    copies[10].wait()
    pulled = nt(y_ref[...], wout_ref[...]).astype(BF16)
    pulled_ref[...] = pulled
    weighted = (pulled.astype(F32) * spread_heads(ccols, OPENING)).astype(BF16)
    second = state_rows(weighted, csel, STATE, 1)
    message_ref[:, :HALF] = (first + second).astype(BF16)
    local_scan(pulled_ref, csel, crows, ccols, cskip_ref, clocal_ref, True)
    copies[11].wait()


def logs_spread(tiles):
    spread = onehot(
        (iota((LOGS, HALF), 0) % 4 == iota((LOGS, HALF), 1) // PART) & (iota((LOGS, HALF), 0) < 12)
    )
    return nn(tiles, spread)


def inner_order(j):
    return j % 2 * 8 + j // 2


def outer_order(j):
    return j % 4 * 4 + j // 4


def tile_at(j):
    return slice(j * 8, (j + 1) * 8)


def stream_mask():
    return iota((8, HALF), 0) % 4 < 2


def pick(a_forward, forward, backward):
    first = stream_mask()
    return jnp.where(first, forward, backward) if a_forward else jnp.where(first, backward, forward)


def inner_pass(got_ref, logs_ref, a_forward, through_ref, before_ref, decay_ref):
    logs = logs_spread(logs_ref[...])
    decay_ref[...] = jnp.exp(logs)
    spots = [inner_order(j) for j in range(GROUP)]
    state = jnp.zeros((8, HALF), F32)
    gone = jnp.zeros((8, HALF), F32)
    forward = {}
    for j in spots:
        forward[j] = state, gone
        state = decay_ref[tile_at(j), :] * state + got_ref[tile_at(j), :HALF].astype(F32)
        gone = gone + logs[tile_at(j), :]
    ahead = state
    state = jnp.zeros((8, HALF), F32)
    gone = jnp.zeros((8, HALF), F32)
    for j in reversed(spots):
        before_ref[tile_at(j), :] = pick(a_forward, forward[j][0], state)
        through_ref[tile_at(j), :] = jnp.exp(pick(a_forward, forward[j][1], gone))
        state = decay_ref[tile_at(j), :] * state + got_ref[tile_at(j), :HALF].astype(F32)
        gone = gone + logs[tile_at(j), :]
    return pick(a_forward, ahead, state).astype(BF16)


def inner_first_kernel(got_ref, before_ref, through_ref, logs_ref, total_ref, decay_ref):
    logs_ref[...] = got_ref[:, HALF:]
    total = inner_pass(got_ref, logs_ref, True, through_ref, before_ref, decay_ref)
    compact = jnp.zeros((8, LOGS), F32)
    for j in range(GROUP):
        compact = compact + got_ref[tile_at(j), HALF:].astype(F32)
    compact = compact + pltpu.roll(compact, LOGS - 4, 1) + pltpu.roll(compact, LOGS - 8, 1)
    compact = jnp.where(iota((8, LOGS), 1) < 4, compact, 0.0)
    high = compact.astype(BF16).astype(F32)
    middle = (compact - high).astype(BF16).astype(F32)
    low = compact - high - middle
    compact = (high + pltpu.roll(middle, 4, 1) + pltpu.roll(low, 8, 1)).astype(BF16)
    for j in range(GROUP):
        total_ref[tile_at(j), :HALF] = total
        total_ref[tile_at(j), HALF:] = compact


def inner_second_kernel(got_ref, logs_ref, before_ref, through_ref, total_ref, decay_ref):
    total = inner_pass(got_ref, logs_ref, False, through_ref, before_ref, decay_ref)
    for j in range(GROUP):
        total_ref[tile_at(j), :] = total


def outer_pass(mine, got_ref, logs, a_forward, before_ref, through_ref, out_ref, decay_ref):
    decay_ref[...] = jnp.exp(logs_spread(logs))

    def step(state, at):
        return decay_ref[tile_at(at), :] * state + got_ref[tile_at(at), :HALF].astype(F32)

    state = jnp.zeros((8, HALF), F32)
    for j in range(GROUP):
        state = jnp.where(j < mine, step(state, outer_order(j)), state)
    ahead = state
    state = jnp.zeros((8, HALF), F32)
    for j in reversed(range(GROUP)):
        state = jnp.where(j > mine, step(state, outer_order(j)), state)
    both = pick(a_forward, ahead, state)
    for j in range(GROUP):
        at = tile_at(j)
        out_ref[at, :] = (through_ref[at, :] * both + before_ref[at, :]).astype(BF16)


def outer_first_kernel(
    mine_ref, got_ref, before_ref, through_ref, logs_ref, out_ref, decay_ref
):
    logs_ref[...] = got_ref[:, HALF:]
    outer_pass(
        mine_ref[0], got_ref, got_ref[:, HALF:], True, before_ref, through_ref, out_ref, decay_ref
    )


def outer_second_kernel(
    mine_ref, got_ref, before_ref, through_ref, logs_ref, out_ref, decay_ref
):
    outer_pass(
        mine_ref[0], got_ref, logs_ref[...], False, before_ref, through_ref, out_ref, decay_ref
    )


def finish_kernel(
    rlocal_ref, rcols_ref, rplaced_ref, got_ref, wout_ref,
    clocal_ref, ccols_ref, cplaced_ref, win_ref, gain_hbm, x_hbm, sent_hbm,
    mixed_ref, message_ref, gain_ref, x_ref, sem,
):
    copies = [
        pltpu.make_async_copy(x_hbm, x_ref, sem.at[0]),
        pltpu.make_async_copy(gain_hbm, gain_ref, sem.at[1]),
        pltpu.make_async_copy(sent_hbm, message_ref.at[:, HALF : 2 * HALF], sem.at[2]),
    ]
    for copy in copies:
        copy.start()
    got = got_ref[...]
    carried = carried_of(rplaced_ref[...], got) * spread_heads(rcols_ref[...], OPENING)
    scanned = (rlocal_ref[...] + carried).astype(BF16)
    total = nn(scanned, wout_ref[...])
    carried = carried_of(cplaced_ref[...], got) * spread_heads(ccols_ref[...], ENDING)
    scanned = (clocal_ref[...] + carried).astype(BF16)
    returned = nt(scanned, win_ref[...])
    copies[0].wait()
    mixed = (x_ref[...].astype(F32) + total).astype(BF16)
    mixed_ref[...] = mixed
    message_ref[:, :HALF] = to_message(mixed, row_target)
    copies[1].wait()
    scaled = (gain_ref[...] * returned).astype(BF16)
    message_ref[:, 2 * HALF :] = to_message(scaled, column_target)
    copies[2].wait()


def cross_kernel(
    got_ref, mixed_ref, rsel_ref, rcols_ref, wout_ref, csel_ref, ccols_ref, gain_ref, win_ref,
    cx_ref, cvalue_ref, y_ref, pulled_ref, message_ref,
):
    y = from_message(got_ref[:, HALF : 2 * HALF], row_target)
    scaled = from_message(got_ref[:, 2 * HALF :], row_target)
    y = input_gradient(mixed_ref[...].astype(F32), y, scaled)
    y_ref[...] = y
    pulled = nt(y, wout_ref[...]).astype(BF16)
    pulled_ref[...] = pulled
    weighted = (pulled.astype(F32) * spread_heads(rcols_ref[...], OPENING)).astype(BF16)
    first = state_rows(weighted, turned_select(rsel_ref), STATE, 0)
    x = from_message(got_ref[:, :HALF], column_target)
    cx_ref[...] = x.astype(BF16)
    value = nn(normalized(x, gain_ref[...]), win_ref[...]).astype(BF16)
    cvalue_ref[...] = value
    weighted = (value.astype(F32) * spread_heads(ccols_ref[...], ENDING)).astype(BF16)
    second = state_rows(weighted, turned_select(csel_ref), 0, 1)
    message_ref[...] = (first + second).astype(BF16)


def col_scan_kernel(
    value_ref, sel_ref, rows_ref, cols_ref, skip_ref, x_ref, local_ref, placed_ref, kept_ref
):
    kept_ref[...] = x_ref[...]
    select = turned_select(sel_ref)
    placed_ref[...] = placed(select, STATE, 1)
    local_scan(value_ref, select, rows_ref[...], cols_ref[...], skip_ref, local_ref, False)


def row_scan_back_kernel(
    value_ref, sel_ref, rows_ref, cols_ref, skip_ref, gain_ref, local_ref, placed_ref, kept_ref
):
    kept_ref[...] = gain_ref[...]
    select = turned_select(sel_ref)
    placed_ref[...] = placed(select, 0, 0)
    local_scan(value_ref, select, rows_ref[...], cols_ref[...], skip_ref, local_ref, True)


def end_kernel(
    got_ref, cplaced_ref, ccols_ref, clocal_ref, rplaced_ref, rcols_ref, rlocal_ref, rwin_ref,
    gain_ref, x_ref, y_ref, cx_hbm, cwout_hbm,
    mixed_hbm, grad_hbm, cx_ref, cwout_ref, mixed_ref, grad_ref, sem,
):
    def copy(a, b, i):
        return pltpu.make_async_copy(a, b, sem.at[i])

    cwout_in, cx_in = copy(cwout_hbm, cwout_ref, 0), copy(cx_hbm, cx_ref, 1)
    cwout_in.start()
    cx_in.start()
    got = got_ref[...]
    carried = carried_of(rplaced_ref[...], got) * spread_heads(rcols_ref[...], ENDING)
    scanned = (rlocal_ref[...] + carried).astype(BF16)
    scaled = gain_ref[...] * nt(scanned, rwin_ref[...])
    grad_ref[...] = input_gradient(x_ref[...].astype(F32), y_ref[...].astype(F32), scaled)
    grad_out = copy(grad_ref, grad_hbm, 2)
    grad_out.start()
    carried = carried_of(cplaced_ref[...], got) * spread_heads(ccols_ref[...], OPENING)
    scanned = (clocal_ref[...] + carried).astype(BF16)
    cwout_in.wait()
    cx_in.wait()
    outs = [copy(mixed_ref.at[rows], mixed_hbm.at[rows], 3 + k) for k, rows in enumerate(QUARTERS)]
    for rows, out in zip(QUARTERS, outs):
        mixed = cx_ref[rows, :].astype(F32) + nn(scanned[rows, :], cwout_ref[...])
        mixed_ref[rows, :] = mixed.astype(BF16)
        out.start()
    grad_out.wait()
    for out in outs:
        out.wait()


QUARTERS = [slice(k * 64, (k + 1) * 64) for k in range(4)]

VM = pl.BlockSpec(memory_space=pltpu.VMEM)
SM = pl.BlockSpec(memory_space=pltpu.SMEM)
ANY = pl.BlockSpec(memory_space=pl.ANY)


class Near(tuple):
    pass


class Far(tuple):
    pass


def shaped(out):
    if isinstance(out, Near):
        return pltpu.VMEM(*out)
    if isinstance(out, Far):
        return pltpu.HBM(*out)
    return jax.ShapeDtypeStruct(*out)


def near(array):
    return pltpu.with_memory_space_constraint(array, pltpu.VMEM)


def far(array):
    return pltpu.with_memory_space_constraint(array, pltpu.HBM)


def call(kernel, name, outs, args, scalars=(), left=(), kept=(), scratch=(), flops=1e9):
    return pl.pallas_call(
        kernel,
        name=name,
        out_shape=[shaped(out) for out in outs],
        in_specs=[SM if i in scalars else ANY if i in left else VM for i in range(len(args))],
        out_specs=[ANY if i in kept else VM for i in range(len(outs))],
        scratch_shapes=list(scratch),
        compiler_params=pltpu.CompilerParams(vmem_limit_bytes=16 << 20),
        cost_estimate=pl.CostEstimate(flops=int(flops), bytes_accessed=1 << 20, transcendentals=0),
    )(*args)


TOKS = (TOK, WIDTH)
MSG = (LINES, HALF)
LOGGED = (LINES, HALF + LOGS)
PAIR = (TOK, 2 * LINES)
BIG = (2 * TOK, HALF)
WIDE = (2 * TOK, 3 * HALF)
ROWS = (2 * HEADS, TOK)
COLS = (TOK, 4 * HEADS)
SEL = (2, 2 * STATE, 128)
LAM = (HEADS, 2, 128)


def swapped(array, axes):
    count = 1
    for axis in axes:
        count *= lax.axis_size(axis)
    split = array.reshape(count, array.shape[0] // count, array.shape[1])
    return lax.all_to_all(split, axes, split_axis=0, concat_axis=0, tiled=True).reshape(array.shape)


def body(
    tokens, row_select, row_decay, row_gain, row_skip, row_in, row_out,
    col_select, col_decay, col_gain, col_skip, col_in, col_out, cotangent,
):
    mine = (lax.axis_index("frame") * lax.axis_size("seq_0") + lax.axis_index("seq_0")).reshape(1)
    x = tokens.reshape(TOKS)
    y = cotangent.reshape(TOKS)
    rsel = row_select.reshape(2, 128, 2 * STATE).swapaxes(1, 2)
    csel = col_select.reshape(2, 128, 2 * STATE).swapaxes(1, 2)
    rlam = row_decay.reshape(HEADS, 2, 128)
    clam = col_decay.reshape(HEADS, 2, 128)
    rgain = row_gain.reshape(1, WIDTH)
    cgain = col_gain.reshape(1, WIDTH)
    rskip = row_skip.reshape(1, HEADS)
    cskip = col_skip.reshape(1, HEADS)

    rlocal, rcols, rrows, rplaced, clocal, ccols, crows, cplaced, sent, message = call(
        start_kernel, "start",
        [Near((TOKS, F32)), Near((COLS, F32)), Near((ROWS, F32)), Near((PAIR, BF16)),
         Near((TOKS, F32)), Near((COLS, F32)), Near((ROWS, F32)), Near((PAIR, BF16)),
         Far((BIG, BF16)), Near((LOGGED, BF16))],
        [far(a) for a in
         (x, rsel, rlam, rskip, rgain, row_in, y, csel, clam, cskip, col_out)],
        left=range(11), kept=(8,),
        scratch=[
            pltpu.VMEM(TOKS, BF16), pltpu.VMEM(SEL, BF16), pltpu.VMEM(LAM, F32),
            pltpu.VMEM((1, HEADS), F32), pltpu.VMEM((1, WIDTH), F32),
            pltpu.VMEM((WIDTH, WIDTH), BF16), pltpu.VMEM(TOKS, BF16), pltpu.VMEM(SEL, BF16),
            pltpu.VMEM(LAM, F32), pltpu.VMEM((1, HEADS), F32), pltpu.VMEM((WIDTH, WIDTH), BF16),
            pltpu.VMEM(TOKS, BF16), pltpu.VMEM(TOKS, BF16), pltpu.VMEM(BIG, BF16),
            pltpu.SemaphoreType.DMA((12,)),
        ],
    )
    message, mine = lax.optimization_barrier((message, mine))
    got = swapped(message, INNER)
    before, through, inner_logs, total = call(
        inner_first_kernel, "inner_first",
        [Near((MSG, F32)), Near((MSG, F32)), Near(((LINES, LOGS), BF16)), Near((LOGGED, BF16))],
        [near(got)], scratch=[pltpu.VMEM(MSG, F32)], flops=1e7,
    )
    groups = swapped(total, OUTER)
    outer_logs, down = call(
        outer_first_kernel, "outer_first", [Near(((LINES, LOGS), BF16)), Near((MSG, BF16))],
        [mine, near(groups), before, through], (0,), scratch=[pltpu.VMEM(MSG, F32)], flops=1e7,
    )
    got = near(swapped(down, INNER))
    rmixed, sending, gain = call(
        finish_kernel, "finish",
        [Near((TOKS, BF16)), Near((WIDE, BF16)), Near(((1, WIDTH), F32))],
        [rlocal, rcols, rplaced, got, near(row_out), clocal, ccols, cplaced, near(col_in),
         far(cgain), far(x), far(sent)],
        left=(9, 10, 11),
        scratch=[pltpu.VMEM(TOKS, BF16), pltpu.SemaphoreType.DMA((3,))],
    )
    arrived = swapped(sending, SEQ)
    cx, cvalue, ry, rpulled, message = call(
        cross_kernel, "cross",
        [Near((TOKS, BF16)), Near((TOKS, BF16)), Near((TOKS, BF16)), Near((TOKS, BF16)),
         Near((MSG, BF16))],
        [near(arrived), rmixed, near(rsel), rcols, near(row_out), near(csel), ccols,
         gain, near(col_in)],
    )
    got = swapped(message, INNER)
    before, through, total = call(
        inner_second_kernel, "inner_second", [Near((MSG, F32)), Near((MSG, F32)), Near((MSG, BF16))],
        [near(got), inner_logs], scratch=[pltpu.VMEM(MSG, F32)], flops=1e7,
    )
    groups = swapped(total, OUTER)
    (down,) = call(
        outer_second_kernel, "outer_second", [Near((MSG, BF16))],
        [mine, near(groups), before, through, outer_logs], (0,),
        scratch=[pltpu.VMEM(MSG, F32)], flops=1e7,
    )
    got = swapped(down, INNER)
    clocal, cplaced, cx = call(
        col_scan_kernel, "col_scan", [Near((TOKS, F32)), Near((PAIR, BF16)), Far((TOKS, BF16))],
        [cvalue, far(csel), crows, ccols, far(cskip), cx],
    )
    rlocal, rplaced, gain = call(
        row_scan_back_kernel, "row_scan_back",
        [Near((TOKS, F32)), Near((PAIR, BF16)), Near(((1, WIDTH), F32))],
        [rpulled, far(rsel), rrows, rcols, far(rskip), far(rgain)],
    )
    mixed, grad = call(
        end_kernel, "end", [Far((TOKS, BF16)), Far((TOKS, BF16))],
        [near(got), cplaced, ccols, clocal, rplaced, rcols, rlocal, near(row_in),
         gain, near(x), ry, far(cx), far(col_out)],
        left=(11, 12), kept=(0, 1),
        scratch=[
            pltpu.VMEM(TOKS, BF16), pltpu.VMEM((WIDTH, WIDTH), BF16), pltpu.VMEM(TOKS, BF16),
            pltpu.VMEM(TOKS, BF16), pltpu.SemaphoreType.DMA((7,)),
        ],
    )
    return mixed.reshape(cotangent.shape), grad.reshape(tokens.shape)


def solution(mesh):
    torus = Mesh(
        mesh.devices.reshape(4, 8, 2, mesh.shape["frame"]), ("seq_0", "seq_1", "seq_2", "frame")
    )
    tall = P("frame", SEQ, None, None)
    flat = P("frame", None, SEQ, None)
    in_specs = (tall, tall, flat, P(), P(), P(), P(), tall, flat, P(), P(), P(), P(), tall)
    return jax.shard_map(
        body, mesh=torus, in_specs=in_specs, out_specs=(tall, tall), check_vma=False
    )
```

```python
from functools import partial

import jax
import jax.numpy as jnp
from jax import lax
from jax.experimental import pallas as pl
from jax.experimental.pallas import tpu as pltpu
from jax.sharding import Mesh
from jax.sharding import PartitionSpec as P

SEQ = ("seq_0", "seq_1", "seq_2")
INNER = ("seq_2", "seq_1")
OUTER = ("seq_0", "frame")

EPSILON = 1e-05
LOG2E = 1.4426950408889634

TOK = 256
WIDTH = 512
HEADS = 8
PART = 64
STATE = 32
GROUP = 16
HALF = 256
LINES = GROUP * 8
LOGS = 128

F32 = jnp.float32
BF16 = jnp.bfloat16


def iota(shape, axis):
    return lax.broadcasted_iota(jnp.int32, shape, axis)


def onehot(mask):
    return mask.astype(F32).astype(BF16)


def dot(left, right, left_axis, right_axis):
    return lax.dot_general(
        left, right, (((left_axis,), (right_axis,)), ((), ())), preferred_element_type=F32
    )


def nn(left, right):
    return dot(left, right, 1, 0)


def nt(left, right):
    return dot(left, right, 1, 1)


def tn(left, right):
    return dot(left, right, 0, 0)


def parts_of(values, count):
    out = []
    rest = values
    for _ in range(count):
        piece = rest.astype(BF16)
        out.append(piece)
        rest = rest - piece.astype(F32)
    return out


def one_minus_exp(v):
    series = 1.0 - v * (1.0 / 9.0)
    for k in range(8, 1, -1):
        series = 1.0 - v * (1.0 / k) * series
    return jnp.where(v < 0.5, v * series, 1.0 - jnp.exp(-v))


def lam_of(lam_ref):
    return jnp.concatenate([lam_ref[:, 0, :], lam_ref[:, 1, :]], axis=1)


def turned_select(select_ref):
    return jnp.concatenate([select_ref[0], select_ref[1]], axis=1)


def block_terms(lam):
    upto = onehot(iota((TOK, TOK), 1) <= iota((TOK, TOK), 0))
    stacked = nt(jnp.concatenate(parts_of(lam, 3), axis=0), upto)
    cum = stacked[:8] + stacked[8:16] + stacked[16:]
    square = one_minus_exp(-2.0 * lam)
    ending = jnp.exp(cum[:, TOK - 1 :] - cum) * jnp.sqrt(square)
    log_inward = jnp.maximum(0.5 * jnp.log2(square), -500.0)
    rows = jnp.concatenate([cum * LOG2E, log_inward - cum * LOG2E], axis=0)
    cols = jnp.concatenate([rows, jnp.exp(cum), ending], axis=0).T
    return cum, rows, cols


OPENING = 16
ENDING = 24


def spread_heads(cols, offset):
    spread = onehot(
        iota((4 * HEADS, WIDTH), 1) // PART + offset == iota((4 * HEADS, WIDTH), 0)
    )
    return sum(nn(p, spread) for p in reversed(parts_of(cols, 2)))


def placed(select, offset, stream):
    at = iota((2 * STATE, 2 * LINES), 0)
    col = iota((2 * STATE, 2 * LINES), 1)
    row = col % LINES
    hit = (at == offset + 2 * (row // 8) + row % 2) & (row % 8 // 2 == col // LINES * 2 + stream)
    return tn(select, onehot(hit)).astype(BF16)


def carried_of(placed_pair, got):
    return jnp.concatenate(
        [nn(placed_pair[:, half * LINES : (half + 1) * LINES], got) for half in (0, 1)], axis=1
    )


def state_rows(weighted, select, offset, stream):
    at = iota((LINES, 2 * STATE), 1)
    row = iota((LINES, 2 * STATE), 0)
    out = None
    for half in (0, 1):
        hit = (at == offset + 2 * (row // 8) + row % 2) & (row % 8 // 2 == half * 2 + stream)
        rows = nn(onehot(hit), select).astype(BF16)
        part = nn(rows, weighted[:, half * HALF : (half + 1) * HALF])
        out = part if out is None else out + part
    return out


def normalized(x, gain):
    factor = lax.rsqrt(jnp.mean(x * x, axis=-1, keepdims=True) + EPSILON)
    return (x * factor * gain).astype(BF16)


def input_gradient(x, y, scaled):
    factor = lax.rsqrt(jnp.mean(x * x, axis=-1, keepdims=True) + EPSILON)
    inner = jnp.mean(scaled * x, axis=-1, keepdims=True)
    return (y + factor * scaled - x * (factor * factor * factor) * inner).astype(BF16)


def local_scan(values_ref, select, rows, cols, skip_ref, out_ref, backward):
    source = select[:STATE]
    target = select[STATE:]
    if backward:
        affinity = tn(source, target)
        left, right = cols[:, HEADS : 2 * HEADS], rows[:HEADS]
    else:
        affinity = tn(target, source)
        left, right = cols[:, :HEADS], rows[HEADS : 2 * HEADS]
    first = iota((128, 128), 0)
    second = iota((128, 128), 1)
    keep = second >= first if backward else second <= first
    lower = iota((1, 2 * PART), 1) < PART
    lo, hi = slice(0, 128), slice(128, 256)

    def tile(h, a, b):
        m = jnp.exp2(left[a, h : h + 1] + right[h : h + 1, b]) * affinity[a, b]
        return (jnp.where(keep, m, 0.0) if a == b else m).astype(BF16)

    def mixed(pair, rows, sources, parts):
        tiles = [tile(h, rows, b) for h in pair for b in sources]
        values = [part[b] for part in parts for b in sources]
        return nn(jnp.concatenate(tiles, axis=1), jnp.concatenate(values, axis=0))

    for h in range(0, HEADS, 2):
        span = slice(h * PART, (h + 2) * PART)
        v = values_ref[:, span].astype(F32)
        parts = [jnp.where(lower, v, 0.0).astype(BF16), jnp.where(lower, 0.0, v).astype(BF16)]
        skip = jnp.where(lower, skip_ref[0:1, h : h + 1], skip_ref[0:1, h + 1 : h + 2])
        top = mixed((h, h + 1), lo, (lo, hi) if backward else (lo,), parts)
        low = mixed((h, h + 1), hi, (hi,) if backward else (lo, hi), parts)
        out_ref[lo, span] = top + skip * v[lo]
        out_ref[hi, span] = low + skip * v[hi]


def row_target(token):
    column = token % 128
    return column // 2 * 8 + column % 2 * 2 + token // 128


def column_target(token):
    row = token % 128
    return row // 2 * 8 + token // 128 * 2 + row % 2


def to_message(tokens, target):
    off = iota((2 * TOK, TOK), 0) - target(iota((1, TOK), 1))
    left = nn(onehot(off == 0), tokens[:, :HALF])
    return (left + nn(onehot(off == 4), tokens[:, HALF:])).astype(BF16)


def from_message(message, target):
    off = iota((TOK, 2 * TOK), 1) - target(iota((TOK, 1), 0))
    return jnp.concatenate([nn(onehot(off == 0), message), nn(onehot(off == 4), message)], axis=1)


def start_kernel(
    x_hbm, rsel_hbm, rlam_hbm, rskip_hbm, gain_hbm, win_hbm,
    y_hbm, csel_hbm, clam_hbm, cskip_hbm, wout_hbm,
    rlocal_ref, rcols_ref, rrows_ref, rplaced_ref, clocal_ref, ccols_ref, crows_ref, cplaced_ref,
    sent_ref, message_ref,
    x_ref, rsel_ref, rlam_ref, rskip_ref, gain_ref, win_ref,
    y_ref, csel_ref, clam_ref, cskip_ref, wout_ref, value_ref, pulled_ref, sem,
):
    pairs = (
        (rlam_hbm, rlam_ref), (clam_hbm, clam_ref), (rsel_hbm, rsel_ref), (csel_hbm, csel_ref),
        (rskip_hbm, rskip_ref), (cskip_hbm, cskip_ref), (gain_hbm, gain_ref), (x_hbm, x_ref),
        (win_hbm, win_ref), (y_hbm, y_ref), (wout_hbm, wout_ref),
    )
    copies = [pltpu.make_async_copy(a, b, sem.at[i]) for i, (a, b) in enumerate(pairs)]
    for copy in copies:
        copy.start()
    for copy in copies[:7]:
        copy.wait()
    rcum, rrows, rcols = block_terms(lam_of(rlam_ref))
    ccum, crows, ccols = block_terms(lam_of(clam_ref))
    rrows_ref[...] = rrows
    rcols_ref[...] = rcols
    crows_ref[...] = crows
    ccols_ref[...] = ccols
    rsel = turned_select(rsel_ref)
    csel = turned_select(csel_ref)
    row = iota((8, HEADS), 0)
    head = iota((8, HEADS), 1)
    rlast = jnp.broadcast_to(rcum[:, TOK - 1 :], (HEADS, HEADS)).T
    clast = jnp.broadcast_to(ccum[:, TOK - 1 :], (HEADS, HEADS)).T
    logs = jnp.where(row % 4 < 2, rlast, clast)
    logs = jnp.where(head // 4 == row // 4, logs, 0.0)
    tile = None
    for k, piece in enumerate(parts_of(logs, 3)):
        place = onehot(iota((HEADS, LOGS), 1) == 4 * k + iota((HEADS, LOGS), 0) % 4)
        part = nn(piece, place)
        tile = part if tile is None else tile + part
    tile = tile.astype(BF16)
    for j in range(GROUP):
        message_ref[j * 8 : (j + 1) * 8, HALF:] = tile
    rplaced_ref[...] = placed(rsel, STATE, 0)
    cplaced_ref[...] = placed(csel, 0, 1)
    copies[7].wait()
    normed = normalized(x_ref[...].astype(F32), gain_ref[...])
    copies[8].wait()
    value = nn(normed, win_ref[...]).astype(BF16)
    value_ref[...] = value
    weighted = (value.astype(F32) * spread_heads(rcols, ENDING)).astype(BF16)
    first = state_rows(weighted, rsel, 0, 0)
    copies[9].wait()
    sent_ref[...] = to_message(y_ref[...], column_target)
    local_scan(value_ref, rsel, rrows, rcols, rskip_ref, rlocal_ref, False)
    copies[10].wait()
    pulled = nt(y_ref[...], wout_ref[...]).astype(BF16)
    pulled_ref[...] = pulled
    weighted = (pulled.astype(F32) * spread_heads(ccols, OPENING)).astype(BF16)
    second = state_rows(weighted, csel, STATE, 1)
    message_ref[:, :HALF] = (first + second).astype(BF16)
    local_scan(pulled_ref, csel, crows, ccols, cskip_ref, clocal_ref, True)


def logs_spread(tiles):
    spread = onehot(
        (iota((LOGS, HALF), 0) % 4 == iota((LOGS, HALF), 1) // PART) & (iota((LOGS, HALF), 0) < 12)
    )
    return nn(tiles, spread)


def inner_order(j):
    return j % 2 * 8 + j // 2


def outer_order(j):
    return j % 4 * 4 + j // 4


def tile_at(j):
    return slice(j * 8, (j + 1) * 8)


def stream_mask():
    return iota((8, HALF), 0) % 4 < 2


def pick(a_forward, forward, backward):
    first = stream_mask()
    return jnp.where(first, forward, backward) if a_forward else jnp.where(first, backward, forward)


def inner_pass(got_ref, logs_ref, a_forward, through_ref, before_ref, decay_ref):
    logs = logs_spread(logs_ref[...])
    decay_ref[...] = jnp.exp(logs)
    spots = [inner_order(j) for j in range(GROUP)]
    state = jnp.zeros((8, HALF), F32)
    gone = jnp.zeros((8, HALF), F32)
    forward = {}
    for j in spots:
        forward[j] = state, gone
        state = decay_ref[tile_at(j), :] * state + got_ref[tile_at(j), :HALF].astype(F32)
        gone = gone + logs[tile_at(j), :]
    ahead = state
    state = jnp.zeros((8, HALF), F32)
    gone = jnp.zeros((8, HALF), F32)
    for j in reversed(spots):
        before_ref[tile_at(j), :] = pick(a_forward, forward[j][0], state)
        through_ref[tile_at(j), :] = jnp.exp(pick(a_forward, forward[j][1], gone))
        state = decay_ref[tile_at(j), :] * state + got_ref[tile_at(j), :HALF].astype(F32)
        gone = gone + logs[tile_at(j), :]
    return pick(a_forward, ahead, state).astype(BF16)


def inner_first_kernel(got_ref, before_ref, through_ref, logs_ref, total_ref, decay_ref):
    logs_ref[...] = got_ref[:, HALF:]
    total = inner_pass(got_ref, logs_ref, True, through_ref, before_ref, decay_ref)
    compact = jnp.zeros((8, LOGS), F32)
    for j in range(GROUP):
        compact = compact + got_ref[tile_at(j), HALF:].astype(F32)
    compact = compact + pltpu.roll(compact, LOGS - 4, 1) + pltpu.roll(compact, LOGS - 8, 1)
    compact = jnp.where(iota((8, LOGS), 1) < 4, compact, 0.0)
    high = compact.astype(BF16).astype(F32)
    middle = (compact - high).astype(BF16).astype(F32)
    low = compact - high - middle
    compact = (high + pltpu.roll(middle, 4, 1) + pltpu.roll(low, 8, 1)).astype(BF16)
    for j in range(GROUP):
        total_ref[tile_at(j), :HALF] = total
        total_ref[tile_at(j), HALF:] = compact


def inner_second_kernel(got_ref, logs_ref, before_ref, through_ref, total_ref, decay_ref):
    total = inner_pass(got_ref, logs_ref, False, through_ref, before_ref, decay_ref)
    for j in range(GROUP):
        total_ref[tile_at(j), :] = total


def outer_pass(mine, got_ref, logs, a_forward, before_ref, through_ref, out_ref, decay_ref):
    decay_ref[...] = jnp.exp(logs_spread(logs))

    def step(state, at):
        return decay_ref[tile_at(at), :] * state + got_ref[tile_at(at), :HALF].astype(F32)

    state = jnp.zeros((8, HALF), F32)
    for j in range(GROUP):
        state = jnp.where(j < mine, step(state, outer_order(j)), state)
    ahead = state
    state = jnp.zeros((8, HALF), F32)
    for j in reversed(range(GROUP)):
        state = jnp.where(j > mine, step(state, outer_order(j)), state)
    both = pick(a_forward, ahead, state)
    for j in range(GROUP):
        at = tile_at(j)
        out_ref[at, :] = (through_ref[at, :] * both + before_ref[at, :]).astype(BF16)


def outer_first_kernel(
    mine_ref, got_ref, before_ref, through_ref, logs_ref, out_ref, decay_ref
):
    logs_ref[...] = got_ref[:, HALF:]
    outer_pass(
        mine_ref[0], got_ref, got_ref[:, HALF:], True, before_ref, through_ref, out_ref, decay_ref
    )


def outer_second_kernel(
    mine_ref, got_ref, before_ref, through_ref, logs_ref, out_ref, decay_ref
):
    outer_pass(
        mine_ref[0], got_ref, logs_ref[...], False, before_ref, through_ref, out_ref, decay_ref
    )


def finish_kernel(
    rlocal_ref, rcols_ref, rplaced_ref, got_ref, wout_ref,
    clocal_ref, ccols_ref, cplaced_ref, win_ref, gain_hbm, x_ref, sent_ref,
    mixed_ref, message_ref, gain_ref, sem,
):
    gain_in = pltpu.make_async_copy(gain_hbm, gain_ref, sem.at[0])
    gain_in.start()
    message_ref[:, HALF : 2 * HALF] = sent_ref[...]
    got = got_ref[...]
    carried = carried_of(rplaced_ref[...], got) * spread_heads(rcols_ref[...], OPENING)
    scanned = (rlocal_ref[...] + carried).astype(BF16)
    total = nn(scanned, wout_ref[...])
    carried = carried_of(cplaced_ref[...], got) * spread_heads(ccols_ref[...], ENDING)
    scanned = (clocal_ref[...] + carried).astype(BF16)
    returned = nt(scanned, win_ref[...])
    mixed = (x_ref[...].astype(F32) + total).astype(BF16)
    mixed_ref[...] = mixed
    message_ref[:, :HALF] = to_message(mixed, row_target)
    gain_in.wait()
    scaled = (gain_ref[...] * returned).astype(BF16)
    message_ref[:, 2 * HALF :] = to_message(scaled, column_target)


def cross_kernel(
    got_ref, mixed_ref, rsel_ref, rcols_ref, wout_ref, csel_ref, ccols_ref, gain_ref, win_ref,
    cx_ref, cvalue_ref, y_ref, pulled_ref, message_ref,
):
    y = from_message(got_ref[:, HALF : 2 * HALF], row_target)
    scaled = from_message(got_ref[:, 2 * HALF :], row_target)
    y = input_gradient(mixed_ref[...].astype(F32), y, scaled)
    y_ref[...] = y
    pulled = nt(y, wout_ref[...]).astype(BF16)
    pulled_ref[...] = pulled
    weighted = (pulled.astype(F32) * spread_heads(rcols_ref[...], OPENING)).astype(BF16)
    first = state_rows(weighted, turned_select(rsel_ref), STATE, 0)
    x = from_message(got_ref[:, :HALF], column_target)
    cx_ref[...] = x.astype(BF16)
    value = nn(normalized(x, gain_ref[...]), win_ref[...]).astype(BF16)
    cvalue_ref[...] = value
    weighted = (value.astype(F32) * spread_heads(ccols_ref[...], ENDING)).astype(BF16)
    second = state_rows(weighted, turned_select(csel_ref), 0, 1)
    message_ref[...] = (first + second).astype(BF16)


def col_scan_kernel(
    value_ref, sel_ref, rows_ref, cols_ref, skip_ref, local_ref, placed_ref
):
    select = turned_select(sel_ref)
    placed_ref[...] = placed(select, STATE, 1)
    local_scan(value_ref, select, rows_ref[...], cols_ref[...], skip_ref, local_ref, False)


def row_scan_back_kernel(
    value_ref, sel_ref, rows_ref, cols_ref, skip_ref, gain_ref, local_ref, placed_ref, kept_ref
):
    kept_ref[...] = gain_ref[...]
    select = turned_select(sel_ref)
    placed_ref[...] = placed(select, 0, 0)
    local_scan(value_ref, select, rows_ref[...], cols_ref[...], skip_ref, local_ref, True)


def end_kernel(
    got_ref, cplaced_ref, ccols_ref, clocal_ref, rplaced_ref, rcols_ref, rlocal_ref, rwin_ref,
    gain_ref, x_ref, y_ref, cx_ref, cwout_hbm,
    mixed_hbm, grad_hbm, cwout_ref, mixed_ref, grad_ref, sem,
):
    def copy(a, b, i):
        return pltpu.make_async_copy(a, b, sem.at[i])

    cwout_in = copy(cwout_hbm, cwout_ref, 0)
    cwout_in.start()
    got = got_ref[...]
    carried = carried_of(rplaced_ref[...], got) * spread_heads(rcols_ref[...], ENDING)
    scanned = (rlocal_ref[...] + carried).astype(BF16)
    scaled = gain_ref[...] * nt(scanned, rwin_ref[...])
    grad_ref[...] = input_gradient(x_ref[...].astype(F32), y_ref[...].astype(F32), scaled)
    grad_out = copy(grad_ref, grad_hbm, 1)
    grad_out.start()
    carried = carried_of(cplaced_ref[...], got) * spread_heads(ccols_ref[...], OPENING)
    scanned = (clocal_ref[...] + carried).astype(BF16)
    cwout_in.wait()
    outs = [copy(mixed_ref.at[rows], mixed_hbm.at[rows], 2 + k) for k, rows in enumerate(QUARTERS)]
    for rows, out in zip(QUARTERS, outs):
        mixed = cx_ref[rows, :].astype(F32) + nn(scanned[rows, :], cwout_ref[...])
        mixed_ref[rows, :] = mixed.astype(BF16)
        out.start()
    grad_out.wait()
    for out in outs:
        out.wait()


QUARTERS = [slice(k * 64, (k + 1) * 64) for k in range(4)]

VM = pl.BlockSpec(memory_space=pltpu.VMEM)
SM = pl.BlockSpec(memory_space=pltpu.SMEM)
ANY = pl.BlockSpec(memory_space=pl.ANY)


class Near(tuple):
    pass


class Far(tuple):
    pass


def shaped(out):
    if isinstance(out, Near):
        return pltpu.VMEM(*out)
    if isinstance(out, Far):
        return pltpu.HBM(*out)
    return jax.ShapeDtypeStruct(*out)


def near(array):
    return pltpu.with_memory_space_constraint(array, pltpu.VMEM)


def far(array):
    return pltpu.with_memory_space_constraint(array, pltpu.HBM)


def call(kernel, name, outs, args, scalars=(), left=(), kept=(), scratch=(), flops=1e9):
    return pl.pallas_call(
        kernel,
        name=name,
        out_shape=[shaped(out) for out in outs],
        in_specs=[SM if i in scalars else ANY if i in left else VM for i in range(len(args))],
        out_specs=[ANY if i in kept else VM for i in range(len(outs))],
        scratch_shapes=list(scratch),
        compiler_params=pltpu.CompilerParams(vmem_limit_bytes=16 << 20),
        cost_estimate=pl.CostEstimate(flops=int(flops), bytes_accessed=1 << 20, transcendentals=0),
    )(*args)


TOKS = (TOK, WIDTH)
MSG = (LINES, HALF)
LOGGED = (LINES, HALF + LOGS)
PAIR = (TOK, 2 * LINES)
BIG = (2 * TOK, HALF)
WIDE = (2 * TOK, 3 * HALF)
ROWS = (2 * HEADS, TOK)
COLS = (TOK, 4 * HEADS)
SEL = (2, 2 * STATE, 128)
LAM = (HEADS, 2, 128)


def swapped(array, axes):
    count = 1
    for axis in axes:
        count *= lax.axis_size(axis)
    split = array.reshape(count, array.shape[0] // count, array.shape[1])
    return lax.all_to_all(split, axes, split_axis=0, concat_axis=0, tiled=True).reshape(array.shape)


def body(
    tokens, row_select, row_decay, row_gain, row_skip, row_in, row_out,
    col_select, col_decay, col_gain, col_skip, col_in, col_out, cotangent,
):
    mine = (lax.axis_index("frame") * lax.axis_size("seq_0") + lax.axis_index("seq_0")).reshape(1)
    x = tokens.reshape(TOKS)
    y = cotangent.reshape(TOKS)
    rsel = row_select.reshape(2, 128, 2 * STATE).swapaxes(1, 2)
    csel = col_select.reshape(2, 128, 2 * STATE).swapaxes(1, 2)
    rlam = row_decay.reshape(HEADS, 2, 128)
    clam = col_decay.reshape(HEADS, 2, 128)
    rgain = row_gain.reshape(1, WIDTH)
    cgain = col_gain.reshape(1, WIDTH)
    rskip = row_skip.reshape(1, HEADS)
    cskip = col_skip.reshape(1, HEADS)

    rlocal, rcols, rrows, rplaced, clocal, ccols, crows, cplaced, sent, message = call(
        start_kernel, "start",
        [Near((TOKS, F32)), Near((COLS, F32)), Near((ROWS, F32)), Near((PAIR, BF16)),
         Near((TOKS, F32)), Near((COLS, F32)), Near((ROWS, F32)), Near((PAIR, BF16)),
         Near((BIG, BF16)), Near((LOGGED, BF16))],
        [far(a) for a in
         (x, rsel, rlam, rskip, rgain, row_in, y, csel, clam, cskip, col_out)],
        left=range(11),
        scratch=[
            pltpu.VMEM(TOKS, BF16), pltpu.VMEM(SEL, BF16), pltpu.VMEM(LAM, F32),
            pltpu.VMEM((1, HEADS), F32), pltpu.VMEM((1, WIDTH), F32),
            pltpu.VMEM((WIDTH, WIDTH), BF16), pltpu.VMEM(TOKS, BF16), pltpu.VMEM(SEL, BF16),
            pltpu.VMEM(LAM, F32), pltpu.VMEM((1, HEADS), F32), pltpu.VMEM((WIDTH, WIDTH), BF16),
            pltpu.VMEM(TOKS, BF16), pltpu.VMEM(TOKS, BF16), pltpu.SemaphoreType.DMA((11,)),
        ],
    )
    message, mine = lax.optimization_barrier((message, mine))
    got = swapped(message, INNER)
    before, through, inner_logs, total = call(
        inner_first_kernel, "inner_first",
        [Near((MSG, F32)), Near((MSG, F32)), Near(((LINES, LOGS), BF16)), Near((LOGGED, BF16))],
        [near(got)], scratch=[pltpu.VMEM(MSG, F32)], flops=1e7,
    )
    groups = swapped(total, OUTER)
    outer_logs, down = call(
        outer_first_kernel, "outer_first", [Near(((LINES, LOGS), BF16)), Near((MSG, BF16))],
        [mine, near(groups), before, through], (0,), scratch=[pltpu.VMEM(MSG, F32)], flops=1e7,
    )
    got = near(swapped(down, INNER))
    rmixed, sending, gain = call(
        finish_kernel, "finish",
        [Near((TOKS, BF16)), Near((WIDE, BF16)), Near(((1, WIDTH), F32))],
        [rlocal, rcols, rplaced, got, near(row_out), clocal, ccols, cplaced, near(col_in),
         far(cgain), near(x), sent],
        left=(9,),
        scratch=[pltpu.SemaphoreType.DMA((1,))],
    )
    arrived = swapped(sending, SEQ)
    cx, cvalue, ry, rpulled, message = call(
        cross_kernel, "cross",
        [Near((TOKS, BF16)), Near((TOKS, BF16)), Near((TOKS, BF16)), Near((TOKS, BF16)),
         Near((MSG, BF16))],
        [near(arrived), rmixed, near(rsel), rcols, near(row_out), near(csel), ccols,
         gain, near(col_in)],
    )
    got = swapped(message, INNER)
    before, through, total = call(
        inner_second_kernel, "inner_second", [Near((MSG, F32)), Near((MSG, F32)), Near((MSG, BF16))],
        [near(got), inner_logs], scratch=[pltpu.VMEM(MSG, F32)], flops=1e7,
    )
    groups = swapped(total, OUTER)
    (down,) = call(
        outer_second_kernel, "outer_second", [Near((MSG, BF16))],
        [mine, near(groups), before, through, outer_logs], (0,),
        scratch=[pltpu.VMEM(MSG, F32)], flops=1e7,
    )
    got = swapped(down, INNER)
    clocal, cplaced = call(
        col_scan_kernel, "col_scan", [Near((TOKS, F32)), Near((PAIR, BF16))],
        [cvalue, far(csel), crows, ccols, far(cskip)],
    )
    rlocal, rplaced, gain = call(
        row_scan_back_kernel, "row_scan_back",
        [Near((TOKS, F32)), Near((PAIR, BF16)), Near(((1, WIDTH), F32))],
        [rpulled, far(rsel), rrows, rcols, far(rskip), far(rgain)],
    )
    mixed, grad = call(
        end_kernel, "end", [Far((TOKS, BF16)), Far((TOKS, BF16))],
        [near(got), cplaced, ccols, clocal, rplaced, rcols, rlocal, near(row_in),
         gain, near(x), ry, cx, far(col_out)],
        left=(12,), kept=(0, 1),
        scratch=[
            pltpu.VMEM((WIDTH, WIDTH), BF16), pltpu.VMEM(TOKS, BF16), pltpu.VMEM(TOKS, BF16),
            pltpu.SemaphoreType.DMA((6,)),
        ],
    )
    return mixed.reshape(cotangent.shape), grad.reshape(tokens.shape)


def solution(mesh):
    torus = Mesh(
        mesh.devices.reshape(4, 8, 2, mesh.shape["frame"]), ("seq_0", "seq_1", "seq_2", "frame")
    )
    tall = P("frame", SEQ, None, None)
    flat = P("frame", None, SEQ, None)
    in_specs = (tall, tall, flat, P(), P(), P(), P(), tall, flat, P(), P(), P(), P(), tall)
    return jax.shard_map(
        body, mesh=torus, in_specs=in_specs, out_specs=(tall, tall), check_vma=False
    )
```

```python
from functools import partial

import jax
import jax.numpy as jnp
from jax import lax
from jax.experimental import pallas as pl
from jax.experimental.pallas import tpu as pltpu
from jax.sharding import Mesh
from jax.sharding import PartitionSpec as P

SEQ = ("seq_0", "seq_1", "seq_2")
INNER = ("seq_2", "seq_1")
OUTER = ("seq_0", "frame")

EPSILON = 1e-05
LOG2E = 1.4426950408889634

TOK = 256
WIDTH = 512
HEADS = 8
PART = 64
STATE = 32
GROUP = 16
HALF = 256
LINES = GROUP * 8
LOGS = 128

F32 = jnp.float32
BF16 = jnp.bfloat16


def iota(shape, axis):
    return lax.broadcasted_iota(jnp.int32, shape, axis)


def onehot(mask):
    return mask.astype(F32).astype(BF16)


def dot(left, right, left_axis, right_axis):
    return lax.dot_general(
        left, right, (((left_axis,), (right_axis,)), ((), ())), preferred_element_type=F32
    )


def nn(left, right):
    return dot(left, right, 1, 0)


def nt(left, right):
    return dot(left, right, 1, 1)


def tn(left, right):
    return dot(left, right, 0, 0)


def parts_of(values, count):
    out = []
    rest = values
    for _ in range(count):
        piece = rest.astype(BF16)
        out.append(piece)
        rest = rest - piece.astype(F32)
    return out


def one_minus_exp(v):
    series = 1.0 - v * (1.0 / 9.0)
    for k in range(8, 1, -1):
        series = 1.0 - v * (1.0 / k) * series
    return jnp.where(v < 0.5, v * series, 1.0 - jnp.exp(-v))


def lam_of(lam_ref):
    return jnp.concatenate([lam_ref[:, 0, :], lam_ref[:, 1, :]], axis=1)


def turned_select(select_ref):
    return jnp.concatenate([select_ref[0], select_ref[1]], axis=1)


def block_terms(lam):
    upto = onehot(iota((TOK, TOK), 1) <= iota((TOK, TOK), 0))
    stacked = nt(jnp.concatenate(parts_of(lam, 3), axis=0), upto)
    cum = stacked[:8] + stacked[8:16] + stacked[16:]
    square = one_minus_exp(-2.0 * lam)
    ending = jnp.exp(cum[:, TOK - 1 :] - cum) * jnp.sqrt(square)
    log_inward = jnp.maximum(0.5 * jnp.log2(square), -500.0)
    rows = jnp.concatenate([cum * LOG2E, log_inward - cum * LOG2E], axis=0)
    cols = jnp.concatenate([rows, jnp.exp(cum), ending], axis=0).T
    return cum, rows, cols


OPENING = 16
ENDING = 24


def spread_heads(cols, offset):
    spread = onehot(
        iota((4 * HEADS, WIDTH), 1) // PART + offset == iota((4 * HEADS, WIDTH), 0)
    )
    return sum(nn(p, spread) for p in reversed(parts_of(cols, 2)))


def placed(select, offset, stream):
    at = iota((2 * STATE, 2 * LINES), 0)
    col = iota((2 * STATE, 2 * LINES), 1)
    row = col % LINES
    hit = (at == offset + 2 * (row // 8) + row % 2) & (row % 8 // 2 == col // LINES * 2 + stream)
    return tn(select, onehot(hit)).astype(BF16)


def carried_of(placed_pair, got):
    return jnp.concatenate(
        [nn(placed_pair[:, half * LINES : (half + 1) * LINES], got) for half in (0, 1)], axis=1
    )


def state_rows(weighted, select, offset, stream):
    at = iota((LINES, 2 * STATE), 1)
    row = iota((LINES, 2 * STATE), 0)
    out = None
    for half in (0, 1):
        hit = (at == offset + 2 * (row // 8) + row % 2) & (row % 8 // 2 == half * 2 + stream)
        rows = nn(onehot(hit), select).astype(BF16)
        part = nn(rows, weighted[:, half * HALF : (half + 1) * HALF])
        out = part if out is None else out + part
    return out


def normalized(x, gain):
    factor = lax.rsqrt(jnp.mean(x * x, axis=-1, keepdims=True) + EPSILON)
    return (x * factor * gain).astype(BF16)


def input_gradient(x, y, scaled):
    factor = lax.rsqrt(jnp.mean(x * x, axis=-1, keepdims=True) + EPSILON)
    inner = jnp.mean(scaled * x, axis=-1, keepdims=True)
    return (y + factor * scaled - x * (factor * factor * factor) * inner).astype(BF16)


def local_scan(values_ref, select, rows, cols, skip_ref, out_ref, backward):
    source = select[:STATE]
    target = select[STATE:]
    if backward:
        affinity = tn(source, target)
        left, right = cols[:, HEADS : 2 * HEADS], rows[:HEADS]
    else:
        affinity = tn(target, source)
        left, right = cols[:, :HEADS], rows[HEADS : 2 * HEADS]
    first = iota((128, 128), 0)
    second = iota((128, 128), 1)
    keep = second >= first if backward else second <= first
    lower = iota((1, 2 * PART), 1) < PART
    lo, hi = slice(0, 128), slice(128, 256)

    def tile(h, a, b):
        m = jnp.exp2(left[a, h : h + 1] + right[h : h + 1, b]) * affinity[a, b]
        return (jnp.where(keep, m, 0.0) if a == b else m).astype(BF16)

    def mixed(pair, rows, sources, parts):
        tiles = [tile(h, rows, b) for h in pair for b in sources]
        values = [part[b] for part in parts for b in sources]
        return nn(jnp.concatenate(tiles, axis=1), jnp.concatenate(values, axis=0))

    for h in range(0, HEADS, 2):
        span = slice(h * PART, (h + 2) * PART)
        v = values_ref[:, span].astype(F32)
        parts = [jnp.where(lower, v, 0.0).astype(BF16), jnp.where(lower, 0.0, v).astype(BF16)]
        skip = jnp.where(lower, skip_ref[0:1, h : h + 1], skip_ref[0:1, h + 1 : h + 2])
        top = mixed((h, h + 1), lo, (lo, hi) if backward else (lo,), parts)
        low = mixed((h, h + 1), hi, (hi,) if backward else (lo, hi), parts)
        out_ref[lo, span] = top + skip * v[lo]
        out_ref[hi, span] = low + skip * v[hi]


def row_target(token):
    column = token % 128
    return column // 2 * 8 + column % 2 * 2 + token // 128


def column_target(token):
    row = token % 128
    return row // 2 * 8 + token // 128 * 2 + row % 2


def to_message(tokens, target):
    off = iota((2 * TOK, TOK), 0) - target(iota((1, TOK), 1))
    left = nn(onehot(off == 0), tokens[:, :HALF])
    return (left + nn(onehot(off == 4), tokens[:, HALF:])).astype(BF16)


def from_message(message, target):
    off = iota((TOK, 2 * TOK), 1) - target(iota((TOK, 1), 0))
    return jnp.concatenate([nn(onehot(off == 0), message), nn(onehot(off == 4), message)], axis=1)


def start_kernel(
    x_hbm, rsel_hbm, rlam_hbm, rskip_hbm, gain_hbm, win_hbm,
    y_hbm, csel_hbm, clam_hbm, cskip_hbm, wout_hbm,
    rlocal_ref, rcols_ref, rrows_ref, rplaced_ref, clocal_ref, ccols_ref, crows_ref, cplaced_ref,
    sent_ref, message_ref,
    x_ref, rsel_ref, rlam_ref, rskip_ref, gain_ref, win_ref,
    y_ref, csel_ref, clam_ref, cskip_ref, wout_ref, value_ref, pulled_ref, sem,
):
    pairs = (
        (rlam_hbm, rlam_ref), (clam_hbm, clam_ref), (rsel_hbm, rsel_ref), (csel_hbm, csel_ref),
        (rskip_hbm, rskip_ref), (cskip_hbm, cskip_ref), (gain_hbm, gain_ref), (x_hbm, x_ref),
        (win_hbm, win_ref), (y_hbm, y_ref), (wout_hbm, wout_ref),
    )
    copies = [pltpu.make_async_copy(a, b, sem.at[i]) for i, (a, b) in enumerate(pairs)]
    for copy in copies:
        copy.start()
    for copy in copies[:7]:
        copy.wait()
    rcum, rrows, rcols = block_terms(lam_of(rlam_ref))
    ccum, crows, ccols = block_terms(lam_of(clam_ref))
    rrows_ref[...] = rrows
    rcols_ref[...] = rcols
    crows_ref[...] = crows
    ccols_ref[...] = ccols
    rsel = turned_select(rsel_ref)
    csel = turned_select(csel_ref)
    row = iota((8, HEADS), 0)
    head = iota((8, HEADS), 1)
    rlast = jnp.broadcast_to(rcum[:, TOK - 1 :], (HEADS, HEADS)).T
    clast = jnp.broadcast_to(ccum[:, TOK - 1 :], (HEADS, HEADS)).T
    logs = jnp.where(row % 4 < 2, rlast, clast)
    logs = jnp.where(head // 4 == row // 4, logs, 0.0)
    tile = None
    for k, piece in enumerate(parts_of(logs, 3)):
        place = onehot(iota((HEADS, LOGS), 1) == 4 * k + iota((HEADS, LOGS), 0) % 4)
        part = nn(piece, place)
        tile = part if tile is None else tile + part
    tile = tile.astype(BF16)
    for j in range(GROUP):
        message_ref[j * 8 : (j + 1) * 8, HALF:] = tile
    rplaced_ref[...] = placed(rsel, STATE, 0)
    cplaced_ref[...] = placed(csel, 0, 1)
    copies[7].wait()
    normed = normalized(x_ref[...].astype(F32), gain_ref[...])
    copies[8].wait()
    value = nn(normed, win_ref[...]).astype(BF16)
    value_ref[...] = value
    weighted = (value.astype(F32) * spread_heads(rcols, ENDING)).astype(BF16)
    first = state_rows(weighted, rsel, 0, 0)
    copies[9].wait()
    sent_ref[...] = to_message(y_ref[...], column_target)
    local_scan(value_ref, rsel, rrows, rcols, rskip_ref, rlocal_ref, False)
    copies[10].wait()
    pulled = nt(y_ref[...], wout_ref[...]).astype(BF16)
    pulled_ref[...] = pulled
    weighted = (pulled.astype(F32) * spread_heads(ccols, OPENING)).astype(BF16)
    second = state_rows(weighted, csel, STATE, 1)
    message_ref[:, :HALF] = (first + second).astype(BF16)
    local_scan(pulled_ref, csel, crows, ccols, cskip_ref, clocal_ref, True)


def logs_spread(tiles):
    spread = onehot(
        (iota((LOGS, HALF), 0) % 4 == iota((LOGS, HALF), 1) // PART) & (iota((LOGS, HALF), 0) < 12)
    )
    return nn(tiles, spread)


def inner_order(j):
    return j % 2 * 8 + j // 2


def outer_order(j):
    return j % 4 * 4 + j // 4


def tile_at(j):
    return slice(j * 8, (j + 1) * 8)


def stream_mask():
    return iota((8, HALF), 0) % 4 < 2


def pick(a_forward, forward, backward):
    first = stream_mask()
    return jnp.where(first, forward, backward) if a_forward else jnp.where(first, backward, forward)


def inner_pass(got_ref, logs_ref, a_forward, through_ref, before_ref, decay_ref):
    logs = logs_spread(logs_ref[...])
    decay_ref[...] = jnp.exp(logs)
    spots = [inner_order(j) for j in range(GROUP)]
    state = jnp.zeros((8, HALF), F32)
    gone = jnp.zeros((8, HALF), F32)
    forward = {}
    for j in spots:
        forward[j] = state, gone
        state = decay_ref[tile_at(j), :] * state + got_ref[tile_at(j), :HALF].astype(F32)
        gone = gone + logs[tile_at(j), :]
    ahead = state
    state = jnp.zeros((8, HALF), F32)
    gone = jnp.zeros((8, HALF), F32)
    for j in reversed(spots):
        before_ref[tile_at(j), :] = pick(a_forward, forward[j][0], state)
        through_ref[tile_at(j), :] = jnp.exp(pick(a_forward, forward[j][1], gone))
        state = decay_ref[tile_at(j), :] * state + got_ref[tile_at(j), :HALF].astype(F32)
        gone = gone + logs[tile_at(j), :]
    return pick(a_forward, ahead, state).astype(BF16)


def inner_first_kernel(got_ref, before_ref, through_ref, logs_ref, total_ref, decay_ref):
    logs_ref[...] = got_ref[:, HALF:]
    total = inner_pass(got_ref, logs_ref, True, through_ref, before_ref, decay_ref)
    compact = jnp.zeros((8, LOGS), F32)
    for j in range(GROUP):
        compact = compact + got_ref[tile_at(j), HALF:].astype(F32)
    compact = compact + pltpu.roll(compact, LOGS - 4, 1) + pltpu.roll(compact, LOGS - 8, 1)
    compact = jnp.where(iota((8, LOGS), 1) < 4, compact, 0.0)
    high = compact.astype(BF16).astype(F32)
    middle = (compact - high).astype(BF16).astype(F32)
    low = compact - high - middle
    compact = (high + pltpu.roll(middle, 4, 1) + pltpu.roll(low, 8, 1)).astype(BF16)
    for j in range(GROUP):
        total_ref[tile_at(j), :HALF] = total
        total_ref[tile_at(j), HALF:] = compact


def inner_second_kernel(got_ref, logs_ref, before_ref, through_ref, total_ref, decay_ref):
    total = inner_pass(got_ref, logs_ref, False, through_ref, before_ref, decay_ref)
    for j in range(GROUP):
        total_ref[tile_at(j), :] = total


def outer_pass(mine, got_ref, logs, a_forward, before_ref, through_ref, out_ref, decay_ref):
    decay_ref[...] = jnp.exp(logs_spread(logs))

    def step(state, at):
        return decay_ref[tile_at(at), :] * state + got_ref[tile_at(at), :HALF].astype(F32)

    state = jnp.zeros((8, HALF), F32)
    for j in range(GROUP):
        state = jnp.where(j < mine, step(state, outer_order(j)), state)
    ahead = state
    state = jnp.zeros((8, HALF), F32)
    for j in reversed(range(GROUP)):
        state = jnp.where(j > mine, step(state, outer_order(j)), state)
    both = pick(a_forward, ahead, state)
    for j in range(GROUP):
        at = tile_at(j)
        out_ref[at, :] = (through_ref[at, :] * both + before_ref[at, :]).astype(BF16)


def outer_first_kernel(
    mine_ref, got_ref, before_ref, through_ref, logs_ref, out_ref, decay_ref
):
    logs_ref[...] = got_ref[:, HALF:]
    outer_pass(
        mine_ref[0], got_ref, got_ref[:, HALF:], True, before_ref, through_ref, out_ref, decay_ref
    )


def outer_second_kernel(
    mine_ref, got_ref, before_ref, through_ref, logs_ref, out_ref, decay_ref
):
    outer_pass(
        mine_ref[0], got_ref, logs_ref[...], False, before_ref, through_ref, out_ref, decay_ref
    )


def finish_kernel(
    rlocal_ref, rcols_ref, rplaced_ref, got_ref, wout_ref,
    clocal_ref, ccols_ref, cplaced_ref, win_ref, gain_hbm, x_ref, sent_ref,
    mixed_ref, message_ref, gain_ref, sem,
):
    gain_in = pltpu.make_async_copy(gain_hbm, gain_ref, sem.at[0])
    gain_in.start()
    message_ref[:, HALF : 2 * HALF] = sent_ref[...]
    got = got_ref[...]
    carried = carried_of(rplaced_ref[...], got) * spread_heads(rcols_ref[...], OPENING)
    scanned = (rlocal_ref[...] + carried).astype(BF16)
    total = nn(scanned, wout_ref[...])
    carried = carried_of(cplaced_ref[...], got) * spread_heads(ccols_ref[...], ENDING)
    scanned = (clocal_ref[...] + carried).astype(BF16)
    returned = nt(scanned, win_ref[...])
    mixed = (x_ref[...].astype(F32) + total).astype(BF16)
    mixed_ref[...] = mixed
    message_ref[:, :HALF] = to_message(mixed, row_target)
    gain_in.wait()
    scaled = (gain_ref[...] * returned).astype(BF16)
    message_ref[:, 2 * HALF :] = to_message(scaled, column_target)


def cross_kernel(
    got_ref, mixed_ref, rsel_ref, rcols_ref, wout_ref, csel_ref, ccols_ref, gain_ref, win_ref,
    cx_ref, cvalue_ref, y_ref, pulled_ref, message_ref,
):
    off = iota((TOK, 2 * TOK), 1) - row_target(iota((TOK, 1), 0))
    low = nn(onehot(off == 0), got_ref[:, HALF:])
    high = nn(onehot(off == 4), got_ref[:, HALF:])
    y = jnp.concatenate([low[:, :HALF], high[:, :HALF]], axis=1)
    scaled = jnp.concatenate([low[:, HALF:], high[:, HALF:]], axis=1)
    y = input_gradient(mixed_ref[...].astype(F32), y, scaled)
    y_ref[...] = y
    pulled = nt(y, wout_ref[...]).astype(BF16)
    pulled_ref[...] = pulled
    weighted = (pulled.astype(F32) * spread_heads(rcols_ref[...], OPENING)).astype(BF16)
    first = state_rows(weighted, turned_select(rsel_ref), STATE, 0)
    x = from_message(got_ref[:, :HALF], column_target)
    cx_ref[...] = x.astype(BF16)
    value = nn(normalized(x, gain_ref[...]), win_ref[...]).astype(BF16)
    cvalue_ref[...] = value
    weighted = (value.astype(F32) * spread_heads(ccols_ref[...], ENDING)).astype(BF16)
    second = state_rows(weighted, turned_select(csel_ref), 0, 1)
    message_ref[...] = (first + second).astype(BF16)


def col_scan_kernel(
    value_ref, sel_ref, rows_ref, cols_ref, skip_ref, local_ref, placed_ref
):
    select = turned_select(sel_ref)
    placed_ref[...] = placed(select, STATE, 1)
    local_scan(value_ref, select, rows_ref[...], cols_ref[...], skip_ref, local_ref, False)


def row_scan_back_kernel(
    value_ref, sel_ref, rows_ref, cols_ref, skip_ref, gain_ref, local_ref, placed_ref, kept_ref
):
    kept_ref[...] = gain_ref[...]
    select = turned_select(sel_ref)
    placed_ref[...] = placed(select, 0, 0)
    local_scan(value_ref, select, rows_ref[...], cols_ref[...], skip_ref, local_ref, True)


def end_kernel(
    got_ref, cplaced_ref, ccols_ref, clocal_ref, rplaced_ref, rcols_ref, rlocal_ref, rwin_ref,
    gain_ref, x_ref, y_ref, cx_ref, cwout_hbm,
    mixed_hbm, grad_hbm, cwout_ref, mixed_ref, grad_ref, sem,
):
    def copy(a, b, i):
        return pltpu.make_async_copy(a, b, sem.at[i])

    cwout_in = copy(cwout_hbm, cwout_ref, 0)
    cwout_in.start()
    got = got_ref[...]
    carried = carried_of(rplaced_ref[...], got) * spread_heads(rcols_ref[...], ENDING)
    scanned = (rlocal_ref[...] + carried).astype(BF16)
    scaled = gain_ref[...] * nt(scanned, rwin_ref[...])
    grad_ref[...] = input_gradient(x_ref[...].astype(F32), y_ref[...].astype(F32), scaled)
    grad_out = copy(grad_ref, grad_hbm, 1)
    grad_out.start()
    carried = carried_of(cplaced_ref[...], got) * spread_heads(ccols_ref[...], OPENING)
    scanned = (clocal_ref[...] + carried).astype(BF16)
    cwout_in.wait()
    outs = [copy(mixed_ref.at[rows], mixed_hbm.at[rows], 2 + k) for k, rows in enumerate(QUARTERS)]
    for rows, out in zip(QUARTERS, outs):
        mixed = cx_ref[rows, :].astype(F32) + nn(scanned[rows, :], cwout_ref[...])
        mixed_ref[rows, :] = mixed.astype(BF16)
        out.start()
    grad_out.wait()
    for out in outs:
        out.wait()


QUARTERS = [slice(k * 64, (k + 1) * 64) for k in range(4)]

VM = pl.BlockSpec(memory_space=pltpu.VMEM)
SM = pl.BlockSpec(memory_space=pltpu.SMEM)
ANY = pl.BlockSpec(memory_space=pl.ANY)


class Near(tuple):
    pass


class Far(tuple):
    pass


def shaped(out):
    if isinstance(out, Near):
        return pltpu.VMEM(*out)
    if isinstance(out, Far):
        return pltpu.HBM(*out)
    return jax.ShapeDtypeStruct(*out)


def near(array):
    return pltpu.with_memory_space_constraint(array, pltpu.VMEM)


def far(array):
    return pltpu.with_memory_space_constraint(array, pltpu.HBM)


def call(kernel, name, outs, args, scalars=(), left=(), kept=(), scratch=(), flops=1e9):
    return pl.pallas_call(
        kernel,
        name=name,
        out_shape=[shaped(out) for out in outs],
        in_specs=[SM if i in scalars else ANY if i in left else VM for i in range(len(args))],
        out_specs=[ANY if i in kept else VM for i in range(len(outs))],
        scratch_shapes=list(scratch),
        compiler_params=pltpu.CompilerParams(vmem_limit_bytes=16 << 20),
        cost_estimate=pl.CostEstimate(flops=int(flops), bytes_accessed=1 << 20, transcendentals=0),
    )(*args)


TOKS = (TOK, WIDTH)
MSG = (LINES, HALF)
LOGGED = (LINES, HALF + LOGS)
PAIR = (TOK, 2 * LINES)
BIG = (2 * TOK, HALF)
WIDE = (2 * TOK, 3 * HALF)
ROWS = (2 * HEADS, TOK)
COLS = (TOK, 4 * HEADS)
SEL = (2, 2 * STATE, 128)
LAM = (HEADS, 2, 128)


def swapped(array, axes):
    count = 1
    for axis in axes:
        count *= lax.axis_size(axis)
    split = array.reshape(count, array.shape[0] // count, array.shape[1])
    return lax.all_to_all(split, axes, split_axis=0, concat_axis=0, tiled=True).reshape(array.shape)


def body(
    tokens, row_select, row_decay, row_gain, row_skip, row_in, row_out,
    col_select, col_decay, col_gain, col_skip, col_in, col_out, cotangent,
):
    mine = (lax.axis_index("frame") * lax.axis_size("seq_0") + lax.axis_index("seq_0")).reshape(1)
    x = tokens.reshape(TOKS)
    y = cotangent.reshape(TOKS)
    rsel = row_select.reshape(2, 128, 2 * STATE).swapaxes(1, 2)
    csel = col_select.reshape(2, 128, 2 * STATE).swapaxes(1, 2)
    rlam = row_decay.reshape(HEADS, 2, 128)
    clam = col_decay.reshape(HEADS, 2, 128)
    rgain = row_gain.reshape(1, WIDTH)
    cgain = col_gain.reshape(1, WIDTH)
    rskip = row_skip.reshape(1, HEADS)
    cskip = col_skip.reshape(1, HEADS)

    rlocal, rcols, rrows, rplaced, clocal, ccols, crows, cplaced, sent, message = call(
        start_kernel, "start",
        [Near((TOKS, F32)), Near((COLS, F32)), Near((ROWS, F32)), Near((PAIR, BF16)),
         Near((TOKS, F32)), Near((COLS, F32)), Near((ROWS, F32)), Near((PAIR, BF16)),
         Near((BIG, BF16)), Near((LOGGED, BF16))],
        [far(a) for a in
         (x, rsel, rlam, rskip, rgain, row_in, y, csel, clam, cskip, col_out)],
        left=range(11),
        scratch=[
            pltpu.VMEM(TOKS, BF16), pltpu.VMEM(SEL, BF16), pltpu.VMEM(LAM, F32),
            pltpu.VMEM((1, HEADS), F32), pltpu.VMEM((1, WIDTH), F32),
            pltpu.VMEM((WIDTH, WIDTH), BF16), pltpu.VMEM(TOKS, BF16), pltpu.VMEM(SEL, BF16),
            pltpu.VMEM(LAM, F32), pltpu.VMEM((1, HEADS), F32), pltpu.VMEM((WIDTH, WIDTH), BF16),
            pltpu.VMEM(TOKS, BF16), pltpu.VMEM(TOKS, BF16), pltpu.SemaphoreType.DMA((11,)),
        ],
    )
    message, mine = lax.optimization_barrier((message, mine))
    got = swapped(message, INNER)
    before, through, inner_logs, total = call(
        inner_first_kernel, "inner_first",
        [Near((MSG, F32)), Near((MSG, F32)), Near(((LINES, LOGS), BF16)), Near((LOGGED, BF16))],
        [near(got)], scratch=[pltpu.VMEM(MSG, F32)], flops=1e7,
    )
    groups = swapped(total, OUTER)
    outer_logs, down = call(
        outer_first_kernel, "outer_first", [Near(((LINES, LOGS), BF16)), Near((MSG, BF16))],
        [mine, near(groups), before, through], (0,), scratch=[pltpu.VMEM(MSG, F32)], flops=1e7,
    )
    got = near(swapped(down, INNER))
    rmixed, sending, gain = call(
        finish_kernel, "finish",
        [Near((TOKS, BF16)), Near((WIDE, BF16)), Near(((1, WIDTH), F32))],
        [rlocal, rcols, rplaced, got, near(row_out), clocal, ccols, cplaced, near(col_in),
         far(cgain), near(x), sent],
        left=(9,),
        scratch=[pltpu.SemaphoreType.DMA((1,))],
    )
    arrived = swapped(sending, SEQ)
    cx, cvalue, ry, rpulled, message = call(
        cross_kernel, "cross",
        [Near((TOKS, BF16)), Near((TOKS, BF16)), Near((TOKS, BF16)), Near((TOKS, BF16)),
         Near((MSG, BF16))],
        [near(arrived), rmixed, near(rsel), rcols, near(row_out), near(csel), ccols,
         gain, near(col_in)],
    )
    got = swapped(message, INNER)
    before, through, total = call(
        inner_second_kernel, "inner_second", [Near((MSG, F32)), Near((MSG, F32)), Near((MSG, BF16))],
        [near(got), inner_logs], scratch=[pltpu.VMEM(MSG, F32)], flops=1e7,
    )
    groups = swapped(total, OUTER)
    (down,) = call(
        outer_second_kernel, "outer_second", [Near((MSG, BF16))],
        [mine, near(groups), before, through, outer_logs], (0,),
        scratch=[pltpu.VMEM(MSG, F32)], flops=1e7,
    )
    got = swapped(down, INNER)
    clocal, cplaced = call(
        col_scan_kernel, "col_scan", [Near((TOKS, F32)), Near((PAIR, BF16))],
        [cvalue, far(csel), crows, ccols, far(cskip)],
    )
    rlocal, rplaced, gain = call(
        row_scan_back_kernel, "row_scan_back",
        [Near((TOKS, F32)), Near((PAIR, BF16)), Near(((1, WIDTH), F32))],
        [rpulled, far(rsel), rrows, rcols, far(rskip), far(rgain)],
    )
    mixed, grad = call(
        end_kernel, "end", [Far((TOKS, BF16)), Far((TOKS, BF16))],
        [near(got), cplaced, ccols, clocal, rplaced, rcols, rlocal, near(row_in),
         gain, near(x), ry, cx, far(col_out)],
        left=(12,), kept=(0, 1),
        scratch=[
            pltpu.VMEM((WIDTH, WIDTH), BF16), pltpu.VMEM(TOKS, BF16), pltpu.VMEM(TOKS, BF16),
            pltpu.SemaphoreType.DMA((6,)),
        ],
    )
    return mixed.reshape(cotangent.shape), grad.reshape(tokens.shape)


def solution(mesh):
    torus = Mesh(
        mesh.devices.reshape(4, 8, 2, mesh.shape["frame"]), ("seq_0", "seq_1", "seq_2", "frame")
    )
    tall = P("frame", SEQ, None, None)
    flat = P("frame", None, SEQ, None)
    in_specs = (tall, tall, flat, P(), P(), P(), P(), tall, flat, P(), P(), P(), P(), tall)
    return jax.shard_map(
        body, mesh=torus, in_specs=in_specs, out_specs=(tall, tall), check_vma=False
    )
```

```python
from functools import partial

import jax
import jax.numpy as jnp
from jax import lax
from jax.experimental import pallas as pl
from jax.experimental.pallas import tpu as pltpu
from jax.sharding import Mesh
from jax.sharding import PartitionSpec as P

SEQ = ("seq_0", "seq_1", "seq_2")
INNER = ("seq_2", "seq_1")
OUTER = ("seq_0", "frame")

EPSILON = 1e-05
LOG2E = 1.4426950408889634

TOK = 256
WIDTH = 512
HEADS = 8
PART = 64
STATE = 32
GROUP = 16
HALF = 256
LINES = GROUP * 8
LOGS = 128

F32 = jnp.float32
BF16 = jnp.bfloat16


def iota(shape, axis):
    return lax.broadcasted_iota(jnp.int32, shape, axis)


def onehot(mask):
    return mask.astype(F32).astype(BF16)


def dot(left, right, left_axis, right_axis):
    return lax.dot_general(
        left, right, (((left_axis,), (right_axis,)), ((), ())), preferred_element_type=F32
    )


def nn(left, right):
    return dot(left, right, 1, 0)


def nt(left, right):
    return dot(left, right, 1, 1)


def tn(left, right):
    return dot(left, right, 0, 0)


def parts_of(values, count):
    out = []
    rest = values
    for _ in range(count):
        piece = rest.astype(BF16)
        out.append(piece)
        rest = rest - piece.astype(F32)
    return out


def one_minus_exp(v):
    series = 1.0 - v * (1.0 / 9.0)
    for k in range(8, 1, -1):
        series = 1.0 - v * (1.0 / k) * series
    return jnp.where(v < 0.5, v * series, 1.0 - jnp.exp(-v))


def lam_of(lam_ref):
    return jnp.concatenate([lam_ref[:, 0, :], lam_ref[:, 1, :]], axis=1)


def turned_select(select_ref):
    return jnp.concatenate([select_ref[0], select_ref[1]], axis=1)


def block_terms(lam):
    upto = onehot(iota((TOK, TOK), 1) <= iota((TOK, TOK), 0))
    stacked = nt(jnp.concatenate(parts_of(lam, 3), axis=0), upto)
    cum = stacked[:8] + stacked[8:16] + stacked[16:]
    square = one_minus_exp(-2.0 * lam)
    ending = jnp.exp(cum[:, TOK - 1 :] - cum) * jnp.sqrt(square)
    log_inward = jnp.maximum(0.5 * jnp.log2(square), -500.0)
    rows = jnp.concatenate([cum * LOG2E, log_inward - cum * LOG2E], axis=0)
    cols = jnp.concatenate([rows, jnp.exp(cum), ending], axis=0).T
    return cum, rows, cols


OPENING = 16
ENDING = 24


def spread_heads(cols, offset):
    spread = onehot(
        iota((4 * HEADS, WIDTH), 1) // PART + offset == iota((4 * HEADS, WIDTH), 0)
    )
    return sum(nn(p, spread) for p in reversed(parts_of(cols, 2)))


def placed(select, offset, stream):
    at = iota((2 * STATE, 2 * LINES), 0)
    col = iota((2 * STATE, 2 * LINES), 1)
    row = col % LINES
    hit = (at == offset + 2 * (row // 8) + row % 2) & (row % 8 // 2 == col // LINES * 2 + stream)
    return tn(select, onehot(hit)).astype(BF16)


def carried_of(placed_pair, got):
    return jnp.concatenate(
        [nn(placed_pair[:, half * LINES : (half + 1) * LINES], got) for half in (0, 1)], axis=1
    )


def state_rows(weighted, select, offset, stream):
    at = iota((LINES, 2 * STATE), 1)
    row = iota((LINES, 2 * STATE), 0)
    out = None
    for half in (0, 1):
        hit = (at == offset + 2 * (row // 8) + row % 2) & (row % 8 // 2 == half * 2 + stream)
        rows = nn(onehot(hit), select).astype(BF16)
        part = nn(rows, weighted[:, half * HALF : (half + 1) * HALF])
        out = part if out is None else out + part
    return out


def normalized(x, gain):
    factor = lax.rsqrt(jnp.mean(x * x, axis=-1, keepdims=True) + EPSILON)
    return (x * factor * gain).astype(BF16)


def input_gradient(x, y, scaled):
    factor = lax.rsqrt(jnp.mean(x * x, axis=-1, keepdims=True) + EPSILON)
    inner = jnp.mean(scaled * x, axis=-1, keepdims=True)
    return (y + factor * scaled - x * (factor * factor * factor) * inner).astype(BF16)


def local_scan(values_ref, select, rows, cols, skip_ref, out_ref, backward):
    source = select[:STATE]
    target = select[STATE:]
    if backward:
        affinity = tn(source, target)
        left, right = cols[:, HEADS : 2 * HEADS], rows[:HEADS]
    else:
        affinity = tn(target, source)
        left, right = cols[:, :HEADS], rows[HEADS : 2 * HEADS]
    first = iota((128, 128), 0)
    second = iota((128, 128), 1)
    keep = second >= first if backward else second <= first
    lower = iota((1, 2 * PART), 1) < PART
    lo, hi = slice(0, 128), slice(128, 256)

    def tile(h, a, b):
        m = jnp.exp2(left[a, h : h + 1] + right[h : h + 1, b]) * affinity[a, b]
        return (jnp.where(keep, m, 0.0) if a == b else m).astype(BF16)

    def mixed(pair, rows, sources, parts):
        tiles = [tile(h, rows, b) for h in pair for b in sources]
        values = [part[b] for part in parts for b in sources]
        return nn(jnp.concatenate(tiles, axis=1), jnp.concatenate(values, axis=0))

    for h in range(0, HEADS, 2):
        span = slice(h * PART, (h + 2) * PART)
        v = values_ref[:, span].astype(F32)
        parts = [jnp.where(lower, v, 0.0).astype(BF16), jnp.where(lower, 0.0, v).astype(BF16)]
        skip = jnp.where(lower, skip_ref[0:1, h : h + 1], skip_ref[0:1, h + 1 : h + 2])
        top = mixed((h, h + 1), lo, (lo, hi) if backward else (lo,), parts)
        low = mixed((h, h + 1), hi, (hi,) if backward else (lo, hi), parts)
        out_ref[lo, span] = top + skip * v[lo]
        out_ref[hi, span] = low + skip * v[hi]


def row_target(token):
    column = token % 128
    return column // 2 * 8 + column % 2 * 2 + token // 128


def column_target(token):
    row = token % 128
    return row // 2 * 8 + token // 128 * 2 + row % 2


def to_message(tokens, target):
    off = iota((2 * TOK, TOK), 0) - target(iota((1, TOK), 1))
    left = nn(onehot(off == 0), tokens[:, :HALF])
    return (left + nn(onehot(off == 4), tokens[:, HALF:])).astype(BF16)


def from_message(message, target):
    off = iota((TOK, 2 * TOK), 1) - target(iota((TOK, 1), 0))
    return jnp.concatenate([nn(onehot(off == 0), message), nn(onehot(off == 4), message)], axis=1)


def start_kernel(
    x_hbm, rsel_hbm, rlam_hbm, rskip_hbm, gain_hbm, win_hbm,
    y_hbm, csel_hbm, clam_hbm, cskip_hbm, wout_hbm,
    rlocal_ref, rcols_ref, rrows_ref, rplaced_ref, clocal_ref, ccols_ref, crows_ref, cplaced_ref,
    sent_ref, message_ref,
    x_ref, rsel_ref, rlam_ref, rskip_ref, gain_ref, win_ref,
    y_ref, csel_ref, clam_ref, cskip_ref, wout_ref, value_ref, pulled_ref, sem,
):
    pairs = (
        (rlam_hbm, rlam_ref), (clam_hbm, clam_ref), (rsel_hbm, rsel_ref), (csel_hbm, csel_ref),
        (rskip_hbm, rskip_ref), (cskip_hbm, cskip_ref), (gain_hbm, gain_ref), (x_hbm, x_ref),
        (win_hbm, win_ref), (y_hbm, y_ref), (wout_hbm, wout_ref),
    )
    copies = [pltpu.make_async_copy(a, b, sem.at[i]) for i, (a, b) in enumerate(pairs)]
    for copy in copies:
        copy.start()
    for copy in copies[:7]:
        copy.wait()
    rcum, rrows, rcols = block_terms(lam_of(rlam_ref))
    ccum, crows, ccols = block_terms(lam_of(clam_ref))
    rrows_ref[...] = rrows
    rcols_ref[...] = rcols
    crows_ref[...] = crows
    ccols_ref[...] = ccols
    rsel = turned_select(rsel_ref)
    csel = turned_select(csel_ref)
    row = iota((8, HEADS), 0)
    head = iota((8, HEADS), 1)
    rlast = jnp.broadcast_to(rcum[:, TOK - 1 :], (HEADS, HEADS)).T
    clast = jnp.broadcast_to(ccum[:, TOK - 1 :], (HEADS, HEADS)).T
    logs = jnp.where(row % 4 < 2, rlast, clast)
    logs = jnp.where(head // 4 == row // 4, logs, 0.0)
    tile = None
    for k, piece in enumerate(parts_of(logs, 3)):
        place = onehot(iota((HEADS, LOGS), 1) == 4 * k + iota((HEADS, LOGS), 0) % 4)
        part = nn(piece, place)
        tile = part if tile is None else tile + part
    tile = tile.astype(BF16)
    for j in range(GROUP):
        message_ref[j * 8 : (j + 1) * 8, HALF:] = tile
    rplaced_ref[...] = placed(rsel, STATE, 0)
    cplaced_ref[...] = placed(csel, 0, 1)
    copies[7].wait()
    normed = normalized(x_ref[...].astype(F32), gain_ref[...])
    copies[8].wait()
    value = nn(normed, win_ref[...]).astype(BF16)
    value_ref[...] = value
    weighted = (value.astype(F32) * spread_heads(rcols, ENDING)).astype(BF16)
    first = state_rows(weighted, rsel, 0, 0)
    copies[9].wait()
    sent_ref[...] = to_message(y_ref[...], column_target)
    local_scan(value_ref, rsel, rrows, rcols, rskip_ref, rlocal_ref, False)
    copies[10].wait()
    pulled = nt(y_ref[...], wout_ref[...]).astype(BF16)
    pulled_ref[...] = pulled
    weighted = (pulled.astype(F32) * spread_heads(ccols, OPENING)).astype(BF16)
    second = state_rows(weighted, csel, STATE, 1)
    message_ref[:, :HALF] = (first + second).astype(BF16)
    local_scan(pulled_ref, csel, crows, ccols, cskip_ref, clocal_ref, True)


def logs_spread(tiles):
    spread = onehot(
        (iota((LOGS, HALF), 0) % 4 == iota((LOGS, HALF), 1) // PART) & (iota((LOGS, HALF), 0) < 12)
    )
    return nn(tiles, spread)


def inner_order(j):
    return j % 2 * 8 + j // 2


def outer_order(j):
    return j % 4 * 4 + j // 4


def tile_at(j):
    return slice(j * 8, (j + 1) * 8)


def stream_mask():
    return iota((8, HALF), 0) % 4 < 2


def pick(a_forward, forward, backward):
    first = stream_mask()
    return jnp.where(first, forward, backward) if a_forward else jnp.where(first, backward, forward)


def inner_pass(got_ref, logs_ref, a_forward, through_ref, before_ref, decay_ref):
    logs = logs_spread(logs_ref[...])
    decay_ref[...] = jnp.exp(logs)
    spots = [inner_order(j) for j in range(GROUP)]
    state = jnp.zeros((8, HALF), F32)
    gone = jnp.zeros((8, HALF), F32)
    forward = {}
    for j in spots:
        forward[j] = state, gone
        state = decay_ref[tile_at(j), :] * state + got_ref[tile_at(j), :HALF].astype(F32)
        gone = gone + logs[tile_at(j), :]
    ahead = state
    state = jnp.zeros((8, HALF), F32)
    gone = jnp.zeros((8, HALF), F32)
    for j in reversed(spots):
        before_ref[tile_at(j), :] = pick(a_forward, forward[j][0], state)
        through_ref[tile_at(j), :] = jnp.exp(pick(a_forward, forward[j][1], gone))
        state = decay_ref[tile_at(j), :] * state + got_ref[tile_at(j), :HALF].astype(F32)
        gone = gone + logs[tile_at(j), :]
    return pick(a_forward, ahead, state).astype(BF16)


def inner_first_kernel(got_ref, before_ref, through_ref, logs_ref, total_ref, decay_ref):
    logs_ref[...] = got_ref[:, HALF:]
    total = inner_pass(got_ref, logs_ref, True, through_ref, before_ref, decay_ref)
    compact = jnp.zeros((8, LOGS), F32)
    for j in range(GROUP):
        compact = compact + got_ref[tile_at(j), HALF:].astype(F32)
    compact = compact + pltpu.roll(compact, LOGS - 4, 1) + pltpu.roll(compact, LOGS - 8, 1)
    compact = jnp.where(iota((8, LOGS), 1) < 4, compact, 0.0)
    high = compact.astype(BF16).astype(F32)
    middle = (compact - high).astype(BF16).astype(F32)
    low = compact - high - middle
    compact = (high + pltpu.roll(middle, 4, 1) + pltpu.roll(low, 8, 1)).astype(BF16)
    for j in range(GROUP):
        total_ref[tile_at(j), :HALF] = total
        total_ref[tile_at(j), HALF:] = compact


def inner_second_kernel(got_ref, logs_ref, before_ref, through_ref, total_ref, decay_ref):
    total = inner_pass(got_ref, logs_ref, False, through_ref, before_ref, decay_ref)
    for j in range(GROUP):
        total_ref[tile_at(j), :] = total


def outer_pass(mine, got_ref, logs, a_forward, before_ref, through_ref, out_ref, decay_ref):
    decay_ref[...] = jnp.exp(logs_spread(logs))

    def step(state, at):
        return decay_ref[tile_at(at), :] * state + got_ref[tile_at(at), :HALF].astype(F32)

    state = jnp.zeros((8, HALF), F32)
    for j in range(GROUP):
        state = jnp.where(j < mine, step(state, outer_order(j)), state)
    ahead = state
    state = jnp.zeros((8, HALF), F32)
    for j in reversed(range(GROUP)):
        state = jnp.where(j > mine, step(state, outer_order(j)), state)
    both = pick(a_forward, ahead, state)
    for j in range(GROUP):
        at = tile_at(j)
        out_ref[at, :] = (through_ref[at, :] * both + before_ref[at, :]).astype(BF16)


def outer_first_kernel(
    mine_ref, got_ref, before_ref, through_ref, logs_ref, out_ref, decay_ref
):
    logs_ref[...] = got_ref[:, HALF:]
    outer_pass(
        mine_ref[0], got_ref, got_ref[:, HALF:], True, before_ref, through_ref, out_ref, decay_ref
    )


def outer_second_kernel(
    mine_ref, got_ref, before_ref, through_ref, logs_ref, out_ref, decay_ref
):
    outer_pass(
        mine_ref[0], got_ref, logs_ref[...], False, before_ref, through_ref, out_ref, decay_ref
    )


def finish_kernel(
    rlocal_ref, rcols_ref, rplaced_ref, got_ref, wout_ref,
    clocal_ref, ccols_ref, cplaced_ref, win_ref, gain_hbm, x_ref, sent_ref,
    mixed_ref, message_ref, gain_ref, sem,
):
    gain_in = pltpu.make_async_copy(gain_hbm, gain_ref, sem.at[0])
    gain_in.start()
    message_ref[:, HALF : 2 * HALF] = sent_ref[...]
    got = got_ref[...]
    carried = carried_of(rplaced_ref[...], got) * spread_heads(rcols_ref[...], OPENING)
    scanned = (rlocal_ref[...] + carried).astype(BF16)
    total = nn(scanned, wout_ref[...])
    carried = carried_of(cplaced_ref[...], got) * spread_heads(ccols_ref[...], ENDING)
    scanned = (clocal_ref[...] + carried).astype(BF16)
    returned = nt(scanned, win_ref[...])
    mixed = (x_ref[...].astype(F32) + total).astype(BF16)
    mixed_ref[...] = mixed
    message_ref[:, :HALF] = to_message(mixed, row_target)
    gain_in.wait()
    scaled = (gain_ref[...] * returned).astype(BF16)
    message_ref[:, 2 * HALF :] = to_message(scaled, column_target)


def cross_kernel(
    got_ref, mixed_ref, rsel_ref, rcols_ref, rrows_ref, rskip_hbm, wout_ref,
    csel_ref, ccols_ref, crows_ref, cskip_hbm, gain_ref, win_ref, rgain_hbm,
    cx_ref, y_ref, rlocal_ref, rplaced_ref, clocal_ref, cplaced_ref, rgain_ref, message_ref,
    rskip_ref, cskip_ref, value_ref, pulled_ref, sem,
):
    pairs = ((rskip_hbm, rskip_ref), (cskip_hbm, cskip_ref), (rgain_hbm, rgain_ref))
    copies = [pltpu.make_async_copy(a, b, sem.at[i]) for i, (a, b) in enumerate(pairs)]
    for copy in copies:
        copy.start()
    y = from_message(got_ref[:, HALF : 2 * HALF], row_target)
    scaled = from_message(got_ref[:, 2 * HALF :], row_target)
    y = input_gradient(mixed_ref[...].astype(F32), y, scaled)
    y_ref[...] = y
    pulled = nt(y, wout_ref[...]).astype(BF16)
    pulled_ref[...] = pulled
    weighted = (pulled.astype(F32) * spread_heads(rcols_ref[...], OPENING)).astype(BF16)
    first = state_rows(weighted, turned_select(rsel_ref), STATE, 0)
    x = from_message(got_ref[:, :HALF], column_target)
    cx_ref[...] = x.astype(BF16)
    value = nn(normalized(x, gain_ref[...]), win_ref[...]).astype(BF16)
    value_ref[...] = value
    weighted = (value.astype(F32) * spread_heads(ccols_ref[...], ENDING)).astype(BF16)
    second = state_rows(weighted, turned_select(csel_ref), 0, 1)
    message_ref[...] = (first + second).astype(BF16)
    rsel = turned_select(rsel_ref)
    csel = turned_select(csel_ref)
    rplaced_ref[...] = placed(rsel, 0, 0)
    cplaced_ref[...] = placed(csel, STATE, 1)
    for copy in copies:
        copy.wait()
    local_scan(pulled_ref, rsel, rrows_ref[...], rcols_ref[...], rskip_ref, rlocal_ref, True)
    local_scan(value_ref, csel, crows_ref[...], ccols_ref[...], cskip_ref, clocal_ref, False)


def end_kernel(
    got_ref, cplaced_ref, ccols_ref, clocal_ref, rplaced_ref, rcols_ref, rlocal_ref, rwin_ref,
    gain_ref, x_ref, y_ref, cx_ref, cwout_hbm,
    mixed_hbm, grad_hbm, cwout_ref, mixed_ref, grad_ref, sem,
):
    def copy(a, b, i):
        return pltpu.make_async_copy(a, b, sem.at[i])

    cwout_in = copy(cwout_hbm, cwout_ref, 0)
    cwout_in.start()
    got = got_ref[...]
    carried = carried_of(rplaced_ref[...], got) * spread_heads(rcols_ref[...], ENDING)
    scanned = (rlocal_ref[...] + carried).astype(BF16)
    scaled = gain_ref[...] * nt(scanned, rwin_ref[...])
    grad_ref[...] = input_gradient(x_ref[...].astype(F32), y_ref[...].astype(F32), scaled)
    grad_out = copy(grad_ref, grad_hbm, 1)
    grad_out.start()
    carried = carried_of(cplaced_ref[...], got) * spread_heads(ccols_ref[...], OPENING)
    scanned = (clocal_ref[...] + carried).astype(BF16)
    cwout_in.wait()
    outs = [copy(mixed_ref.at[rows], mixed_hbm.at[rows], 2 + k) for k, rows in enumerate(QUARTERS)]
    for rows, out in zip(QUARTERS, outs):
        mixed = cx_ref[rows, :].astype(F32) + nn(scanned[rows, :], cwout_ref[...])
        mixed_ref[rows, :] = mixed.astype(BF16)
        out.start()
    grad_out.wait()
    for out in outs:
        out.wait()


QUARTERS = [slice(k * 64, (k + 1) * 64) for k in range(4)]

VM = pl.BlockSpec(memory_space=pltpu.VMEM)
SM = pl.BlockSpec(memory_space=pltpu.SMEM)
ANY = pl.BlockSpec(memory_space=pl.ANY)


class Near(tuple):
    pass


class Far(tuple):
    pass


def shaped(out):
    if isinstance(out, Near):
        return pltpu.VMEM(*out)
    if isinstance(out, Far):
        return pltpu.HBM(*out)
    return jax.ShapeDtypeStruct(*out)


def near(array):
    return pltpu.with_memory_space_constraint(array, pltpu.VMEM)


def far(array):
    return pltpu.with_memory_space_constraint(array, pltpu.HBM)


def call(kernel, name, outs, args, scalars=(), left=(), kept=(), scratch=(), flops=1e9):
    return pl.pallas_call(
        kernel,
        name=name,
        out_shape=[shaped(out) for out in outs],
        in_specs=[SM if i in scalars else ANY if i in left else VM for i in range(len(args))],
        out_specs=[ANY if i in kept else VM for i in range(len(outs))],
        scratch_shapes=list(scratch),
        compiler_params=pltpu.CompilerParams(vmem_limit_bytes=16 << 20),
        cost_estimate=pl.CostEstimate(flops=int(flops), bytes_accessed=1 << 20, transcendentals=0),
    )(*args)


TOKS = (TOK, WIDTH)
MSG = (LINES, HALF)
LOGGED = (LINES, HALF + LOGS)
PAIR = (TOK, 2 * LINES)
BIG = (2 * TOK, HALF)
WIDE = (2 * TOK, 3 * HALF)
ROWS = (2 * HEADS, TOK)
COLS = (TOK, 4 * HEADS)
SEL = (2, 2 * STATE, 128)
LAM = (HEADS, 2, 128)


def swapped(array, axes):
    count = 1
    for axis in axes:
        count *= lax.axis_size(axis)
    split = array.reshape(count, array.shape[0] // count, array.shape[1])
    return lax.all_to_all(split, axes, split_axis=0, concat_axis=0, tiled=True).reshape(array.shape)


def body(
    tokens, row_select, row_decay, row_gain, row_skip, row_in, row_out,
    col_select, col_decay, col_gain, col_skip, col_in, col_out, cotangent,
):
    mine = (lax.axis_index("frame") * lax.axis_size("seq_0") + lax.axis_index("seq_0")).reshape(1)
    x = tokens.reshape(TOKS)
    y = cotangent.reshape(TOKS)
    rsel = row_select.reshape(2, 128, 2 * STATE).swapaxes(1, 2)
    csel = col_select.reshape(2, 128, 2 * STATE).swapaxes(1, 2)
    rlam = row_decay.reshape(HEADS, 2, 128)
    clam = col_decay.reshape(HEADS, 2, 128)
    rgain = row_gain.reshape(1, WIDTH)
    cgain = col_gain.reshape(1, WIDTH)
    rskip = row_skip.reshape(1, HEADS)
    cskip = col_skip.reshape(1, HEADS)

    rlocal, rcols, rrows, rplaced, clocal, ccols, crows, cplaced, sent, message = call(
        start_kernel, "start",
        [Near((TOKS, F32)), Near((COLS, F32)), Near((ROWS, F32)), Near((PAIR, BF16)),
         Near((TOKS, F32)), Near((COLS, F32)), Near((ROWS, F32)), Near((PAIR, BF16)),
         Near((BIG, BF16)), Near((LOGGED, BF16))],
        [far(a) for a in
         (x, rsel, rlam, rskip, rgain, row_in, y, csel, clam, cskip, col_out)],
        left=range(11),
        scratch=[
            pltpu.VMEM(TOKS, BF16), pltpu.VMEM(SEL, BF16), pltpu.VMEM(LAM, F32),
            pltpu.VMEM((1, HEADS), F32), pltpu.VMEM((1, WIDTH), F32),
            pltpu.VMEM((WIDTH, WIDTH), BF16), pltpu.VMEM(TOKS, BF16), pltpu.VMEM(SEL, BF16),
            pltpu.VMEM(LAM, F32), pltpu.VMEM((1, HEADS), F32), pltpu.VMEM((WIDTH, WIDTH), BF16),
            pltpu.VMEM(TOKS, BF16), pltpu.VMEM(TOKS, BF16), pltpu.SemaphoreType.DMA((11,)),
        ],
    )
    message, mine = lax.optimization_barrier((message, mine))
    got = swapped(message, INNER)
    before, through, inner_logs, total = call(
        inner_first_kernel, "inner_first",
        [Near((MSG, F32)), Near((MSG, F32)), Near(((LINES, LOGS), BF16)), Near((LOGGED, BF16))],
        [near(got)], scratch=[pltpu.VMEM(MSG, F32)], flops=1e7,
    )
    groups = swapped(total, OUTER)
    outer_logs, down = call(
        outer_first_kernel, "outer_first", [Near(((LINES, LOGS), BF16)), Near((MSG, BF16))],
        [mine, near(groups), before, through], (0,), scratch=[pltpu.VMEM(MSG, F32)], flops=1e7,
    )
    got = near(swapped(down, INNER))
    rmixed, sending, gain = call(
        finish_kernel, "finish",
        [Near((TOKS, BF16)), Near((WIDE, BF16)), Near(((1, WIDTH), F32))],
        [rlocal, rcols, rplaced, got, near(row_out), clocal, ccols, cplaced, near(col_in),
         far(cgain), near(x), sent],
        left=(9,),
        scratch=[pltpu.SemaphoreType.DMA((1,))],
    )
    arrived = swapped(sending, SEQ)
    cx, ry, rlocal, rplaced, clocal, cplaced, gain, message = call(
        cross_kernel, "cross",
        [Near((TOKS, BF16)), Near((TOKS, BF16)), Near((TOKS, F32)), Near((PAIR, BF16)),
         Near((TOKS, F32)), Near((PAIR, BF16)), Near(((1, WIDTH), F32)), Near((MSG, BF16))],
        [near(arrived), rmixed, near(rsel), rcols, rrows, far(rskip), near(row_out),
         near(csel), ccols, crows, far(cskip), gain, near(col_in), far(rgain)],
        left=(5, 10, 13),
        scratch=[
            pltpu.VMEM((1, HEADS), F32), pltpu.VMEM((1, HEADS), F32), pltpu.VMEM(TOKS, BF16),
            pltpu.VMEM(TOKS, BF16), pltpu.SemaphoreType.DMA((3,)),
        ],
    )
    got = swapped(message, INNER)
    before, through, total = call(
        inner_second_kernel, "inner_second", [Near((MSG, F32)), Near((MSG, F32)), Near((MSG, BF16))],
        [near(got), inner_logs], scratch=[pltpu.VMEM(MSG, F32)], flops=1e7,
    )
    groups = swapped(total, OUTER)
    (down,) = call(
        outer_second_kernel, "outer_second", [Near((MSG, BF16))],
        [mine, near(groups), before, through, outer_logs], (0,),
        scratch=[pltpu.VMEM(MSG, F32)], flops=1e7,
    )
    got = swapped(down, INNER)
    mixed, grad = call(
        end_kernel, "end", [Far((TOKS, BF16)), Far((TOKS, BF16))],
        [near(got), cplaced, ccols, clocal, rplaced, rcols, rlocal, near(row_in),
         gain, near(x), ry, cx, far(col_out)],
        left=(12,), kept=(0, 1),
        scratch=[
            pltpu.VMEM((WIDTH, WIDTH), BF16), pltpu.VMEM(TOKS, BF16), pltpu.VMEM(TOKS, BF16),
            pltpu.SemaphoreType.DMA((6,)),
        ],
    )
    return mixed.reshape(cotangent.shape), grad.reshape(tokens.shape)


def solution(mesh):
    torus = Mesh(
        mesh.devices.reshape(4, 8, 2, mesh.shape["frame"]), ("seq_0", "seq_1", "seq_2", "frame")
    )
    tall = P("frame", SEQ, None, None)
    flat = P("frame", None, SEQ, None)
    in_specs = (tall, tall, flat, P(), P(), P(), P(), tall, flat, P(), P(), P(), P(), tall)
    return jax.shard_map(
        body, mesh=torus, in_specs=in_specs, out_specs=(tall, tall), check_vma=False
    )
```
